256 devices in a mesh: dp: 64 (over z, x_hi, y), rep: 4 (over x_lo, core).
Axes of the slice: x: 4 (x_hi: 2, x_lo: 2; x = x_hi * 2 + x_lo), y: 4, z: 8, core: 2. Of those that a mesh axis runs over, the one named last changes fastest.
Arguments:
- tokens: bfloat16 [1024, 128, 2048], P(('dp', 'rep')), may hold values from -32 to 32, as said below
- cotangent: bfloat16 [1024, 128, 1024], P(('dp', 'rep')), may hold values from -6 to 6
- projection: bfloat16 [2048, 1536], replicated, may hold values from -0.25 to 0.25
- block_lengths: int32 [256, 4], P(('dp', 'rep')), may hold values from 0 to 128, as said below
- destination: int32 [256], P(('dp', 'rep')), may hold values from -1 to 63, as said below
Outputs:
- direction: float32 [2048, 1536], P(('dp', 'rep'))
The draws below stay inside these ranges and needn't reach their ends.
Inputs may be any that keep to these rules, and one draw needn't show every extreme that they name: `tokens`: clipped at the range's ends. `block_lengths`: A device's live slots come first, all of length 128 except the last live one, which holds 64 to 128 tokens; later slots have length 0. A device has 1 to 4 live slots, and some device has 4 in every draw. A device has a destination exactly when it has 4 live slots. The destination's dp index differs from the sender's in exactly one bit, the rep index is the same, the receiver has at most 2 live slots, and no device receives from two senders.
All inputs are finite; a program needn't handle non-finite values.
Results may differ from the reference program's by a relative error of at most 0.006.
The reference program's roundings to bfloat16 on the way (of `joined`, `probs`, `grad_values` and `grad_scores`) count: a program that leaves them out, or rounds other values in their place, can miss the bound.
Values may be sent and summed in bfloat16 or wider, within the bound.
A program may use at most 128 MiB of HBM per device.

```python
import math
import jax
import jax.numpy as jnp
from jax import lax

D = 2048
HS = 256
HEADS = 4
BLOCK = 128
SLOTS = 4
QKV = 1536
N_DP = 64
N_REP = 4


def draw_tokens(key, part):
    count = N_DP * N_REP * SLOTS
    base = jax.random.normal(jax.random.fold_in(key, 101), (count, BLOCK, D), jnp.float32)
    return jnp.clip(base, -32.0, 32.0).astype(jnp.bfloat16)


def draw_projection(key, part):
    base = jax.random.normal(jax.random.fold_in(key, 201), (D, QKV), jnp.float32) / jnp.sqrt(1.0 * D)
    return jnp.clip(base, -0.25, 0.25).astype(jnp.bfloat16)


def plan_tables(key):
    keys = jax.random.split(jax.random.fold_in(key, 301), 6)
    levels = N_DP.bit_length() - 1
    bits = jax.random.permutation(keys[0], levels)[:3].astype(jnp.int32)
    index = jnp.arange(N_DP, dtype=jnp.int32)
    use = jnp.where(jnp.bitwise_and(jnp.right_shift(index, bits[1]), 1) == 0, bits[0], bits[2])
    partner = jnp.bitwise_xor(index, jnp.left_shift(jnp.ones_like(index), use))
    lower = jnp.minimum(index, partner)
    heavy_pair = jax.random.randint(keys[1], (N_REP, N_DP), 0, 2)
    heavy_pair = heavy_pair.at[0, 0].set(1)
    heavy_side = jax.random.randint(keys[2], (N_REP, N_DP), 0, 2)
    pair_heavy = jnp.take(heavy_pair, lower, axis=1) == 1
    side = jnp.take(heavy_side, lower, axis=1) == 1
    is_lower = (index == lower)[None, :]
    am_heavy = pair_heavy & (is_lower == side)
    am_light = pair_heavy & jnp.logical_not(am_heavy)
    light_count = jax.random.randint(keys[3], (N_REP, N_DP), 1, 3)
    other_count = jax.random.randint(keys[4], (N_REP, N_DP), 1, 4)
    count = jnp.where(am_heavy, 4, jnp.where(am_light, light_count, other_count))
    target = jnp.where(am_heavy, partner[None, :], -1)
    last = jax.random.randint(keys[5], (N_REP, N_DP), BLOCK // 2, BLOCK + 1)
    slot = jnp.arange(SLOTS, dtype=jnp.int32)
    length = jnp.where(slot[None, None, :] < count[:, :, None] - 1, BLOCK, jnp.where(slot[None, None, :] == count[:, :, None] - 1, last[:, :, None], 0))
    length = jnp.transpose(length, (1, 0, 2)).reshape(N_DP * N_REP, SLOTS)
    target = jnp.transpose(target, (1, 0)).reshape(N_DP * N_REP)
    return (length.astype(jnp.int32), target.astype(jnp.int32))


def draw_block_lengths(key, part):
    return plan_tables(key)[0]


def draw_destination(key, part):
    return plan_tables(key)[1]


def level_of(key, extent, cuts, least, high):
    level, own = 1.0, jax.random.fold_in(key, 6)
    for dim, shards_of in cuts:
        heights = jnp.exp(jax.random.uniform(jax.random.fold_in(own, dim), (shards_of,), jnp.float32, least / len(cuts), high / len(cuts)))
        level = level * jnp.repeat(heights, extent[dim] // shards_of).reshape([-1 if axis == dim else 1 for axis in range(len(extent))])
    return level


def normal_values(key, extent, scale, reach, pieces=(), kind=jnp.bfloat16):
    result = scale * jax.random.normal(key, extent, jnp.float32)
    if pieces:
        result = result * level_of(key, extent, pieces, -0.22, 0.18)
    return jnp.clip(result, -reach, reach).astype(kind)


def setup_inputs(seed: int = 0) -> dict:
    key_list = jax.random.split(jax.random.key(seed), 6)
    tokens = draw_tokens(jax.random.fold_in(key_list[5], 71), 0)
    cotangent = normal_values(key_list[1], (N_DP * N_REP * SLOTS, BLOCK, HEADS * HS), 1.0, 6.0, ((0, 256),))
    projection = draw_projection(jax.random.fold_in(key_list[5], 71), 0)
    block_lengths = draw_block_lengths(jax.random.fold_in(key_list[5], 71), 0)
    destination = draw_destination(jax.random.fold_in(key_list[5], 71), 0)
    return dict(tokens=tokens, cotangent=cotangent, projection=projection, block_lengths=block_lengths, destination=destination)


def block_gradient(blocks, upstream, projection, lengths):
    count = blocks.shape[0]
    width = blocks.shape[2]
    rows = blocks.reshape(count * BLOCK, width)
    joined = jnp.dot(rows, projection, preferred_element_type=jnp.float32).astype(jnp.bfloat16)
    joined = joined.reshape(count, BLOCK, (HEADS + 2) * HS)
    query = joined[:, :, :HEADS * HS].reshape(count, BLOCK, HEADS, HS).astype(jnp.float32)
    keys = joined[:, :, HEADS * HS:(HEADS + 1) * HS].astype(jnp.float32)
    values = joined[:, :, (HEADS + 1) * HS:].astype(jnp.float32)
    scale = HS ** (-0.5)
    scores = jnp.einsum('sihd,sjd->shij', query, keys) * scale
    position = jnp.arange(BLOCK, dtype=jnp.int32)
    causal = position[None, :] <= position[:, None]
    inside = position[None, None, :] < lengths[:, None, None]
    allowed = causal[None] & inside
    scores = jnp.where(allowed[:, None], scores, -1e+30)
    peak = lax.optimization_barrier(jnp.max(scores, axis=-1, keepdims=True))
    expo = jnp.exp(scores - peak)
    weights = expo / lax.optimization_barrier(jnp.sum(expo, axis=-1, keepdims=True))
    probs = weights.astype(jnp.bfloat16)
    live = position[None, :] < lengths[:, None]
    masked = jnp.where(live[:, :, None], upstream, jnp.zeros_like(upstream))
    masked = masked.reshape(count, BLOCK, HEADS, HS).astype(jnp.float32)
    grad_values = jnp.einsum('shij,sihd->sjd', probs.astype(jnp.float32), masked).astype(jnp.bfloat16)
    grad_probs = jnp.einsum('sihd,sjd->shij', masked, values)
    centre = lax.optimization_barrier(jnp.sum(weights * grad_probs, axis=-1, keepdims=True))
    grad_scores = (weights * (grad_probs - centre) * scale).astype(jnp.bfloat16).astype(jnp.float32)
    grad_query = jnp.einsum('shij,sjd->sihd', grad_scores, keys).astype(jnp.bfloat16)
    grad_query = grad_query.reshape(count, BLOCK, HEADS * HS)
    grad_keys = jnp.einsum('shij,sihd->sjd', grad_scores, query).astype(jnp.bfloat16)
    combined = jnp.concatenate([grad_query, grad_keys, grad_values], axis=-1)
    combined = combined.reshape(count * BLOCK, (HEADS + 2) * HS)
    return lax.dot_general(rows, combined, (((0,), (0,)), ((), ())), preferred_element_type=jnp.float32)

def soft_vote(gradient):
    rows = gradient.shape[0]
    grouped = gradient.reshape(rows, HEADS + 2, HS)
    spread = jnp.sqrt(lax.optimization_barrier(jnp.mean(grouped * grouped, axis=(0, 2), keepdims=True)) + 1e-06)
    soft = grouped / (jnp.abs(grouped) + 0.25 * spread)
    return soft.reshape(rows, (HEADS + 2) * HS)

def reference(tokens, cotangent, projection, block_lengths, destination):
    devices = N_DP * N_REP
    blocks = tokens.reshape(N_DP, N_REP, SLOTS, BLOCK, D)
    upstream = cotangent.reshape(N_DP, N_REP, SLOTS, BLOCK, HEADS * HS)
    lengths = block_lengths.reshape(N_DP, N_REP, SLOTS)
    target = destination.reshape(N_DP, N_REP)
    ranks = jnp.arange(N_DP, dtype=jnp.int32)
    hits = target[:, :, None] == ranks[None, None, :]
    receives = jnp.transpose(jnp.any(hits, axis=0))
    sender = jnp.transpose(jnp.argmax(hits.astype(jnp.int32), axis=0)).astype(jnp.int32)

    def accumulate(total, flat):
        data_rank = (flat // N_REP).astype(jnp.int32)
        pair_rank = (flat % N_REP).astype(jnp.int32)
        source = sender[data_rank, pair_rank]
        taken = receives[data_rank, pair_rank]
        own_blocks = blocks[data_rank, pair_rank]
        own_upstream = upstream[data_rank, pair_rank]
        own_lengths = lengths[data_rank, pair_rank]
        third_block = jnp.where(taken, blocks[source, pair_rank, 3], own_blocks[2])
        third_upstream = jnp.where(taken, upstream[source, pair_rank, 3], own_upstream[2])
        third_length = jnp.where(taken, lengths[source, pair_rank, 3], own_lengths[2])
        work_blocks = jnp.concatenate([own_blocks[:2], third_block[None]], axis=0)
        work_upstream = jnp.concatenate([own_upstream[:2], third_upstream[None]], axis=0)
        work_lengths = jnp.concatenate([own_lengths[:2], third_length[None]], axis=0)
        gradient = block_gradient(work_blocks, work_upstream, projection, work_lengths)
        return (total + soft_vote(gradient), None)
    start = jnp.zeros((D, QKV), jnp.float32)
    total, _ = lax.scan(accumulate, start, jnp.arange(devices, dtype=jnp.int32))
    return total / math.sqrt(devices)
```

```python
import math

import jax
import jax.numpy as jnp
from jax import lax
from jax.experimental import pallas as pl
from jax.experimental.pallas import tpu as pltpu
from jax.sharding import Mesh
from jax.sharding import PartitionSpec as P

HS = 256
HEADS = 4
BLOCK = 128
DP_REP = ("dp_0", "dp_1", "dp_2", "rep_0", "rep_1")
REP = ("rep_0", "rep_1")
DP = ("dp_0", "dp_1", "dp_2")
GROUPS = HEADS + 2
D = 2048
MESH = pl.DeviceIdType.MESH
F32 = jnp.float32
BF16 = jnp.bfloat16


def dot(a, b, ca, cb):
    return lax.dot_general(a, b, (((ca,), (cb,)), ((), ())), preferred_element_type=F32)


def gradient_kernel(
    lengths, tok, third, cot, third_cot, proj, soft, x, up, joined, comb, xt, grad
):
    rows = 3 * BLOCK
    x[0 : 2 * BLOCK, :] = tok[...].reshape(2 * BLOCK, D)
    x[2 * BLOCK : rows, :] = third[...]
    up[0 : 2 * BLOCK, :] = cot[...].reshape(2 * BLOCK, HEADS * HS)
    up[2 * BLOCK : rows, :] = third_cot[...]

    @pl.loop(0, GROUPS)
    def _(g):
        cols = pl.ds(pl.multiple_of(g * HS, HS), HS)
        joined[:, cols] = dot(x[...], proj[:, cols], 1, 0).astype(BF16)

    @pl.loop(0, D // 256)
    def _(r):
        at = pl.ds(pl.multiple_of(r * 256, 256), 256)
        xt[at, :] = x[:, at].T

    scale = HS ** (-0.5)

    @pl.loop(0, 3)
    def _(b):
        at = pl.ds(pl.multiple_of(b * BLOCK, BLOCK), BLOCK)
        length = lengths[b]

        def heads(ref):
            return jnp.concatenate(
                [ref[at, h * HS : (h + 1) * HS] for h in range(HEADS)], axis=0
            )

        query = heads(joined)
        keys = joined[at, HEADS * HS : (HEADS + 1) * HS]
        values = joined[at, (HEADS + 1) * HS :]
        shape = (HEADS * BLOCK, BLOCK)
        row = lax.rem(lax.broadcasted_iota(jnp.int32, shape, 0), BLOCK)
        col = lax.broadcasted_iota(jnp.int32, shape, 1)
        allowed = (col <= row) & (col < length)
        scores = jnp.where(allowed, dot(query, keys, 1, 1) * scale, -1e30)
        peak = jnp.max(scores, axis=-1, keepdims=True)
        expo = jnp.exp(scores - peak)
        weights = expo / jnp.sum(expo, axis=-1, keepdims=True)
        wide = (HEADS * BLOCK, HS)
        live = lax.rem(lax.broadcasted_iota(jnp.int32, wide, 0), BLOCK) < length
        upstream = jnp.where(live, heads(up).astype(F32), 0.0).astype(BF16)
        probs = weights.astype(BF16)
        grad_values = dot(probs.T, upstream, 1, 0).astype(BF16)
        grad_probs = dot(upstream, values, 1, 1)
        centre = jnp.sum(weights * grad_probs, axis=-1, keepdims=True)
        grad_scores = (weights * (grad_probs - centre) * scale).astype(BF16)
        grad_query = dot(grad_scores, keys, 1, 0).astype(BF16)
        grad_keys = dot(grad_scores.T, query, 1, 0).astype(BF16)
        for h in range(HEADS):
            comb[at, h * HS : (h + 1) * HS] = grad_query[h * BLOCK : (h + 1) * BLOCK]
        comb[at, HEADS * HS : (HEADS + 1) * HS] = grad_keys
        comb[at, (HEADS + 1) * HS :] = grad_values

    tile = 256

    @pl.loop(0, GROUPS)
    def _(g):
        cols = pl.ds(pl.multiple_of(g * HS, HS), HS)
        total = jnp.zeros((8, HS), F32)
        for r in range(D // tile):
            part = dot(xt[r * tile : (r + 1) * tile, :], comb[:, cols], 1, 0)
            grad[r * tile : (r + 1) * tile, :] = part
            total += jnp.sum((part * part).reshape(tile // 8, 8, HS), axis=0)
        total = jnp.sum(jnp.sum(total, axis=0, keepdims=True), axis=1, keepdims=True)
        spread = 0.25 * jnp.sqrt(total * (1.0 / (D * HS)) + 1e-06)

        @pl.loop(0, D // 128)
        def _(r):
            at = pl.ds(pl.multiple_of(r * 128, 128), 128)
            part = grad[at, :]
            soft[g, at, :] = (part / (jnp.abs(part) + spread)).astype(BF16)


def soft_signs(lengths, tokens, third, cotangent, third_cot, projection):
    vmem = pltpu.VMEM
    rows = 3 * BLOCK
    width = GROUPS * HS
    return pl.pallas_call(
        gradient_kernel,
        out_shape=jax.ShapeDtypeStruct((GROUPS, D, HS), BF16),
        grid=(1,),
        in_specs=[
            pl.BlockSpec(memory_space=pltpu.SMEM),
            pl.BlockSpec((2, BLOCK, D), lambda i: (0, 0, 0)),
            pl.BlockSpec((BLOCK, D), lambda i: (0, 0)),
            pl.BlockSpec((2, BLOCK, HEADS * HS), lambda i: (0, 0, 0)),
            pl.BlockSpec((BLOCK, HEADS * HS), lambda i: (0, 0)),
            pl.BlockSpec((D, width), lambda i: (0, 0)),
        ],
        out_specs=pl.BlockSpec((GROUPS, D, HS), lambda i: (0, 0, 0)),
        scratch_shapes=[
            vmem((rows, D), BF16),
            vmem((rows, HEADS * HS), BF16),
            vmem((rows, width), BF16),
            vmem((rows, width), BF16),
            vmem((D, rows), BF16),
            vmem((D, HS), F32),
        ],
        compiler_params=pltpu.CompilerParams(vmem_limit_bytes=60 << 20),
        name="soft_signs",
    )(lengths, tokens, third, cotangent, third_cot, projection)


NZ, NY, NX = 8, 4, 4


def wrap(i, n):
    return lax.rem(i + n, n)


def vote_kernel(soft, out, own, part, wz, wx, wy, rzp0, rzp1, rzm0, rzm1, szp0, szp1, szm0,
                szm1, rx, sx, ry, sy, ux, uy, uz, vx, vy, vz, tx, ty, tz, qx, qy, qz, res, fin,
                loc, s0, r0, s1, r1, s2, r2, s3, r3, s4, r4):
    z, xh, y, xl, core = [lax.axis_index(a) for a in DP_REP]
    x = xh * 2 + xl

    def at_x(i):
        return {"dp_1": lax.div(i, 2), "rep_0": lax.rem(i, 2)}

    def at_y(i):
        return {"dp_2": i}

    def at_z(i):
        return {"dp_0": i}

    partner = {"rep_1": 1 - core}

    barrier = pltpu.get_barrier_semaphore()
    peers = [partner]
    peers += [at_x(wrap(x + d, NX)) for d in range(1, NX)]
    peers += [at_y(wrap(y + d, NY)) for d in range(1, NY)]
    peers += [at_z(wrap(z + d, NZ)) for d in range(1, NZ)]
    for j in range(3):
        pltpu.make_async_copy(soft.at[core * 3 + j], own.at[j], loc.at[j]).start()
    for peer in peers:
        pl.semaphore_signal(barrier, inc=1, device_id=peer, device_id_type=MESH)
    pl.semaphore_wait(barrier, len(peers))

    sent = []

    def send(src, dst, ss, rs, dev):
        copy = pltpu.make_async_remote_copy(
            src_ref=src, dst_ref=dst, send_sem=ss, recv_sem=rs, device_id=dev, device_id_type=MESH
        )
        copy.start()
        sent.append(copy)
        return copy

    first = [
        send(soft.at[(1 - core) * 3 + j], part.at[j], s0.at[j], r0.at[j], partner)
        for j in range(3)
    ]

    def add(*refs):
        total = refs[0][...].astype(F32)
        for ref in refs[1:]:
            total = total + ref[...].astype(F32)
        return total

    def arrive(j):
        pltpu.make_async_copy(soft.at[core * 3 + j], own.at[j], loc.at[j]).wait()
        first[j].wait_recv()

    arrive(0)

    @pl.loop(0, NZ)
    def _(a):
        for h in range(2):
            wz[a, h] = add(own.at[0, a, h], part.at[0, a, h]).astype(BF16)

    up_z, down_z = at_z(wrap(z + 1, NZ)), at_z(wrap(z - 1, NZ))

    def zpiece(d, h):
        return wz.at[wrap(z + d, NZ), h]

    zp0 = [send(zpiece(4, 0), rzp0.at[0], s1.at[0], r1.at[0], up_z)]
    zm1 = [send(zpiece(-4, 1), rzm1.at[0], s1.at[1], r1.at[1], down_z)]
    zp1 = [send(zpiece(3, 1), rzp1.at[0], s1.at[2], r1.at[2], up_z)]
    zm0 = [send(zpiece(-3, 0), rzm0.at[0], s1.at[3], r1.at[3], down_z)]

    def four_ring(j, c, w, dev, recv, base):
        ahead, behind = dev(wrap(c + 1, 4)), dev(wrap(c - 1, 4))
        far = wrap(c + 2, 4)
        lo, hi = pl.ds(0, 4), pl.ds(4, 4)
        sem = lambda i: (s2.at[base + i], r2.at[base + i])
        return [
            send(w(far).at[lo], recv.at[0], *sem(0), ahead),
            send(w(far).at[hi], recv.at[1], *sem(1), behind),
            send(w(wrap(c + 1, 4)).at[hi], recv.at[3], *sem(2), ahead),
            send(w(wrap(c - 1, 4)).at[lo], recv.at[4], *sem(3), behind),
        ]

    def relay(c, w, dev, recv, hold, base, begun):
        ahead, behind = dev(wrap(c + 1, 4)), dev(wrap(c - 1, 4))
        sem = lambda i: (s2.at[base + i], r2.at[base + i])
        out_copies = []
        for i, (step, half, slot, to) in enumerate(((1, 0, 2, ahead), (-1, 4, 5, behind))):
            begun[i].wait_recv()
            mine = w(wrap(c + step, 4))

            @pl.loop(0, 4)
            def _(a):
                hold[i, a] = add(mine.at[half + a], recv.at[i, a]).astype(BF16)

            out_copies.append(send(hold.at[i], recv.at[slot], *sem(4 + i), to))
        return out_copies

    wx_of = lambda c: wx.at[lax.div(c, 2), lax.rem(c, 2)]
    wy_of = lambda c: wy.at[c]

    arrive(1)

    @pl.loop(0, NZ)
    def _(a):
        for h in range(2):
            for l in range(2):
                wx[h, l, a] = add(own.at[1, a, h, :, l], part.at[1, a, h, :, l]).astype(BF16)

    bx = four_ring(1, x, wx_of, at_x, rx, 0)
    arrive(2)

    @pl.loop(0, NZ)
    def _(a):
        for b in range(NY):
            wy[b, a] = add(own.at[2, a, :, b], part.at[2, a, :, b]).astype(BF16)

    by = four_ring(2, y, wy_of, at_y, ry, 6)

    def z_relay(k):
        def hop(chain, recv, hold, d, h, sem, to):
            chain[k - 1].wait_recv()
            hold[k - 1] = add(zpiece(d, h), recv.at[k - 1]).astype(BF16)
            chain.append(send(hold.at[k - 1], recv.at[k], s1.at[sem], r1.at[sem], to))

        hop(zp0, rzp0, szp0, 4 - k, 0, 4 * k, up_z)
        hop(zm1, rzm1, szm1, k - 4, 1, 4 * k + 1, down_z)
        if k < 3:
            hop(zp1, rzp1, szp1, 3 - k, 1, 4 * k + 2, up_z)
            hop(zm0, rzm0, szm0, k - 3, 0, 4 * k + 3, down_z)

    z_relay(1)
    cx = relay(x, wx_of, at_x, rx, sx, 0, bx)
    cy = relay(y, wy_of, at_y, ry, sy, 6, by)
    z_relay(2)
    z_relay(3)

    def settle(c, w, recv, begun, later, store):
        later[0].wait_recv()
        begun[2].wait_recv()
        begun[3].wait_recv()
        later[1].wait_recv()
        mine = w(c)

        @pl.loop(0, 4)
        def _(a):
            store(a, add(mine.at[a], recv.at[2, a], recv.at[4, a]))
            store(4 + a, add(mine.at[4 + a], recv.at[3, a], recv.at[5, a]))

    def store_x(a, v):
        ux[:, a] = v.astype(BF16)

    def store_y(a, v):
        uy[:, :, a] = v.astype(BF16)

    def spread(u, c, n, dev, recv, ss, rs, base):
        return [
            send(u(wrap(c + d, n)), recv.at[d - 1], ss.at[base + d - 1], rs.at[base + d - 1],
                 dev(wrap(c + d, n)))
            for d in range(1, n)
        ]

    ux_of = lambda c: ux.at[c]
    uy_of = lambda c: uy.at[lax.div(c, 2), lax.rem(c, 2)]
    uz_of = lambda c: uz.at[lax.div(c, 2), lax.rem(c, 2)]
    settle(x, wx_of, rx, bx, cx, store_x)
    dx = spread(ux_of, y, NY, at_y, vx, s3, r3, 0)
    settle(y, wy_of, ry, by, cy, store_y)
    dy = spread(uy_of, x, NX, at_x, vy, s3, r3, 3)
    for chain in (zp0, zm0, zp1, zm1):
        chain[-1].wait_recv()
    for h, (a, b) in enumerate(((rzp0.at[3], rzm0.at[2]), (rzp1.at[2], rzm1.at[3]))):
        v = add(zpiece(0, h), a, b)
        for l in range(2):
            uz[h, l] = v[:, l].astype(BF16)
    dz = spread(uz_of, x, NX, at_x, vz, s3, r3, 6)

    def gather(copies, u, c, recv, hold):
        for copy in copies:
            copy.wait_recv()
        hold[...] = add(u(c), *[recv.at[i] for i in range(len(copies))]).astype(BF16)

    gather(dx, ux_of, y, vx, tx)
    ex = spread(lambda c: tx.at[c], z, NZ, at_z, qx, s4, r4, 0)
    gather(dy, uy_of, x, vy, ty)
    ey = spread(lambda c: ty.at[c], z, NZ, at_z, qy, s4, r4, 7)
    gather(dz, uz_of, x, vz, tz)
    ez = spread(lambda c: tz.at[c], y, NY, at_y, qz, s4, r4, 14)

    def finish(j, copies, mine, recv):
        for copy in copies:
            copy.wait_recv()
        total = add(mine, *[recv.at[i] for i in range(len(copies))]) * (1.0 / 16.0)
        res[j, 0] = total[0:8]
        res[j, 1] = total[8:16]

    finish(0, ez, tz.at[y], qz)
    finish(1, ex, tx.at[z], qx)
    finish(2, ey, ty.at[z], qy)
    ends = [
        send(res.at[j, 1 - core], fin.at[j], s0.at[3 + j], r0.at[3 + j], partner) for j in range(3)
    ]
    for j in range(3):
        out[core * 3 + j] = res[j, core]
    for j in range(3):
        ends[j].wait_recv()
        out[(1 - core) * 3 + j] = fin[j]
    for copy in sent:
        copy.wait_send()


def vote_sum(soft):
    vmem = pltpu.VMEM
    t = (16, HS)
    bf = lambda *dims: vmem(dims + t, BF16)
    sems = lambda n: pltpu.SemaphoreType.DMA((n,))
    scratch = [
        bf(3, 8, 2, 4, 2),
        bf(3, 8, 2, 4, 2),
        bf(8, 2, 4, 2),
        bf(2, 2, 8, 4),
        bf(4, 8, 2, 2),
        bf(4, 4, 2), bf(3, 4, 2), bf(3, 4, 2), bf(4, 4, 2),
        bf(3, 4, 2), bf(2, 4, 2), bf(2, 4, 2), bf(3, 4, 2),
        bf(6, 4, 4), bf(2, 4, 4),
        bf(6, 4, 2, 2), bf(2, 4, 2, 2),
        bf(4, 8), bf(2, 2, 8), bf(2, 2, 4),
        bf(3, 8), bf(3, 8), bf(3, 4),
        bf(8), bf(8), bf(4),
        bf(7), bf(7), bf(3),
        vmem((3, 2, 8, HS), F32),
        vmem((3, 8, HS), F32),
        sems(3),
        sems(6), sems(6), sems(16), sems(16), sems(12), sems(12), sems(9), sems(9), sems(17), sems(17),
    ]
    return pl.pallas_call(
        vote_kernel,
        out_shape=jax.ShapeDtypeStruct((GROUPS, 8, HS), F32),
        in_specs=[pl.BlockSpec(memory_space=pl.ANY)],
        out_specs=pl.BlockSpec(memory_space=pltpu.VMEM),
        scratch_shapes=scratch,
        compiler_params=pltpu.CompilerParams(
            collective_id=1, has_side_effects=True, vmem_limit_bytes=40 << 20
        ),
        name="vote_sum",
    )(soft)


def swapped(value, axis, apart):
    mask = 2**apart
    pairs = [(source, source ^ mask) for source in range(lax.axis_size(axis))]
    return lax.ppermute(value, axis, pairs)


def level_flags(destination, levels):
    everyone = lax.all_gather(destination, DP_REP).reshape(-1)
    n_pairs = lax.axis_size(REP)
    sender_rank = jnp.arange(everyone.shape[0], dtype=jnp.int32) // n_pairs
    differ = jnp.where(everyone >= 0, jnp.bitwise_xor(sender_rank, everyone), 0)
    return [
        jnp.any(jnp.bitwise_and(jnp.right_shift(differ, bit_number), 1) == 1)
        for bit_number in range(levels)
    ]


def receive_block(tokens, cotangent, lengths, target, flags):
    my_rank = lax.axis_index(DP)
    kept_block = tokens[2]
    kept_upstream = cotangent[2]
    kept_length = lengths[2]
    for bit_number in range(len(flags)):
        partner = jnp.bitwise_xor(my_rank, 1 << bit_number)
        sending = target == partner

        def trade(kept, level=bit_number, sending=sending):
            header = jnp.stack([sending.astype(F32), lengths[3].astype(F32)]).astype(BF16)
            got_block, got_upstream, got_header = swapped(
                (tokens[3], cotangent[3], header), DP, level
            )
            arrived = got_header[0] > 0.5
            return (
                jnp.where(arrived, got_block, kept[0]),
                jnp.where(arrived, got_upstream, kept[1]),
                jnp.where(arrived, got_header[1].astype(jnp.int32), kept[2]),
            )

        kept_block, kept_upstream, kept_length = lax.cond(
            flags[bit_number],
            trade,
            lambda kept: kept,
            (kept_block, kept_upstream, kept_length),
        )
    return (kept_block, kept_upstream, kept_length)


def shards(tokens, cotangent, projection, block_lengths, destination):
    lengths = block_lengths[0]
    target = destination[0]
    levels = lax.axis_size(DP).bit_length() - 1
    flags = level_flags(destination, levels)
    third, third_cot, third_length = receive_block(tokens, cotangent, lengths, target, flags)
    work_lengths = jnp.stack([lengths[0], lengths[1], third_length])
    soft = soft_signs(work_lengths, tokens, third, cotangent, third_cot, projection)
    summed = vote_sum(soft.reshape(GROUPS, 8, 2, 4, 2, 16, HS))
    return summed.transpose(1, 0, 2).reshape(8, GROUPS * HS)


def solution(mesh):
    split = Mesh(mesh.devices.reshape(8, 2, 4, 2, 2), DP_REP)
    placed = (P(DP_REP, None, None), P(DP_REP, None, None), P(), P(DP_REP, None), P(DP_REP))
    return jax.shard_map(
        shards, mesh=split, in_specs=placed, out_specs=P(DP_REP, None), check_vma=False
    )
```

```python
import math

import jax
import jax.numpy as jnp
from jax import lax
from jax.experimental import pallas as pl
from jax.experimental.pallas import tpu as pltpu
from jax.sharding import Mesh
from jax.sharding import PartitionSpec as P

HS = 256
HEADS = 4
BLOCK = 128
DP_REP = ("dp_0", "dp_1", "dp_2", "rep_0", "rep_1")
REP = ("rep_0", "rep_1")
DP = ("dp_0", "dp_1", "dp_2")
GROUPS = HEADS + 2
D = 2048
MESH = pl.DeviceIdType.MESH
F32 = jnp.float32
BF16 = jnp.bfloat16


def dot(a, b, ca, cb):
    return lax.dot_general(a, b, (((ca,), (cb,)), ((), ())), preferred_element_type=F32)


def gradient_kernel(
    lengths, info, tok, cot, tok_a, cot_a, tok_b, cot_b, proj, soft, x, up, joined, comb, xt, grad
):
    rows = 3 * BLOCK
    way = info[1, 0]

    def chosen(own, a, b):
        return jnp.where(way == 1, a, jnp.where(way == 2, b, own))

    x[0 : 2 * BLOCK, :] = tok[0:2].reshape(2 * BLOCK, D)
    x[2 * BLOCK : rows, :] = chosen(tok[2], tok_a[...], tok_b[...])
    up[0 : 2 * BLOCK, :] = cot[0:2].reshape(2 * BLOCK, HEADS * HS)
    up[2 * BLOCK : rows, :] = chosen(cot[2], cot_a[...], cot_b[...])

    @pl.loop(0, GROUPS)
    def _(g):
        cols = pl.ds(pl.multiple_of(g * HS, HS), HS)
        joined[:, cols] = dot(x[...], proj[:, cols], 1, 0).astype(BF16)

    @pl.loop(0, D // 256)
    def _(r):
        at = pl.ds(pl.multiple_of(r * 256, 256), 256)
        xt[at, :] = x[:, at].T

    scale = HS ** (-0.5)

    @pl.loop(0, 3)
    def _(b):
        at = pl.ds(pl.multiple_of(b * BLOCK, BLOCK), BLOCK)
        length = jnp.where(b == 2, info[2, 0], lengths[b])

        def heads(ref):
            return jnp.concatenate(
                [ref[at, h * HS : (h + 1) * HS] for h in range(HEADS)], axis=0
            )

        query = heads(joined)
        keys = joined[at, HEADS * HS : (HEADS + 1) * HS]
        values = joined[at, (HEADS + 1) * HS :]
        shape = (HEADS * BLOCK, BLOCK)
        row = lax.rem(lax.broadcasted_iota(jnp.int32, shape, 0), BLOCK)
        col = lax.broadcasted_iota(jnp.int32, shape, 1)
        allowed = (col <= row) & (col < length)
        scores = jnp.where(allowed, dot(query, keys, 1, 1) * scale, -1e30)
        peak = jnp.max(scores, axis=-1, keepdims=True)
        expo = jnp.exp(scores - peak)
        weights = expo / jnp.sum(expo, axis=-1, keepdims=True)
        wide = (HEADS * BLOCK, HS)
        live = lax.rem(lax.broadcasted_iota(jnp.int32, wide, 0), BLOCK) < length
        upstream = jnp.where(live, heads(up).astype(F32), 0.0).astype(BF16)
        probs = weights.astype(BF16)
        grad_values = dot(probs.T, upstream, 1, 0).astype(BF16)
        grad_probs = dot(upstream, values, 1, 1)
        centre = jnp.sum(weights * grad_probs, axis=-1, keepdims=True)
        grad_scores = (weights * (grad_probs - centre) * scale).astype(BF16)
        grad_query = dot(grad_scores, keys, 1, 0).astype(BF16)
        grad_keys = dot(grad_scores.T, query, 1, 0).astype(BF16)
        for h in range(HEADS):
            comb[at, h * HS : (h + 1) * HS] = grad_query[h * BLOCK : (h + 1) * BLOCK]
        comb[at, HEADS * HS : (HEADS + 1) * HS] = grad_keys
        comb[at, (HEADS + 1) * HS :] = grad_values

    tile = 256

    @pl.loop(0, GROUPS)
    def _(g):
        cols = pl.ds(pl.multiple_of(g * HS, HS), HS)
        total = jnp.zeros((8, HS), F32)
        for r in range(D // tile):
            part = dot(xt[r * tile : (r + 1) * tile, :], comb[:, cols], 1, 0)
            grad[r * tile : (r + 1) * tile, :] = part
            total += jnp.sum((part * part).reshape(tile // 8, 8, HS), axis=0)
        total = jnp.sum(jnp.sum(total, axis=0, keepdims=True), axis=1, keepdims=True)
        spread = 0.25 * jnp.sqrt(total * (1.0 / (D * HS)) + 1e-06)

        @pl.loop(0, D // 128)
        def _(r):
            at = pl.ds(pl.multiple_of(r * 128, 128), 128)
            part = grad[at, :]
            soft[g, at, :] = (part / (jnp.abs(part) + spread)).astype(BF16)


def soft_signs(lengths, info, tokens, cotangent, moved, projection):
    vmem = pltpu.VMEM
    rows = 3 * BLOCK
    width = GROUPS * HS
    return pl.pallas_call(
        gradient_kernel,
        out_shape=jax.ShapeDtypeStruct((GROUPS, D, HS), BF16),
        grid=(1,),
        in_specs=[
            pl.BlockSpec(memory_space=pltpu.SMEM),
            pl.BlockSpec(memory_space=pltpu.SMEM),
            pl.BlockSpec((3, BLOCK, D), lambda i: (0, 0, 0)),
            pl.BlockSpec((3, BLOCK, HEADS * HS), lambda i: (0, 0, 0)),
            pl.BlockSpec((BLOCK, D), lambda i: (0, 0)),
            pl.BlockSpec((BLOCK, HEADS * HS), lambda i: (0, 0)),
            pl.BlockSpec((BLOCK, D), lambda i: (0, 0)),
            pl.BlockSpec((BLOCK, HEADS * HS), lambda i: (0, 0)),
            pl.BlockSpec((D, width), lambda i: (0, 0)),
        ],
        out_specs=pl.BlockSpec((GROUPS, D, HS), lambda i: (0, 0, 0)),
        scratch_shapes=[
            vmem((rows, D), BF16),
            vmem((rows, HEADS * HS), BF16),
            vmem((rows, width), BF16),
            vmem((rows, width), BF16),
            vmem((D, rows), BF16),
            vmem((D, HS), F32),
        ],
        compiler_params=pltpu.CompilerParams(vmem_limit_bytes=60 << 20),
        name="soft_signs",
    )(lengths, info, tokens, cotangent, *moved, projection)


NZ, NY, NX = 8, 4, 4


def wrap(i, n):
    return lax.rem(i + n, n)


def vote_kernel(soft, out, own, part, wz, wx, wy, rzp0, rzp1, rzm0, rzm1, szp0, szp1, szm0,
                szm1, rx, sx, ry, sy, ux, uy, uz, vx, vy, vz, tx, ty, tz, qx, qy, qz, res, fin,
                loc, s0, r0, s1, r1, s2, r2, s3, r3, s4, r4):
    z, xh, y, xl, core = [lax.axis_index(a) for a in DP_REP]
    x = xh * 2 + xl

    def at_x(i):
        return {"dp_1": lax.div(i, 2), "rep_0": lax.rem(i, 2)}

    def at_y(i):
        return {"dp_2": i}

    def at_z(i):
        return {"dp_0": i}

    partner = {"rep_1": 1 - core}

    barrier = pltpu.get_barrier_semaphore()
    peers = [partner]
    peers += [at_x(wrap(x + d, NX)) for d in range(1, NX)]
    peers += [at_y(wrap(y + d, NY)) for d in range(1, NY)]
    peers += [at_z(wrap(z + d, NZ)) for d in range(1, NZ)]
    for j in range(3):
        pltpu.make_async_copy(soft.at[core * 3 + j], own.at[j], loc.at[j]).start()
    for peer in peers:
        pl.semaphore_signal(barrier, inc=1, device_id=peer, device_id_type=MESH)
    pl.semaphore_wait(barrier, len(peers))

    sent = []

    def send(src, dst, ss, rs, dev):
        copy = pltpu.make_async_remote_copy(
            src_ref=src, dst_ref=dst, send_sem=ss, recv_sem=rs, device_id=dev, device_id_type=MESH
        )
        copy.start()
        sent.append(copy)
        return copy

    first = [
        send(soft.at[(1 - core) * 3 + j], part.at[j], s0.at[j], r0.at[j], partner)
        for j in range(3)
    ]

    def add(*refs):
        total = refs[0][...].astype(F32)
        for ref in refs[1:]:
            total = total + ref[...].astype(F32)
        return total

    def arrive(j):
        pltpu.make_async_copy(soft.at[core * 3 + j], own.at[j], loc.at[j]).wait()
        first[j].wait_recv()

    arrive(0)

    @pl.loop(0, NZ)
    def _(a):
        for h in range(2):
            wz[a, h] = add(own.at[0, a, h], part.at[0, a, h]).astype(BF16)

    up_z, down_z = at_z(wrap(z + 1, NZ)), at_z(wrap(z - 1, NZ))

    def zpiece(d, h):
        return wz.at[wrap(z + d, NZ), h]

    zp0 = [send(zpiece(4, 0), rzp0.at[0], s1.at[0], r1.at[0], up_z)]
    zm1 = [send(zpiece(-4, 1), rzm1.at[0], s1.at[1], r1.at[1], down_z)]
    zp1 = [send(zpiece(3, 1), rzp1.at[0], s1.at[2], r1.at[2], up_z)]
    zm0 = [send(zpiece(-3, 0), rzm0.at[0], s1.at[3], r1.at[3], down_z)]

    def four_ring(j, c, w, dev, recv, base):
        ahead, behind = dev(wrap(c + 1, 4)), dev(wrap(c - 1, 4))
        far = wrap(c + 2, 4)
        lo, hi = pl.ds(0, 4), pl.ds(4, 4)
        sem = lambda i: (s2.at[base + i], r2.at[base + i])
        return [
            send(w(far).at[lo], recv.at[0], *sem(0), ahead),
            send(w(far).at[hi], recv.at[1], *sem(1), behind),
            send(w(wrap(c + 1, 4)).at[hi], recv.at[3], *sem(2), ahead),
            send(w(wrap(c - 1, 4)).at[lo], recv.at[4], *sem(3), behind),
        ]

    def relay(c, w, dev, recv, hold, base, begun):
        ahead, behind = dev(wrap(c + 1, 4)), dev(wrap(c - 1, 4))
        sem = lambda i: (s2.at[base + i], r2.at[base + i])
        out_copies = []
        for i, (step, half, slot, to) in enumerate(((1, 0, 2, ahead), (-1, 4, 5, behind))):
            begun[i].wait_recv()
            mine = w(wrap(c + step, 4))

            @pl.loop(0, 4)
            def _(a):
                hold[i, a] = add(mine.at[half + a], recv.at[i, a]).astype(BF16)

            out_copies.append(send(hold.at[i], recv.at[slot], *sem(4 + i), to))
        return out_copies

    wx_of = lambda c: wx.at[lax.div(c, 2), lax.rem(c, 2)]
    wy_of = lambda c: wy.at[c]

    arrive(1)

    @pl.loop(0, NZ)
    def _(a):
        for h in range(2):
            for l in range(2):
                wx[h, l, a] = add(own.at[1, a, h, :, l], part.at[1, a, h, :, l]).astype(BF16)

    bx = four_ring(1, x, wx_of, at_x, rx, 0)
    arrive(2)

    @pl.loop(0, NZ)
    def _(a):
        for b in range(NY):
            wy[b, a] = add(own.at[2, a, :, b], part.at[2, a, :, b]).astype(BF16)

    by = four_ring(2, y, wy_of, at_y, ry, 6)

    def z_relay(k):
        def hop(chain, recv, hold, d, h, sem, to):
            chain[k - 1].wait_recv()
            hold[k - 1] = add(zpiece(d, h), recv.at[k - 1]).astype(BF16)
            chain.append(send(hold.at[k - 1], recv.at[k], s1.at[sem], r1.at[sem], to))

        hop(zp0, rzp0, szp0, 4 - k, 0, 4 * k, up_z)
        hop(zm1, rzm1, szm1, k - 4, 1, 4 * k + 1, down_z)
        if k < 3:
            hop(zp1, rzp1, szp1, 3 - k, 1, 4 * k + 2, up_z)
            hop(zm0, rzm0, szm0, k - 3, 0, 4 * k + 3, down_z)

    z_relay(1)
    cx = relay(x, wx_of, at_x, rx, sx, 0, bx)
    cy = relay(y, wy_of, at_y, ry, sy, 6, by)
    z_relay(2)
    z_relay(3)

    def settle(c, w, recv, begun, later, store):
        later[0].wait_recv()
        begun[2].wait_recv()
        begun[3].wait_recv()
        later[1].wait_recv()
        mine = w(c)

        @pl.loop(0, 4)
        def _(a):
            store(a, add(mine.at[a], recv.at[2, a], recv.at[4, a]))
            store(4 + a, add(mine.at[4 + a], recv.at[3, a], recv.at[5, a]))

    def store_x(a, v):
        ux[:, a] = v.astype(BF16)

    def store_y(a, v):
        uy[:, :, a] = v.astype(BF16)

    def spread(u, c, n, dev, recv, ss, rs, base):
        return [
            send(u(wrap(c + d, n)), recv.at[d - 1], ss.at[base + d - 1], rs.at[base + d - 1],
                 dev(wrap(c + d, n)))
            for d in range(1, n)
        ]

    ux_of = lambda c: ux.at[c]
    uy_of = lambda c: uy.at[lax.div(c, 2), lax.rem(c, 2)]
    uz_of = lambda c: uz.at[lax.div(c, 2), lax.rem(c, 2)]
    settle(x, wx_of, rx, bx, cx, store_x)
    dx = spread(ux_of, y, NY, at_y, vx, s3, r3, 0)
    settle(y, wy_of, ry, by, cy, store_y)
    dy = spread(uy_of, x, NX, at_x, vy, s3, r3, 3)
    for chain in (zp0, zm0, zp1, zm1):
        chain[-1].wait_recv()
    for h, (a, b) in enumerate(((rzp0.at[3], rzm0.at[2]), (rzp1.at[2], rzm1.at[3]))):
        v = add(zpiece(0, h), a, b)
        for l in range(2):
            uz[h, l] = v[:, l].astype(BF16)
    dz = spread(uz_of, x, NX, at_x, vz, s3, r3, 6)

    def gather(copies, u, c, recv, hold):
        for copy in copies:
            copy.wait_recv()
        hold[...] = add(u(c), *[recv.at[i] for i in range(len(copies))]).astype(BF16)

    gather(dx, ux_of, y, vx, tx)
    ex = spread(lambda c: tx.at[c], z, NZ, at_z, qx, s4, r4, 0)
    gather(dy, uy_of, x, vy, ty)
    ey = spread(lambda c: ty.at[c], z, NZ, at_z, qy, s4, r4, 7)
    gather(dz, uz_of, x, vz, tz)
    ez = spread(lambda c: tz.at[c], y, NY, at_y, qz, s4, r4, 14)

    def finish(j, copies, mine, recv):
        for copy in copies:
            copy.wait_recv()
        total = add(mine, *[recv.at[i] for i in range(len(copies))]) * (1.0 / 16.0)
        res[j, 0] = total[0:8]
        res[j, 1] = total[8:16]

    finish(0, ez, tz.at[y], qz)
    finish(1, ex, tx.at[z], qx)
    finish(2, ey, ty.at[z], qy)
    ends = [
        send(res.at[j, 1 - core], fin.at[j], s0.at[3 + j], r0.at[3 + j], partner) for j in range(3)
    ]
    for j in range(3):
        out[core * 3 + j] = res[j, core]
    for j in range(3):
        ends[j].wait_recv()
        out[(1 - core) * 3 + j] = fin[j]
    for copy in sent:
        copy.wait_send()


def vote_sum(soft):
    vmem = pltpu.VMEM
    t = (16, HS)
    bf = lambda *dims: vmem(dims + t, BF16)
    sems = lambda n: pltpu.SemaphoreType.DMA((n,))
    scratch = [
        bf(3, 8, 2, 4, 2),
        bf(3, 8, 2, 4, 2),
        bf(8, 2, 4, 2),
        bf(2, 2, 8, 4),
        bf(4, 8, 2, 2),
        bf(4, 4, 2), bf(3, 4, 2), bf(3, 4, 2), bf(4, 4, 2),
        bf(3, 4, 2), bf(2, 4, 2), bf(2, 4, 2), bf(3, 4, 2),
        bf(6, 4, 4), bf(2, 4, 4),
        bf(6, 4, 2, 2), bf(2, 4, 2, 2),
        bf(4, 8), bf(2, 2, 8), bf(2, 2, 4),
        bf(3, 8), bf(3, 8), bf(3, 4),
        bf(8), bf(8), bf(4),
        bf(7), bf(7), bf(3),
        vmem((3, 2, 8, HS), F32),
        vmem((3, 8, HS), F32),
        sems(3),
        sems(6), sems(6), sems(16), sems(16), sems(12), sems(12), sems(9), sems(9), sems(17), sems(17),
    ]
    return pl.pallas_call(
        vote_kernel,
        out_shape=jax.ShapeDtypeStruct((GROUPS, 8, HS), F32),
        in_specs=[pl.BlockSpec(memory_space=pl.ANY)],
        out_specs=pl.BlockSpec(memory_space=pltpu.VMEM),
        scratch_shapes=scratch,
        compiler_params=pltpu.CompilerParams(
            collective_id=1, has_side_effects=True, vmem_limit_bytes=40 << 20
        ),
        name="vote_sum",
    )(soft)


LEVELS = 6
PAIRS = [(a, b) for a in range(LEVELS) for b in range(a + 1, LEVELS)]
ALONE = {0: (0, 2), 1: (1, 2), 2: (0, 2), 3: (2, 3), 4: (2, 4), 5: (2, 5)}


def flipped(i, m):
    return i + m - 2 * m * lax.rem(lax.div(i, m), 2)


def across(level):
    if level < 2:
        return {"dp_2": flipped(lax.axis_index("dp_2"), 1 << level)}
    if level == 2:
        return {"dp_1": 1 - lax.axis_index("dp_1")}
    return {"dp_0": flipped(lax.axis_index("dp_0"), 1 << (level - 3))}


def plan_kernel(dest, lengths, info, tile, from_x, from_y, from_z, ss, rs):
    z, xh, y, xl, core = [lax.axis_index(a) for a in DP_REP]
    x = xh * 2 + xl
    rank = (z * 2 + xh) * 4 + y
    pair = xl * 2 + core

    def at_x(i, c):
        return {"dp_1": lax.div(i, 2), "rep_0": lax.rem(i, 2), "rep_1": c}

    stage_x = [{"rep_1": 1 - core}]
    stage_x += [at_x(wrap(x + d, NX), core) for d in range(1, NX)]
    stage_x += [at_x(wrap(x + d, NX), 1 - core) for d in range(1, NX)]
    stage_y = [{"dp_2": wrap(y + d, NY)} for d in range(1, NY)]
    stage_z = [{"dp_0": wrap(z + d, NZ)} for d in range(1, NZ)]
    peers = stage_x + stage_y + stage_z
    barrier = pltpu.get_barrier_semaphore()
    for peer in peers:
        pl.semaphore_signal(barrier, inc=1, device_id=peer, device_id_type=MESH)

    shape = (8, 128)
    slot = lax.broadcasted_iota(jnp.int32, shape, 0) * 128 + lax.broadcasted_iota(jnp.int32, shape, 1)
    target = jnp.full(shape, dest[0], jnp.int32)
    code = jnp.zeros(shape, jnp.int32)
    for level in range(LEVELS):
        code = jnp.where(target == flipped(rank, 1 << level), level + 1, code)
    code = code * 256 + jnp.full(shape, lengths[3], jnp.int32)
    mine = (slot == rank * 4 + pair) & (target >= 0)
    tile[0] = jnp.where(mine, code, 0)
    pl.semaphore_wait(barrier, len(peers))

    sent = []
    base = 0
    for k, (stage, landing) in enumerate(((stage_x, from_x), (stage_y, from_y), (stage_z, from_z))):
        copies = []
        for i, peer in enumerate(stage):
            copy = pltpu.make_async_remote_copy(
                src_ref=tile.at[k], dst_ref=landing.at[i], send_sem=ss.at[base + i],
                recv_sem=rs.at[base + i], device_id=peer, device_id_type=MESH,
            )
            copy.start()
            copies.append(copy)
        base += len(stage)
        sent += copies
        for copy in copies:
            copy.wait_recv()
        table = tile[k]
        for i in range(len(stage)):
            table = jnp.maximum(table, landing[i])
        tile[k + 1] = table

    level_of = lax.shift_right_logical(table, 8).astype(F32)
    length_of = jnp.bitwise_and(table, 255).astype(F32)

    def largest(v):
        return jnp.max(jnp.max(v, axis=1, keepdims=True), axis=0, keepdims=True)

    active = jnp.zeros((1, 1), F32)
    inbound = jnp.zeros((1, 1), F32)
    arriving = jnp.zeros((1, 1), F32)
    for level in range(LEVELS):
        here = level_of == level + 1.0
        active += largest(jnp.where(here, 1.0, 0.0)) * (1 << level)
        mine = here & (slot == flipped(rank, 1 << level) * 4 + pair)
        inbound += largest(jnp.where(mine, level + 1.0, 0.0))
        arriving += largest(jnp.where(mine, length_of, 0.0))
    third = jnp.where(inbound > 0.0, arriving, jnp.full((1, 1), lengths[2], jnp.int32).astype(F32))
    branch = jnp.full((1, 1), float(len(PAIRS)), F32)
    way = jnp.ones((1, 1), F32)
    for p, (a, b) in enumerate(PAIRS):
        sets = [(1 << a) + (1 << b)] + [1 << s for s, both in ALONE.items() if both == (a, b)]
        hit = active == float(sets[0])
        for other in sets[1:] + ([0] if p == 0 else []):
            hit = hit | (active == float(other))
        branch = jnp.where(hit, float(p), branch)
        by = jnp.where(inbound == a + 1.0, 1.0, jnp.where(inbound == b + 1.0, 2.0, 0.0))
        way = jnp.where(hit, by, way)
    row = lax.broadcasted_iota(jnp.int32, shape, 0)
    told = jnp.zeros(shape, F32)
    for i, v in enumerate((branch, way, third, inbound, active)):
        told = jnp.where(row == i, v, told)
    info[...] = told.astype(jnp.int32)
    for copy in sent:
        copy.wait_send()


def plan(destination, lengths):
    vmem = pltpu.VMEM
    t = (8, 128)
    n = 2 * NX - 1 + NY - 1 + NZ - 1
    return pl.pallas_call(
        plan_kernel,
        out_shape=jax.ShapeDtypeStruct(t, jnp.int32),
        in_specs=[pl.BlockSpec(memory_space=pltpu.SMEM)] * 2,
        out_specs=pl.BlockSpec(memory_space=vmem),
        scratch_shapes=[
            vmem((4,) + t, jnp.int32),
            vmem((2 * NX - 1,) + t, jnp.int32),
            vmem((NY - 1,) + t, jnp.int32),
            vmem((NZ - 1,) + t, jnp.int32),
            pltpu.SemaphoreType.DMA((n,)),
            pltpu.SemaphoreType.DMA((n,)),
        ],
        compiler_params=pltpu.CompilerParams(collective_id=2, has_side_effects=True),
        name="plan",
    )(destination, lengths)


def move_pair(p):
    peers_of = PAIRS[p]

    def kernel(tokens, cotangent, tok_a, cot_a, tok_b, cot_b, ss, rs):
        peers = [across(level) for level in peers_of]
        barrier = pltpu.get_barrier_semaphore()
        for peer in peers:
            pl.semaphore_signal(barrier, inc=1, device_id=peer, device_id_type=MESH)
        pl.semaphore_wait(barrier, 2)
        copies = []
        for i, (src, dst, peer) in enumerate((
            (tokens, tok_a, peers[0]), (tokens, tok_b, peers[1]),
            (cotangent, cot_a, peers[0]), (cotangent, cot_b, peers[1]),
        )):
            copies.append(pltpu.make_async_remote_copy(
                src_ref=src.at[3], dst_ref=dst, send_sem=ss.at[i], recv_sem=rs.at[i],
                device_id=peer, device_id_type=MESH,
            ))
            copies[-1].start()
        for copy in copies:
            copy.wait()

    def call(tokens, cotangent, info):
        block = jax.ShapeDtypeStruct(tokens.shape[1:], BF16)
        upstream = jax.ShapeDtypeStruct(cotangent.shape[1:], BF16)
        return pl.pallas_call(
            kernel,
            out_shape=(block, upstream, block, upstream),
            in_specs=[pl.BlockSpec(memory_space=pl.ANY)] * 2,
            out_specs=[pl.BlockSpec(memory_space=pl.ANY)] * 4,
            scratch_shapes=[pltpu.SemaphoreType.DMA((4,)), pltpu.SemaphoreType.DMA((4,))],
            compiler_params=pltpu.CompilerParams(collective_id=3 + p, has_side_effects=True),
            name="move",
        )(tokens, cotangent)

    return call


def swapped(value, axis, apart):
    mask = 2**apart
    pairs = [(source, source ^ mask) for source in range(lax.axis_size(axis))]
    return lax.ppermute(value, axis, pairs)


def move_many(tokens, cotangent, info):
    kept = (tokens[2], cotangent[2])
    for level in range(LEVELS):

        def trade(kept, level=level):
            got = swapped((tokens[3], cotangent[3]), DP, level)
            arrived = info[3, 0] == level + 1
            return jax.tree.map(lambda new, old: jnp.where(arrived, new, old), got, kept)

        needed = jnp.bitwise_and(jnp.right_shift(info[4, 0], level), 1) == 1
        kept = lax.cond(needed, trade, lambda kept: kept, kept)
    return (*kept, *kept)


def shards(tokens, cotangent, projection, block_lengths, destination):
    lengths = block_lengths[0]
    info = plan(destination, lengths)
    branches = [move_pair(p) for p in range(len(PAIRS))] + [move_many]
    moved = lax.switch(info[0, 0], branches, tokens, cotangent, info)
    soft = soft_signs(lengths, info, tokens, cotangent, moved, projection)
    summed = vote_sum(soft.reshape(GROUPS, 8, 2, 4, 2, 16, HS))
    return summed.transpose(1, 0, 2).reshape(8, GROUPS * HS)


def solution(mesh):
    split = Mesh(mesh.devices.reshape(8, 2, 4, 2, 2), DP_REP)
    placed = (P(DP_REP, None, None), P(DP_REP, None, None), P(), P(DP_REP, None), P(DP_REP))
    return jax.shard_map(
        shards, mesh=split, in_specs=placed, out_specs=P(DP_REP, None), check_vma=False
    )
```

```python
import math

import jax
import jax.numpy as jnp
from jax import lax
from jax.experimental import pallas as pl
from jax.experimental.pallas import tpu as pltpu
from jax.sharding import Mesh
from jax.sharding import PartitionSpec as P

HS = 256
HEADS = 4
BLOCK = 128
DP_REP = ("dp_0", "dp_1", "dp_2", "rep_0", "rep_1")
REP = ("rep_0", "rep_1")
DP = ("dp_0", "dp_1", "dp_2")
GROUPS = HEADS + 2
D = 2048
MESH = pl.DeviceIdType.MESH
F32 = jnp.float32
BF16 = jnp.bfloat16


def dot(a, b, ca, cb):
    return lax.dot_general(a, b, (((ca,), (cb,)), ((), ())), preferred_element_type=F32)


def attention(at, length, joined, up, comb):
    scale = HS ** (-0.5)

    def heads(ref):
        return jnp.concatenate([ref[at, h * HS : (h + 1) * HS] for h in range(HEADS)], axis=0)

    query = heads(joined)
    keys = joined[at, HEADS * HS : (HEADS + 1) * HS]
    values = joined[at, (HEADS + 1) * HS :]
    shape = (HEADS * BLOCK, BLOCK)
    row = lax.rem(lax.broadcasted_iota(jnp.int32, shape, 0), BLOCK)
    col = lax.broadcasted_iota(jnp.int32, shape, 1)
    allowed = (col <= row) & (col < length)
    scores = jnp.where(allowed, dot(query, keys, 1, 1) * scale, -1e30)
    peak = jnp.max(scores, axis=-1, keepdims=True)
    expo = jnp.exp(scores - peak)
    weights = expo / jnp.sum(expo, axis=-1, keepdims=True)
    wide = (HEADS * BLOCK, HS)
    live = lax.rem(lax.broadcasted_iota(jnp.int32, wide, 0), BLOCK) < length
    upstream = jnp.where(live, heads(up).astype(F32), 0.0).astype(BF16)
    probs = weights.astype(BF16)
    grad_values = dot(probs.T, upstream, 1, 0).astype(BF16)
    grad_probs = dot(upstream, values, 1, 1)
    centre = jnp.sum(weights * grad_probs, axis=-1, keepdims=True)
    grad_scores = (weights * (grad_probs - centre) * scale).astype(BF16)
    grad_query = dot(grad_scores, keys, 1, 0).astype(BF16)
    grad_keys = dot(grad_scores.T, query, 1, 0).astype(BF16)
    for h in range(HEADS):
        comb[at, h * HS : (h + 1) * HS] = grad_query[h * BLOCK : (h + 1) * BLOCK]
    comb[at, HEADS * HS : (HEADS + 1) * HS] = grad_keys
    comb[at, (HEADS + 1) * HS :] = grad_values


def columns(ref, g):
    return ref.at[:, pl.ds(pl.multiple_of(g * HS, HS), HS)]


def join(first, last, proj, proj_v, sem, x, joined):
    @pl.loop(first, last)
    def _(g):
        pltpu.make_async_copy(columns(proj, g), proj_v.at[g], sem.at[g]).wait()
        cols = pl.ds(pl.multiple_of(g * HS, HS), HS)
        joined[:, cols] = dot(x[...], proj_v[g], 1, 0).astype(BF16)


NZ, NY, NX = 8, 4, 4


def wrap(i, n):
    return lax.rem(i + n, n)


def vote_kernel(lengths, info, tok, cot, tok_a, cot_a, tok_b, cot_b, proj, comb_hbm, xt_hbm, out,
                cand_t, cand_c, proj_v, comb01, xt01, x3, up3, joined3, comb3, xt3, grad, mail,
                part, wz, wx, wy, rzp0, rzp1, rzm0, rzm1, szp0, szp1, szm0,
                szm1, rx, sx, ry, sy, ux, uy, uz, vx, vy, vz, tx, ty, tz, qx, qy, qz, res, fin,
                loc, psem, s0, r0, s1, r1, s2, r2, s3, r3, s4, r4):
    z, xh, y, xl, core = [lax.axis_index(a) for a in DP_REP]
    x = xh * 2 + xl

    def at_x(i):
        return {"dp_1": lax.div(i, 2), "rep_0": lax.rem(i, 2)}

    def at_y(i):
        return {"dp_2": i}

    def at_z(i):
        return {"dp_0": i}

    partner = {"rep_1": 1 - core}

    loads = [(tok.at[2], cand_t.at[0]), (tok_a, cand_t.at[1]), (tok_b, cand_t.at[2])]
    loads += [(cot.at[2], cand_c.at[0]), (cot_a, cand_c.at[1]), (cot_b, cand_c.at[2])]
    loads += [(comb_hbm, comb01), (xt_hbm, xt01)]
    loads = [pltpu.make_async_copy(a, b, loc.at[i]) for i, (a, b) in enumerate(loads)]
    for load in loads[:3]:
        load.start()
    for g in range(GROUPS):
        pltpu.make_async_copy(columns(proj, g), proj_v.at[g], psem.at[g]).start()
    for load in loads[3:]:
        load.start()

    barrier = pltpu.get_barrier_semaphore()
    peers = [partner]
    peers += [at_x(wrap(x + d, NX)) for d in range(1, NX)]
    peers += [at_y(wrap(y + d, NY)) for d in range(1, NY)]
    peers += [at_z(wrap(z + d, NZ)) for d in range(1, NZ)]
    for peer in peers:
        pl.semaphore_signal(barrier, inc=1, device_id=peer, device_id_type=MESH)

    sent = []

    def send(src, dst, ss, rs, dev):
        copy = pltpu.make_async_remote_copy(
            src_ref=src, dst_ref=dst, send_sem=ss, recv_sem=rs, device_id=dev, device_id_type=MESH
        )
        copy.start()
        sent.append(copy)
        return copy

    def add(*refs):
        total = refs[0][...].astype(F32)
        for ref in refs[1:]:
            total = total + ref[...].astype(F32)
        return total

    way = info[1, 0]

    def chosen(c):
        return jnp.where(way == 1, c[1], jnp.where(way == 2, c[2], c[0]))

    for load in loads[:3]:
        load.wait()
    x3[...] = chosen(cand_t)
    join(0, GROUPS, proj, proj_v, psem, x3, joined3)
    for r in range(D // 512):
        xt3[r * 512 : (r + 1) * 512, :] = x3[:, r * 512 : (r + 1) * 512].T
    for load in loads[3:]:
        load.wait()
    up3[...] = chosen(cand_c)
    attention(slice(None), info[2, 0], joined3, up3, comb3)
    pl.semaphore_wait(barrier, len(peers))

    tile = 128
    other = 1 - core

    def step(begin, end):
        if begin is not None:
            j, to_partner, buf = begin
            cols = pl.ds(pl.multiple_of(((other if to_partner else core) * 3 + j) * HS, HS), HS)

        def body(a, total):
            for h in range(2):
                at = pl.ds(pl.multiple_of(a * 256 + h * tile, tile), tile)
                if begin is not None:
                    new = dot(xt01[at, :], comb01[:, cols], 1, 0)
                    new = new + dot(xt3[at, :], comb3[:, cols], 1, 0)
                    grad[buf, at, :] = new
                    total = total + jnp.sum((new * new).reshape(tile // 8, 8, HS), axis=0)
                if end is not None:
                    old = grad[end[2], at, :]
                    soft = (old / (jnp.abs(old) + end[3])).reshape(NY, 2, 16, HS)
                    if end[1]:
                        mail[end[0], a, h] = soft.astype(BF16)
                    else:
                        both = (soft + part[end[0], a, h].astype(F32)).astype(BF16)
                        if end[0] == 0:
                            wz[a, h] = both
                        elif end[0] == 1:
                            for l in range(2):
                                wx[h, l, a] = both[:, l]
                        else:
                            for b in range(NY):
                                wy[b, a, h] = both[b]
            return total

        total = lax.fori_loop(0, NZ, body, jnp.zeros((8, HS), F32))
        if begin is None:
            return None
        total = jnp.sum(jnp.sum(total, axis=0, keepdims=True), axis=1, keepdims=True)
        return (*begin, 0.25 * jnp.sqrt(total * (1.0 / (D * HS)) + 1e-06))

    first = {}

    def post(j):
        first[j] = send(mail.at[j], part.at[j], s0.at[j], r0.at[j], partner)

    now = step((0, True, 0), None)
    now = step((1, True, 1), now)
    post(0)
    now = step((0, False, 0), now)
    post(1)
    first[0].wait_recv()
    now = step((2, True, 1), now)

    up_z, down_z = at_z(wrap(z + 1, NZ)), at_z(wrap(z - 1, NZ))

    def zpiece(d, h):
        return wz.at[wrap(z + d, NZ), h]

    zp0 = [send(zpiece(4, 0), rzp0.at[0], s1.at[0], r1.at[0], up_z)]
    zm1 = [send(zpiece(-4, 1), rzm1.at[0], s1.at[1], r1.at[1], down_z)]
    zp1 = [send(zpiece(3, 1), rzp1.at[0], s1.at[2], r1.at[2], up_z)]
    zm0 = [send(zpiece(-3, 0), rzm0.at[0], s1.at[3], r1.at[3], down_z)]

    def four_ring(j, c, w, dev, recv, base):
        ahead, behind = dev(wrap(c + 1, 4)), dev(wrap(c - 1, 4))
        far = wrap(c + 2, 4)
        lo, hi = pl.ds(0, 4), pl.ds(4, 4)
        sem = lambda i: (s2.at[base + i], r2.at[base + i])
        return [
            send(w(far).at[lo], recv.at[0], *sem(0), ahead),
            send(w(far).at[hi], recv.at[1], *sem(1), behind),
            send(w(wrap(c + 1, 4)).at[hi], recv.at[3], *sem(2), ahead),
            send(w(wrap(c - 1, 4)).at[lo], recv.at[4], *sem(3), behind),
        ]

    def relay(c, w, dev, recv, hold, base, begun):
        ahead, behind = dev(wrap(c + 1, 4)), dev(wrap(c - 1, 4))
        sem = lambda i: (s2.at[base + i], r2.at[base + i])
        out_copies = []
        for i, (step, half, slot, to) in enumerate(((1, 0, 2, ahead), (-1, 4, 5, behind))):
            begun[i].wait_recv()
            mine = w(wrap(c + step, 4))

            @pl.loop(0, 4)
            def _(a):
                hold[i, a] = add(mine.at[half + a], recv.at[i, a]).astype(BF16)

            out_copies.append(send(hold.at[i], recv.at[slot], *sem(4 + i), to))
        return out_copies

    wx_of = lambda c: wx.at[lax.div(c, 2), lax.rem(c, 2)]
    wy_of = lambda c: wy.at[c]

    now = step((1, False, 0), now)
    post(2)
    first[1].wait_recv()
    now = step((2, False, 1), now)
    bx = four_ring(1, x, wx_of, at_x, rx, 0)
    first[2].wait_recv()
    step(None, now)
    by = four_ring(2, y, wy_of, at_y, ry, 6)

    def z_relay(k):
        def hop(chain, recv, hold, d, h, sem, to):
            chain[k - 1].wait_recv()
            hold[k - 1] = add(zpiece(d, h), recv.at[k - 1]).astype(BF16)
            chain.append(send(hold.at[k - 1], recv.at[k], s1.at[sem], r1.at[sem], to))

        hop(zp0, rzp0, szp0, 4 - k, 0, 4 * k, up_z)
        hop(zm1, rzm1, szm1, k - 4, 1, 4 * k + 1, down_z)
        if k < 3:
            hop(zp1, rzp1, szp1, 3 - k, 1, 4 * k + 2, up_z)
            hop(zm0, rzm0, szm0, k - 3, 0, 4 * k + 3, down_z)

    z_relay(1)
    cx = relay(x, wx_of, at_x, rx, sx, 0, bx)
    cy = relay(y, wy_of, at_y, ry, sy, 6, by)
    z_relay(2)
    z_relay(3)

    def settle(c, w, recv, begun, later, store):
        later[0].wait_recv()
        begun[2].wait_recv()
        begun[3].wait_recv()
        later[1].wait_recv()
        mine = w(c)

        @pl.loop(0, 4)
        def _(a):
            store(a, add(mine.at[a], recv.at[2, a], recv.at[4, a]))
            store(4 + a, add(mine.at[4 + a], recv.at[3, a], recv.at[5, a]))

    def store_x(a, v):
        ux[:, a] = v.astype(BF16)

    def store_y(a, v):
        uy[:, :, a] = v.astype(BF16)

    def spread(u, c, n, dev, recv, ss, rs, base):
        return [
            send(u(wrap(c + d, n)), recv.at[d - 1], ss.at[base + d - 1], rs.at[base + d - 1],
                 dev(wrap(c + d, n)))
            for d in range(1, n)
        ]

    ux_of = lambda c: ux.at[c]
    uy_of = lambda c: uy.at[lax.div(c, 2), lax.rem(c, 2)]
    uz_of = lambda c: uz.at[lax.div(c, 2), lax.rem(c, 2)]
    settle(x, wx_of, rx, bx, cx, store_x)
    dx = spread(ux_of, y, NY, at_y, vx, s3, r3, 0)
    settle(y, wy_of, ry, by, cy, store_y)
    dy = spread(uy_of, x, NX, at_x, vy, s3, r3, 3)
    for chain in (zp0, zm0, zp1, zm1):
        chain[-1].wait_recv()
    for h, (a, b) in enumerate(((rzp0.at[3], rzm0.at[2]), (rzp1.at[2], rzm1.at[3]))):
        v = add(zpiece(0, h), a, b)
        for l in range(2):
            uz[h, l] = v[:, l].astype(BF16)
    dz = spread(uz_of, x, NX, at_x, vz, s3, r3, 6)

    def gather(copies, u, c, recv, hold):
        for copy in copies:
            copy.wait_recv()
        hold[...] = add(u(c), *[recv.at[i] for i in range(len(copies))]).astype(BF16)

    gather(dx, ux_of, y, vx, tx)
    ex = spread(lambda c: tx.at[c], z, NZ, at_z, qx, s4, r4, 0)
    gather(dy, uy_of, x, vy, ty)
    ey = spread(lambda c: ty.at[c], z, NZ, at_z, qy, s4, r4, 7)
    gather(dz, uz_of, x, vz, tz)
    ez = spread(lambda c: tz.at[c], y, NY, at_y, qz, s4, r4, 14)

    def finish(j, copies, mine, recv):
        for copy in copies:
            copy.wait_recv()
        total = add(mine, *[recv.at[i] for i in range(len(copies))]) * (1.0 / 16.0)
        res[j, 0] = total[0:8]
        res[j, 1] = total[8:16]

    finish(0, ez, tz.at[y], qz)
    finish(1, ex, tx.at[z], qx)
    finish(2, ey, ty.at[z], qy)
    ends = [
        send(res.at[j, 1 - core], fin.at[j], s0.at[3 + j], r0.at[3 + j], partner) for j in range(3)
    ]
    for j in range(3):
        out[core * 3 + j] = res[j, core]
    for j in range(3):
        ends[j].wait_recv()
        out[(1 - core) * 3 + j] = fin[j]
    for copy in sent:
        copy.wait_send()


def vote_sum(lengths, info, tokens, cotangent, moved, projection, comb, xt):
    vmem = pltpu.VMEM
    t = (16, HS)
    bf = lambda *dims: vmem(dims + t, BF16)
    sems = lambda n: pltpu.SemaphoreType.DMA((n,))
    scratch = [
        vmem((3, BLOCK, D), BF16),
        vmem((3, BLOCK, HEADS * HS), BF16),
        vmem((GROUPS, D, HS), BF16),
        vmem((2 * BLOCK, GROUPS * HS), BF16),
        vmem((D, 2 * BLOCK), BF16),
        vmem((BLOCK, D), BF16),
        vmem((BLOCK, HEADS * HS), BF16),
        vmem((BLOCK, GROUPS * HS), BF16),
        vmem((BLOCK, GROUPS * HS), BF16),
        vmem((D, BLOCK), BF16),
        vmem((2, D, HS), F32),
        bf(3, 8, 2, 4, 2),
        bf(3, 8, 2, 4, 2),
        bf(8, 2, 4, 2),
        bf(2, 2, 8, 4),
        bf(4, 8, 2, 2),
        bf(4, 4, 2), bf(3, 4, 2), bf(3, 4, 2), bf(4, 4, 2),
        bf(3, 4, 2), bf(2, 4, 2), bf(2, 4, 2), bf(3, 4, 2),
        bf(6, 4, 4), bf(2, 4, 4),
        bf(6, 4, 2, 2), bf(2, 4, 2, 2),
        bf(4, 8), bf(2, 2, 8), bf(2, 2, 4),
        bf(3, 8), bf(3, 8), bf(3, 4),
        bf(8), bf(8), bf(4),
        bf(7), bf(7), bf(3),
        vmem((3, 2, 8, HS), F32),
        vmem((3, 8, HS), F32),
        sems(8), sems(6),
        sems(6), sems(6), sems(16), sems(16), sems(12), sems(12), sems(9), sems(9), sems(17), sems(17),
    ]
    return pl.pallas_call(
        vote_kernel,
        out_shape=jax.ShapeDtypeStruct((GROUPS, 8, HS), F32),
        in_specs=[pl.BlockSpec(memory_space=pltpu.SMEM)] * 2
        + [pl.BlockSpec(memory_space=pltpu.HBM)] * 9,
        out_specs=pl.BlockSpec(memory_space=pltpu.VMEM),
        scratch_shapes=scratch,
        compiler_params=pltpu.CompilerParams(
            collective_id=1, has_side_effects=True, vmem_limit_bytes=40 << 20
        ),
        name="vote_sum",
    )(lengths, info, tokens, cotangent, *moved, projection, comb, xt)


LEVELS = 6
PAIRS = [(a, b) for a in range(LEVELS) for b in range(a + 1, LEVELS)]
ALONE = {0: (0, 2), 1: (1, 2), 2: (0, 2), 3: (2, 3), 4: (2, 4), 5: (2, 5)}


def flipped(i, m):
    return i + m - 2 * m * lax.rem(lax.div(i, m), 2)


def across(level):
    if level < 2:
        return {"dp_2": flipped(lax.axis_index("dp_2"), 1 << level)}
    if level == 2:
        return {"dp_1": 1 - lax.axis_index("dp_1")}
    return {"dp_0": flipped(lax.axis_index("dp_0"), 1 << (level - 3))}


def plan_kernel(dest, lengths, tok, cot, proj, info, comb, xt, x01, up01, proj_v, joined, tile,
                from_x, from_y, from_z, loc, psem, ss, rs):
    z, xh, y, xl, core = [lax.axis_index(a) for a in DP_REP]
    x = xh * 2 + xl
    rank = (z * 2 + xh) * 4 + y
    pair = xl * 2 + core

    def at_x(i, c):
        return {"dp_1": lax.div(i, 2), "rep_0": lax.rem(i, 2), "rep_1": c}

    stage_x = [{"rep_1": 1 - core}]
    stage_x += [at_x(wrap(x + d, NX), core) for d in range(1, NX)]
    stage_x += [at_x(wrap(x + d, NX), 1 - core) for d in range(1, NX)]
    stage_y = [{"dp_2": wrap(y + d, NY)} for d in range(1, NY)]
    stage_z = [{"dp_0": wrap(z + d, NZ)} for d in range(1, NZ)]
    peers = stage_x + stage_y + stage_z

    halves = [pl.ds(0, BLOCK), pl.ds(BLOCK, BLOCK)]
    loads = [(tok.at[b], x01.at[halves[b]]) for b in range(2)]
    loads += [(cot.at[b], up01.at[halves[b]]) for b in range(2)]
    loads = [pltpu.make_async_copy(a, b, loc.at[i]) for i, (a, b) in enumerate(loads)]
    for load in loads[:2]:
        load.start()
    for g in range(GROUPS):
        pltpu.make_async_copy(columns(proj, g), proj_v.at[g], psem.at[g]).start()
    for load in loads[2:]:
        load.start()

    barrier = pltpu.get_barrier_semaphore()
    for peer in peers:
        pl.semaphore_signal(barrier, inc=1, device_id=peer, device_id_type=MESH)

    shape = (8, 128)
    slot = lax.broadcasted_iota(jnp.int32, shape, 0) * 128 + lax.broadcasted_iota(jnp.int32, shape, 1)
    target = jnp.full(shape, dest[0], jnp.int32)
    code = jnp.zeros(shape, jnp.int32)
    for level in range(LEVELS):
        code = jnp.where(target == flipped(rank, 1 << level), level + 1, code)
    code = code * 256 + jnp.full(shape, lengths[3], jnp.int32)
    mine = (slot == rank * 4 + pair) & (target >= 0)
    tile[0] = jnp.where(mine, code, 0)

    def before_any():
        for load in loads[:2]:
            load.wait()
        join(0, 3, proj, proj_v, psem, x01, joined)

    def beside_x():
        join(3, GROUPS, proj, proj_v, psem, x01, joined)
        for load in loads[2:]:
            load.wait()

    def beside_y():
        attention(halves[0], lengths[0], joined, up01, comb)

    def beside_z():
        attention(halves[1], lengths[1], joined, up01, comb)
        for r in range(D // 256):
            xt[r * 256 : (r + 1) * 256, :] = x01[:, r * 256 : (r + 1) * 256].T

    beside = (beside_x, beside_y, beside_z)
    before_any()
    pl.semaphore_wait(barrier, len(peers))

    sent = []
    base = 0
    for k, (stage, landing) in enumerate(((stage_x, from_x), (stage_y, from_y), (stage_z, from_z))):
        copies = []
        for i, peer in enumerate(stage):
            copy = pltpu.make_async_remote_copy(
                src_ref=tile.at[k], dst_ref=landing.at[i], send_sem=ss.at[base + i],
                recv_sem=rs.at[base + i], device_id=peer, device_id_type=MESH,
            )
            copy.start()
            copies.append(copy)
        base += len(stage)
        sent += copies
        beside[k]()
        for copy in copies:
            copy.wait_recv()
        table = tile[k]
        for i in range(len(stage)):
            table = jnp.maximum(table, landing[i])
        tile[k + 1] = table

    level_of = lax.shift_right_logical(table, 8).astype(F32)
    length_of = jnp.bitwise_and(table, 255).astype(F32)

    def largest(v):
        return jnp.max(jnp.max(v, axis=1, keepdims=True), axis=0, keepdims=True)

    active = jnp.zeros((1, 1), F32)
    inbound = jnp.zeros((1, 1), F32)
    arriving = jnp.zeros((1, 1), F32)
    for level in range(LEVELS):
        here = level_of == level + 1.0
        active += largest(jnp.where(here, 1.0, 0.0)) * (1 << level)
        mine = here & (slot == flipped(rank, 1 << level) * 4 + pair)
        inbound += largest(jnp.where(mine, level + 1.0, 0.0))
        arriving += largest(jnp.where(mine, length_of, 0.0))
    third = jnp.where(inbound > 0.0, arriving, jnp.full((1, 1), lengths[2], jnp.int32).astype(F32))
    branch = jnp.full((1, 1), float(len(PAIRS)), F32)
    way = jnp.ones((1, 1), F32)
    for p, (a, b) in enumerate(PAIRS):
        sets = [(1 << a) + (1 << b)] + [1 << s for s, both in ALONE.items() if both == (a, b)]
        hit = active == float(sets[0])
        for other in sets[1:] + ([0] if p == 0 else []):
            hit = hit | (active == float(other))
        branch = jnp.where(hit, float(p), branch)
        by = jnp.where(inbound == a + 1.0, 1.0, jnp.where(inbound == b + 1.0, 2.0, 0.0))
        way = jnp.where(hit, by, way)
    row = lax.broadcasted_iota(jnp.int32, shape, 0)
    told = jnp.zeros(shape, F32)
    for i, v in enumerate((branch, way, third, inbound, active)):
        told = jnp.where(row == i, v, told)
    info[...] = told.astype(jnp.int32)
    for copy in sent:
        copy.wait_send()


def plan(destination, lengths, tokens, cotangent, projection):
    vmem = pltpu.VMEM
    t = (8, 128)
    n = 2 * NX - 1 + NY - 1 + NZ - 1
    return pl.pallas_call(
        plan_kernel,
        out_shape=(
            jax.ShapeDtypeStruct(t, jnp.int32),
            jax.ShapeDtypeStruct((2 * BLOCK, GROUPS * HS), BF16),
            jax.ShapeDtypeStruct((D, 2 * BLOCK), BF16),
        ),
        in_specs=[pl.BlockSpec(memory_space=pltpu.SMEM)] * 2
        + [pl.BlockSpec(memory_space=pltpu.HBM)] * 3,
        out_specs=[pl.BlockSpec(memory_space=vmem)] * 3,
        scratch_shapes=[
            vmem((2 * BLOCK, D), BF16),
            vmem((2 * BLOCK, HEADS * HS), BF16),
            vmem((GROUPS, D, HS), BF16),
            vmem((2 * BLOCK, GROUPS * HS), BF16),
            vmem((4,) + t, jnp.int32),
            vmem((2 * NX - 1,) + t, jnp.int32),
            vmem((NY - 1,) + t, jnp.int32),
            vmem((NZ - 1,) + t, jnp.int32),
            pltpu.SemaphoreType.DMA((4,)),
            pltpu.SemaphoreType.DMA((GROUPS,)),
            pltpu.SemaphoreType.DMA((n,)),
            pltpu.SemaphoreType.DMA((n,)),
        ],
        compiler_params=pltpu.CompilerParams(
            collective_id=2, has_side_effects=True, vmem_limit_bytes=30 << 20
        ),
        name="plan",
    )(destination, lengths, tokens, cotangent, projection)


def move_pair(p):
    peers_of = PAIRS[p]

    def kernel(tokens, cotangent, tok_a, cot_a, tok_b, cot_b, ss, rs):
        peers = [across(level) for level in peers_of]
        barrier = pltpu.get_barrier_semaphore()
        for peer in peers:
            pl.semaphore_signal(barrier, inc=1, device_id=peer, device_id_type=MESH)
        pl.semaphore_wait(barrier, 2)
        copies = []
        for i, (src, dst, peer) in enumerate((
            (tokens, tok_a, peers[0]), (tokens, tok_b, peers[1]),
            (cotangent, cot_a, peers[0]), (cotangent, cot_b, peers[1]),
        )):
            copies.append(pltpu.make_async_remote_copy(
                src_ref=src.at[3], dst_ref=dst, send_sem=ss.at[i], recv_sem=rs.at[i],
                device_id=peer, device_id_type=MESH,
            ))
            copies[-1].start()
        for copy in copies:
            copy.wait()

    def call(tokens, cotangent, info):
        block = jax.ShapeDtypeStruct(tokens.shape[1:], BF16)
        upstream = jax.ShapeDtypeStruct(cotangent.shape[1:], BF16)
        return pl.pallas_call(
            kernel,
            out_shape=(block, upstream, block, upstream),
            in_specs=[pl.BlockSpec(memory_space=pl.ANY)] * 2,
            out_specs=[pl.BlockSpec(memory_space=pl.ANY)] * 4,
            scratch_shapes=[pltpu.SemaphoreType.DMA((4,)), pltpu.SemaphoreType.DMA((4,))],
            compiler_params=pltpu.CompilerParams(collective_id=3 + p, has_side_effects=True),
            name="move",
        )(tokens, cotangent)

    return call


def swapped(value, axis, apart):
    mask = 2**apart
    pairs = [(source, source ^ mask) for source in range(lax.axis_size(axis))]
    return lax.ppermute(value, axis, pairs)


def move_many(tokens, cotangent, info):
    kept = (tokens[2], cotangent[2])
    for level in range(LEVELS):

        def trade(kept, level=level):
            got = swapped((tokens[3], cotangent[3]), DP, level)
            arrived = info[3, 0] == level + 1
            return jax.tree.map(lambda new, old: jnp.where(arrived, new, old), got, kept)

        needed = jnp.bitwise_and(jnp.right_shift(info[4, 0], level), 1) == 1
        kept = lax.cond(needed, trade, lambda kept: kept, kept)
    return (*kept, *kept)


def shards(tokens, cotangent, projection, block_lengths, destination):
    lengths = block_lengths[0]
    info, comb, xt = plan(destination, lengths, tokens, cotangent, projection)
    branches = [move_pair(p) for p in range(len(PAIRS))] + [move_many]
    moved = lax.switch(info[0, 0], branches, tokens, cotangent, info)
    summed = vote_sum(lengths, info, tokens, cotangent, moved, projection, comb, xt)
    return summed.transpose(1, 0, 2).reshape(8, GROUPS * HS)


def solution(mesh):
    split = Mesh(mesh.devices.reshape(8, 2, 4, 2, 2), DP_REP)
    placed = (P(DP_REP, None, None), P(DP_REP, None, None), P(), P(DP_REP, None), P(DP_REP))
    return jax.shard_map(
        shards, mesh=split, in_specs=placed, out_specs=P(DP_REP, None), check_vma=False
    )
```

```python
import math

import jax
import jax.numpy as jnp
from jax import lax
from jax.experimental import pallas as pl
from jax.experimental.pallas import tpu as pltpu
from jax.sharding import Mesh
from jax.sharding import PartitionSpec as P

HS = 256
HEADS = 4
BLOCK = 128
DP_REP = ("dp_0", "dp_1", "dp_2", "rep_0", "rep_1")
REP = ("rep_0", "rep_1")
DP = ("dp_0", "dp_1", "dp_2")
GROUPS = HEADS + 2
D = 2048
MESH = pl.DeviceIdType.MESH
F32 = jnp.float32
BF16 = jnp.bfloat16


def dot(a, b, ca, cb):
    return lax.dot_general(a, b, (((ca,), (cb,)), ((), ())), preferred_element_type=F32)


def attention(at, length, joined, up, comb):
    scale = HS ** (-0.5)

    def heads(ref):
        return jnp.concatenate([ref[at, h * HS : (h + 1) * HS] for h in range(HEADS)], axis=0)

    query = heads(joined)
    keys = joined[at, HEADS * HS : (HEADS + 1) * HS]
    values = joined[at, (HEADS + 1) * HS :]
    shape = (HEADS * BLOCK, BLOCK)
    row = lax.rem(lax.broadcasted_iota(jnp.int32, shape, 0), BLOCK)
    col = lax.broadcasted_iota(jnp.int32, shape, 1)
    allowed = (col <= row) & (col < length)
    scores = jnp.where(allowed, dot(query, keys, 1, 1) * scale, -1e30)
    peak = jnp.max(scores, axis=-1, keepdims=True)
    expo = jnp.exp(scores - peak)
    weights = expo / jnp.sum(expo, axis=-1, keepdims=True)
    wide = (HEADS * BLOCK, HS)
    live = lax.rem(lax.broadcasted_iota(jnp.int32, wide, 0), BLOCK) < length
    upstream = jnp.where(live, heads(up).astype(F32), 0.0).astype(BF16)
    probs = weights.astype(BF16)
    grad_values = dot(probs.T, upstream, 1, 0).astype(BF16)
    grad_probs = dot(upstream, values, 1, 1)
    centre = jnp.sum(weights * grad_probs, axis=-1, keepdims=True)
    grad_scores = (weights * (grad_probs - centre) * scale).astype(BF16)
    grad_query = dot(grad_scores, keys, 1, 0).astype(BF16)
    grad_keys = dot(grad_scores.T, query, 1, 0).astype(BF16)
    for h in range(HEADS):
        comb[at, h * HS : (h + 1) * HS] = grad_query[h * BLOCK : (h + 1) * BLOCK]
    comb[at, HEADS * HS : (HEADS + 1) * HS] = grad_keys
    comb[at, (HEADS + 1) * HS :] = grad_values


SLABS = 4
SLAB = D // SLABS


def slab_copy(proj, proj_v, sem, k):
    at = pl.ds(k * SLAB, SLAB)
    return pltpu.make_async_copy(proj.at[at], proj_v.at[at], sem.at[k])


def join(proj, proj_v, sem, x, acc, joined):
    for k in range(SLABS):
        slab_copy(proj, proj_v, sem, k).wait()
        at = slice(k * SLAB, (k + 1) * SLAB)
        part = dot(x[:, at], proj_v[at, :], 1, 0)
        if k == SLABS - 1:
            joined[...] = (acc[...] + part).astype(BF16)
        elif k:
            acc[...] += part
        else:
            acc[...] = part


NZ, NY, NX = 8, 4, 4


def wrap(i, n):
    return lax.rem(i + n, n)


def vote_kernel(lengths, info, tok, cot, tok_a, cot_a, tok_b, cot_b, proj, comb_hbm, xt_hbm, out,
                cand_t, cand_c, proj_v, comb01, xt01, x3, up3, acc3, joined3, comb3, xt3, grad, mail,
                part, wz, wx, wy, rzp0, rzp1, rzm0, rzm1, szp0, szp1, szm0,
                szm1, rx, sx, ry, sy, ux, uy, uz, vx, vy, vz, tx, ty, tz, qx, qy, qz, res, fin,
                loc, psem, s0, r0, s1, r1, s2, r2, s3, r3, s4, r4):
    z, xh, y, xl, core = [lax.axis_index(a) for a in DP_REP]
    x = xh * 2 + xl

    def at_x(i):
        return {"dp_1": lax.div(i, 2), "rep_0": lax.rem(i, 2)}

    def at_y(i):
        return {"dp_2": i}

    def at_z(i):
        return {"dp_0": i}

    partner = {"rep_1": 1 - core}

    loads = [(tok.at[2], cand_t.at[0]), (tok_a, cand_t.at[1]), (tok_b, cand_t.at[2])]
    loads += [(cot.at[2], cand_c.at[0]), (cot_a, cand_c.at[1]), (cot_b, cand_c.at[2])]
    loads += [(comb_hbm, comb01), (xt_hbm, xt01)]
    loads = [pltpu.make_async_copy(a, b, loc.at[i]) for i, (a, b) in enumerate(loads)]
    for load in loads[:3]:
        load.start()
    for k in range(SLABS):
        slab_copy(proj, proj_v, psem, k).start()
    for load in loads[3:]:
        load.start()

    barrier = pltpu.get_barrier_semaphore()
    peers = [partner]
    peers += [at_x(wrap(x + d, NX)) for d in range(1, NX)]
    peers += [at_y(wrap(y + d, NY)) for d in range(1, NY)]
    peers += [at_z(wrap(z + d, NZ)) for d in range(1, NZ)]
    for peer in peers:
        pl.semaphore_signal(barrier, inc=1, device_id=peer, device_id_type=MESH)

    sent = []

    def send(src, dst, ss, rs, dev):
        copy = pltpu.make_async_remote_copy(
            src_ref=src, dst_ref=dst, send_sem=ss, recv_sem=rs, device_id=dev, device_id_type=MESH
        )
        copy.start()
        sent.append(copy)
        return copy

    def add(*refs):
        total = refs[0][...].astype(F32)
        for ref in refs[1:]:
            total = total + ref[...].astype(F32)
        return total

    way = info[1, 0]

    def chosen(c):
        return jnp.where(way == 1, c[1], jnp.where(way == 2, c[2], c[0]))

    for load in loads[:3]:
        load.wait()
    x3[...] = chosen(cand_t)
    for r in range(D // 512):
        xt3[r * 512 : (r + 1) * 512, :] = x3[:, r * 512 : (r + 1) * 512].T
    join(proj, proj_v, psem, x3, acc3, joined3)
    for load in loads[3:]:
        load.wait()
    up3[...] = chosen(cand_c)
    attention(slice(None), info[2, 0], joined3, up3, comb3)
    pl.semaphore_wait(barrier, len(peers))

    tile, chunk = 128, 512
    other = 1 - core

    def step(begin, end):
        if begin is not None:
            j, to_partner, buf = begin
            cols = pl.ds(pl.multiple_of(((other if to_partner else core) * 3 + j) * HS, HS), HS)

        total = jnp.zeros((8, HS), F32)
        for q in range(D // chunk):
            if begin is not None:
                at = pl.ds(q * chunk, chunk)
                new = dot(xt01[at, :], comb01[:, cols], 1, 0)
                new = new + dot(xt3[at, :], comb3[:, cols], 1, 0)
                grad[buf, at, :] = new
                total = total + jnp.sum((new * new).reshape(chunk // 8, 8, HS), axis=0)
            if end is None:
                continue
            for t in range(chunk // tile):
                a, h = divmod(q * (chunk // tile) + t, 2)
                old = grad[end[2], pl.ds(a * 256 + h * tile, tile), :]
                soft = (old / (jnp.abs(old) + end[3])).reshape(NY, 2, 16, HS)
                if end[1]:
                    mail[end[0], a, h] = soft.astype(BF16)
                    continue
                both = (soft + part[end[0], a, h].astype(F32)).astype(BF16)
                if end[0] == 0:
                    wz[a, h] = both
                elif end[0] == 1:
                    for l in range(2):
                        wx[h, l, a] = both[:, l]
                else:
                    for b in range(NY):
                        wy[b, a, h] = both[b]
        if begin is None:
            return None
        total = jnp.sum(jnp.sum(total, axis=0, keepdims=True), axis=1, keepdims=True)
        return (*begin, 0.25 * jnp.sqrt(total * (1.0 / (D * HS)) + 1e-06))

    first = {}

    def post(j):
        first[j] = send(mail.at[j], part.at[j], s0.at[j], r0.at[j], partner)

    now = step((0, True, 0), None)
    now = step((1, True, 1), now)
    post(0)
    now = step((2, True, 0), now)
    post(1)
    now = step((0, False, 1), now)
    post(2)
    first[0].wait_recv()
    now = step((1, False, 0), now)

    up_z, down_z = at_z(wrap(z + 1, NZ)), at_z(wrap(z - 1, NZ))

    def zpiece(d, h):
        return wz.at[wrap(z + d, NZ), h]

    zp0 = [send(zpiece(4, 0), rzp0.at[0], s1.at[0], r1.at[0], up_z)]
    zm1 = [send(zpiece(-4, 1), rzm1.at[0], s1.at[1], r1.at[1], down_z)]
    zp1 = [send(zpiece(3, 1), rzp1.at[0], s1.at[2], r1.at[2], up_z)]
    zm0 = [send(zpiece(-3, 0), rzm0.at[0], s1.at[3], r1.at[3], down_z)]

    def four_ring(j, c, w, dev, recv, base):
        ahead, behind = dev(wrap(c + 1, 4)), dev(wrap(c - 1, 4))
        far = wrap(c + 2, 4)
        lo, hi = pl.ds(0, 4), pl.ds(4, 4)
        sem = lambda i: (s2.at[base + i], r2.at[base + i])
        return [
            send(w(far).at[lo], recv.at[0], *sem(0), ahead),
            send(w(far).at[hi], recv.at[1], *sem(1), behind),
            send(w(wrap(c + 1, 4)).at[hi], recv.at[3], *sem(2), ahead),
            send(w(wrap(c - 1, 4)).at[lo], recv.at[4], *sem(3), behind),
        ]

    def relay(c, w, dev, recv, hold, base, begun):
        ahead, behind = dev(wrap(c + 1, 4)), dev(wrap(c - 1, 4))
        sem = lambda i: (s2.at[base + i], r2.at[base + i])
        out_copies = []
        for i, (step, half, slot, to) in enumerate(((1, 0, 2, ahead), (-1, 4, 5, behind))):
            begun[i].wait_recv()
            mine = w(wrap(c + step, 4))

            @pl.loop(0, 4)
            def _(a):
                hold[i, a] = add(mine.at[half + a], recv.at[i, a]).astype(BF16)

            out_copies.append(send(hold.at[i], recv.at[slot], *sem(4 + i), to))
        return out_copies

    wx_of = lambda c: wx.at[lax.div(c, 2), lax.rem(c, 2)]
    wy_of = lambda c: wy.at[c]

    first[1].wait_recv()
    now = step((2, False, 1), now)
    bx = four_ring(1, x, wx_of, at_x, rx, 0)
    first[2].wait_recv()
    step(None, now)
    by = four_ring(2, y, wy_of, at_y, ry, 6)

    def z_relay(k):
        def hop(chain, recv, hold, d, h, sem, to):
            chain[k - 1].wait_recv()
            hold[k - 1] = add(zpiece(d, h), recv.at[k - 1]).astype(BF16)
            chain.append(send(hold.at[k - 1], recv.at[k], s1.at[sem], r1.at[sem], to))

        hop(zp0, rzp0, szp0, 4 - k, 0, 4 * k, up_z)
        hop(zm1, rzm1, szm1, k - 4, 1, 4 * k + 1, down_z)
        if k < 3:
            hop(zp1, rzp1, szp1, 3 - k, 1, 4 * k + 2, up_z)
            hop(zm0, rzm0, szm0, k - 3, 0, 4 * k + 3, down_z)

    z_relay(1)
    cx = relay(x, wx_of, at_x, rx, sx, 0, bx)
    cy = relay(y, wy_of, at_y, ry, sy, 6, by)
    z_relay(2)
    z_relay(3)

    def settle(c, w, recv, begun, later, store):
        later[0].wait_recv()
        begun[2].wait_recv()
        begun[3].wait_recv()
        later[1].wait_recv()
        mine = w(c)

        @pl.loop(0, 4)
        def _(a):
            store(a, add(mine.at[a], recv.at[2, a], recv.at[4, a]))
            store(4 + a, add(mine.at[4 + a], recv.at[3, a], recv.at[5, a]))

    def store_x(a, v):
        ux[:, a] = v.astype(BF16)

    def store_y(a, v):
        uy[:, :, a] = v.astype(BF16)

    def spread(u, c, n, dev, recv, ss, rs, base):
        return [
            send(u(wrap(c + d, n)), recv.at[d - 1], ss.at[base + d - 1], rs.at[base + d - 1],
                 dev(wrap(c + d, n)))
            for d in range(1, n)
        ]

    ux_of = lambda c: ux.at[c]
    uy_of = lambda c: uy.at[lax.div(c, 2), lax.rem(c, 2)]
    uz_of = lambda c: uz.at[lax.div(c, 2), lax.rem(c, 2)]
    settle(x, wx_of, rx, bx, cx, store_x)
    dx = spread(ux_of, y, NY, at_y, vx, s3, r3, 0)
    settle(y, wy_of, ry, by, cy, store_y)
    dy = spread(uy_of, x, NX, at_x, vy, s3, r3, 3)
    for chain in (zp0, zm0, zp1, zm1):
        chain[-1].wait_recv()
    for h, (a, b) in enumerate(((rzp0.at[3], rzm0.at[2]), (rzp1.at[2], rzm1.at[3]))):
        v = add(zpiece(0, h), a, b)
        for l in range(2):
            uz[h, l] = v[:, l].astype(BF16)
    dz = spread(uz_of, x, NX, at_x, vz, s3, r3, 6)

    def gather(copies, u, c, recv, hold):
        for copy in copies:
            copy.wait_recv()
        hold[...] = add(u(c), *[recv.at[i] for i in range(len(copies))]).astype(BF16)

    gather(dx, ux_of, y, vx, tx)
    ex = spread(lambda c: tx.at[c], z, NZ, at_z, qx, s4, r4, 0)
    gather(dy, uy_of, x, vy, ty)
    ey = spread(lambda c: ty.at[c], z, NZ, at_z, qy, s4, r4, 7)
    gather(dz, uz_of, x, vz, tz)
    ez = spread(lambda c: tz.at[c], y, NY, at_y, qz, s4, r4, 14)

    def finish(j, copies, mine, recv):
        for copy in copies:
            copy.wait_recv()
        total = add(mine, *[recv.at[i] for i in range(len(copies))]) * (1.0 / 16.0)
        res[j, 0] = total[0:8]
        res[j, 1] = total[8:16]

    finish(0, ez, tz.at[y], qz)
    finish(1, ex, tx.at[z], qx)
    finish(2, ey, ty.at[z], qy)
    ends = [
        send(res.at[j, 1 - core], fin.at[j], s0.at[3 + j], r0.at[3 + j], partner) for j in range(3)
    ]
    for j in range(3):
        out[core * 3 + j] = res[j, core]
    for j in range(3):
        ends[j].wait_recv()
        out[(1 - core) * 3 + j] = fin[j]
    for copy in sent:
        copy.wait_send()


def vote_sum(lengths, info, tokens, cotangent, moved, projection, comb, xt):
    vmem = pltpu.VMEM
    t = (16, HS)
    bf = lambda *dims: vmem(dims + t, BF16)
    sems = lambda n: pltpu.SemaphoreType.DMA((n,))
    scratch = [
        vmem((3, BLOCK, D), BF16),
        vmem((3, BLOCK, HEADS * HS), BF16),
        vmem((D, GROUPS * HS), BF16),
        vmem((2 * BLOCK, GROUPS * HS), BF16),
        vmem((D, 2 * BLOCK), BF16),
        vmem((BLOCK, D), BF16),
        vmem((BLOCK, HEADS * HS), BF16),
        vmem((BLOCK, GROUPS * HS), F32),
        vmem((BLOCK, GROUPS * HS), BF16),
        vmem((BLOCK, GROUPS * HS), BF16),
        vmem((D, BLOCK), BF16),
        vmem((2, D, HS), F32),
        bf(3, 8, 2, 4, 2),
        bf(3, 8, 2, 4, 2),
        bf(8, 2, 4, 2),
        bf(2, 2, 8, 4),
        bf(4, 8, 2, 2),
        bf(4, 4, 2), bf(3, 4, 2), bf(3, 4, 2), bf(4, 4, 2),
        bf(3, 4, 2), bf(2, 4, 2), bf(2, 4, 2), bf(3, 4, 2),
        bf(6, 4, 4), bf(2, 4, 4),
        bf(6, 4, 2, 2), bf(2, 4, 2, 2),
        bf(4, 8), bf(2, 2, 8), bf(2, 2, 4),
        bf(3, 8), bf(3, 8), bf(3, 4),
        bf(8), bf(8), bf(4),
        bf(7), bf(7), bf(3),
        vmem((3, 2, 8, HS), F32),
        vmem((3, 8, HS), F32),
        sems(8), sems(SLABS),
        sems(6), sems(6), sems(16), sems(16), sems(12), sems(12), sems(9), sems(9), sems(17), sems(17),
    ]
    return pl.pallas_call(
        vote_kernel,
        out_shape=jax.ShapeDtypeStruct((GROUPS, 8, HS), F32),
        in_specs=[pl.BlockSpec(memory_space=pltpu.SMEM)] * 2
        + [pl.BlockSpec(memory_space=pltpu.HBM)] * 9,
        out_specs=pl.BlockSpec(memory_space=pltpu.VMEM),
        scratch_shapes=scratch,
        compiler_params=pltpu.CompilerParams(
            collective_id=1, has_side_effects=True, vmem_limit_bytes=60 << 20
        ),
        name="vote_sum",
    )(lengths, info, tokens, cotangent, *moved, projection, comb, xt)


LEVELS = 6
PAIRS = [(a, b) for a in range(LEVELS) for b in range(a + 1, LEVELS)]
ALONE = {0: (0, 2), 1: (1, 2), 2: (0, 2), 3: (2, 3), 4: (2, 4), 5: (2, 5)}


def flipped(i, m):
    return i + m - 2 * m * lax.rem(lax.div(i, m), 2)


def across(level):
    if level < 2:
        return {"dp_2": flipped(lax.axis_index("dp_2"), 1 << level)}
    if level == 2:
        return {"dp_1": 1 - lax.axis_index("dp_1")}
    return {"dp_0": flipped(lax.axis_index("dp_0"), 1 << (level - 3))}


def plan_kernel(dest, lengths, tok, cot, proj, info, comb, xt, x01, up01, proj_v, acc, joined,
                mine, mixed, from_plane, from_z, loc, psem, ss, rs):
    z, xh, y, xl, core = [lax.axis_index(a) for a in DP_REP]
    x = xh * 2 + xl

    def at_plane(dx, dy, c):
        i = wrap(x + dx, NX)
        return {"dp_1": lax.div(i, 2), "rep_0": lax.rem(i, 2), "dp_2": wrap(y + dy, NY), "rep_1": c}

    plane = [(dx, dy, c) for dx in range(NX) for dy in range(NY) for c in range(2)][1:]
    plane = [at_plane(dx, dy, 1 - core if c else core) for dx, dy, c in plane]
    column = [{"dp_0": wrap(z + d, NZ)} for d in range(1, NZ)]
    peers = plane + column

    halves = [pl.ds(0, BLOCK), pl.ds(BLOCK, BLOCK)]
    loads = [(tok.at[b], x01.at[halves[b]]) for b in range(2)]
    loads += [(cot.at[b], up01.at[halves[b]]) for b in range(2)]
    loads = [pltpu.make_async_copy(a, b, loc.at[i]) for i, (a, b) in enumerate(loads)]
    for load in loads[:2]:
        load.start()
    for k in range(SLABS):
        slab_copy(proj, proj_v, psem, k).start()
    for load in loads[2:]:
        load.start()

    barrier = pltpu.get_barrier_semaphore()
    for peer in peers:
        pl.semaphore_signal(barrier, inc=1, device_id=peer, device_id_type=MESH)

    here = (xh * NY + y) * 4 + xl * 2 + core
    rank = z * 8 + xh * NY + y
    wide = (1, 128)
    lane = lax.broadcasted_iota(jnp.int32, wide, 1)
    target = jnp.full(wide, dest[0], jnp.int32)
    code = jnp.zeros(wide, jnp.int32)
    for level in range(LEVELS):
        code = jnp.where(target == flipped(rank, 1 << level), level + 1, code)
    code = code * 256 + jnp.full(wide, lengths[3], jnp.int32)
    mine[...] = jnp.where((lane == here) & (target >= 0), code, 0)

    for load in loads[:2]:
        load.wait()

    def spread(src, stage, landing, base):
        copies = []
        for i, peer in enumerate(stage):
            copy = pltpu.make_async_remote_copy(
                src_ref=src, dst_ref=landing.at[i], send_sem=ss.at[base + i],
                recv_sem=rs.at[base + i], device_id=peer, device_id_type=MESH,
            )
            copy.start()
            copies.append(copy)
        return copies

    pl.semaphore_wait(barrier, len(peers))
    first = spread(mine, plane, from_plane, 0)
    join(proj, proj_v, psem, x01, acc, joined)
    for load in loads[2:]:
        load.wait()
    for copy in first:
        copy.wait_recv()
    row = mine[...]
    for i in range(len(plane)):
        row = jnp.maximum(row, from_plane[i])
    mixed[...] = row
    second = spread(mixed, column, from_z, len(plane))
    for b in range(2):
        attention(halves[b], lengths[b], joined, up01, comb)
    for r in range(D // 512):
        xt[r * 512 : (r + 1) * 512, :] = x01[:, r * 512 : (r + 1) * 512].T
    for copy in second:
        copy.wait_recv()

    shape = (8, 128)
    behind = lax.broadcasted_iota(jnp.int32, shape, 0)
    lane = lax.broadcasted_iota(jnp.int32, shape, 1)
    table = jnp.broadcast_to(mixed[...], shape)
    for k in range(1, NZ):
        table = jnp.where(behind == k, jnp.broadcast_to(from_z[k - 1], shape), table)
    level_of = lax.shift_right_logical(table, 8)

    def largest(v):
        v = v.astype(F32)
        return jnp.max(jnp.max(v, axis=1, keepdims=True), axis=0, keepdims=True)

    active = jnp.zeros((1, 1), F32)
    sender = jnp.zeros(shape, jnp.int32)
    for level in range(LEVELS):
        found = level_of == level + 1
        active += largest(jnp.where(found, 1 << level, 0))
        if level < 2:
            there, back = here + (flipped(y, 1 << level) - y) * 4, z * 0
        elif level == 2:
            there, back = here + (1 - 2 * xh) * NY * 4, z * 0
        else:
            there, back = here, wrap(z - flipped(z, 1 << (level - 3)), NZ)
        sender = jnp.where(found & (lane == there) & (behind == back), table, sender)
    inbound = largest(lax.shift_right_logical(sender, 8))
    arriving = largest(jnp.bitwise_and(sender, 255))
    third = jnp.where(inbound > 0.0, arriving, jnp.full((1, 1), lengths[2], jnp.int32).astype(F32))
    branch = jnp.full((1, 1), float(len(PAIRS)), F32)
    way = jnp.ones((1, 1), F32)
    for p, (a, b) in enumerate(PAIRS):
        sets = [(1 << a) + (1 << b)] + [1 << s for s, both in ALONE.items() if both == (a, b)]
        hit = active == float(sets[0])
        for other in sets[1:] + ([0] if p == 0 else []):
            hit = hit | (active == float(other))
        branch = jnp.where(hit, float(p), branch)
        by = jnp.where(inbound == a + 1.0, 1.0, jnp.where(inbound == b + 1.0, 2.0, 0.0))
        way = jnp.where(hit, by, way)
    told = jnp.zeros(shape, F32)
    for i, v in enumerate((branch, way, third, inbound, active)):
        told = jnp.where(behind == i, v, told)
    info[...] = told.astype(jnp.int32)
    for copy in first + second:
        copy.wait_send()


def plan(destination, lengths, tokens, cotangent, projection):
    vmem = pltpu.VMEM
    plane, column = 2 * NX * NY - 1, NZ - 1
    width = GROUPS * HS
    return pl.pallas_call(
        plan_kernel,
        out_shape=(
            jax.ShapeDtypeStruct((8, 128), jnp.int32),
            jax.ShapeDtypeStruct((2 * BLOCK, width), BF16),
            jax.ShapeDtypeStruct((D, 2 * BLOCK), BF16),
        ),
        in_specs=[pl.BlockSpec(memory_space=pltpu.SMEM)] * 2
        + [pl.BlockSpec(memory_space=pltpu.HBM)] * 3,
        out_specs=[pl.BlockSpec(memory_space=vmem)] * 3,
        scratch_shapes=[
            vmem((2 * BLOCK, D), BF16),
            vmem((2 * BLOCK, HEADS * HS), BF16),
            vmem((D, width), BF16),
            vmem((2 * BLOCK, width), F32),
            vmem((2 * BLOCK, width), BF16),
            vmem((1, 128), jnp.int32),
            vmem((1, 128), jnp.int32),
            vmem((plane, 1, 128), jnp.int32),
            vmem((column, 1, 128), jnp.int32),
            pltpu.SemaphoreType.DMA((4,)),
            pltpu.SemaphoreType.DMA((SLABS,)),
            pltpu.SemaphoreType.DMA((plane + column,)),
            pltpu.SemaphoreType.DMA((plane + column,)),
        ],
        compiler_params=pltpu.CompilerParams(
            collective_id=2, has_side_effects=True, vmem_limit_bytes=60 << 20
        ),
        name="plan",
    )(destination, lengths, tokens, cotangent, projection)


def move_pair(p):
    peers_of = PAIRS[p]

    def kernel(tokens, cotangent, tok_a, cot_a, tok_b, cot_b, ss, rs):
        peers = [across(level) for level in peers_of]
        barrier = pltpu.get_barrier_semaphore()
        for peer in peers:
            pl.semaphore_signal(barrier, inc=1, device_id=peer, device_id_type=MESH)
        pl.semaphore_wait(barrier, 2)
        copies = []
        for i, (src, dst, peer) in enumerate((
            (tokens, tok_a, peers[0]), (tokens, tok_b, peers[1]),
            (cotangent, cot_a, peers[0]), (cotangent, cot_b, peers[1]),
        )):
            copies.append(pltpu.make_async_remote_copy(
                src_ref=src.at[3], dst_ref=dst, send_sem=ss.at[i], recv_sem=rs.at[i],
                device_id=peer, device_id_type=MESH,
            ))
            copies[-1].start()
        for copy in copies:
            copy.wait()

    def call(tokens, cotangent, info):
        block = jax.ShapeDtypeStruct(tokens.shape[1:], BF16)
        upstream = jax.ShapeDtypeStruct(cotangent.shape[1:], BF16)
        return pl.pallas_call(
            kernel,
            out_shape=(block, upstream, block, upstream),
            in_specs=[pl.BlockSpec(memory_space=pl.ANY)] * 2,
            out_specs=[pl.BlockSpec(memory_space=pl.ANY)] * 4,
            scratch_shapes=[pltpu.SemaphoreType.DMA((4,)), pltpu.SemaphoreType.DMA((4,))],
            compiler_params=pltpu.CompilerParams(collective_id=3 + p, has_side_effects=True),
            name="move",
        )(tokens, cotangent)

    return call


def swapped(value, axis, apart):
    mask = 2**apart
    pairs = [(source, source ^ mask) for source in range(lax.axis_size(axis))]
    return lax.ppermute(value, axis, pairs)


def move_many(tokens, cotangent, info):
    kept = (tokens[2], cotangent[2])
    for level in range(LEVELS):

        def trade(kept, level=level):
            got = swapped((tokens[3], cotangent[3]), DP, level)
            arrived = info[3, 0] == level + 1
            return jax.tree.map(lambda new, old: jnp.where(arrived, new, old), got, kept)

        needed = jnp.bitwise_and(jnp.right_shift(info[4, 0], level), 1) == 1
        kept = lax.cond(needed, trade, lambda kept: kept, kept)
    return (*kept, *kept)


def shards(tokens, cotangent, projection, block_lengths, destination):
    lengths = block_lengths[0]
    info, comb, xt = plan(destination, lengths, tokens, cotangent, projection)
    branches = [move_pair(p) for p in range(len(PAIRS))] + [move_many]
    moved = lax.switch(info[0, 0], branches, tokens, cotangent, info)
    summed = vote_sum(lengths, info, tokens, cotangent, moved, projection, comb, xt)
    return summed.transpose(1, 0, 2).reshape(8, GROUPS * HS)


def solution(mesh):
    split = Mesh(mesh.devices.reshape(8, 2, 4, 2, 2), DP_REP)
    placed = (P(DP_REP, None, None), P(DP_REP, None, None), P(), P(DP_REP, None), P(DP_REP))
    return jax.shard_map(
        shards, mesh=split, in_specs=placed, out_specs=P(DP_REP, None), check_vma=False
    )
```

```python
import math

import jax
import jax.numpy as jnp
from jax import lax
from jax.experimental import pallas as pl
from jax.experimental.pallas import tpu as pltpu
from jax.sharding import Mesh
from jax.sharding import PartitionSpec as P

HS = 256
HEADS = 4
BLOCK = 128
DP_REP = ("dp_0", "dp_1", "dp_2", "rep_0", "rep_1")
REP = ("rep_0", "rep_1")
DP = ("dp_0", "dp_1", "dp_2")
GROUPS = HEADS + 2
D = 2048
MESH = pl.DeviceIdType.MESH
F32 = jnp.float32
BF16 = jnp.bfloat16


def dot(a, b, ca, cb):
    return lax.dot_general(a, b, (((ca,), (cb,)), ((), ())), preferred_element_type=F32)


def attention(at, length, joined, up, comb):
    scale = HS ** (-0.5)

    def heads(ref):
        return jnp.concatenate([ref[at, h * HS : (h + 1) * HS] for h in range(HEADS)], axis=0)

    query = heads(joined)
    keys = joined[at, HEADS * HS : (HEADS + 1) * HS]
    values = joined[at, (HEADS + 1) * HS :]
    shape = (HEADS * BLOCK, BLOCK)
    row = lax.rem(lax.broadcasted_iota(jnp.int32, shape, 0), BLOCK)
    col = lax.broadcasted_iota(jnp.int32, shape, 1)
    allowed = (col <= row) & (col < jnp.broadcast_to(length, shape))
    scores = jnp.where(allowed, dot(query, keys, 1, 1) * scale, -1e30)
    peak = jnp.max(scores, axis=-1, keepdims=True)
    expo = jnp.exp(scores - peak)
    weights = expo / jnp.sum(expo, axis=-1, keepdims=True)
    wide = (HEADS * BLOCK, HS)
    live = lax.rem(lax.broadcasted_iota(jnp.int32, wide, 0), BLOCK) < jnp.broadcast_to(length, wide)
    upstream = jnp.where(live, heads(up).astype(F32), 0.0).astype(BF16)
    probs = weights.astype(BF16)
    grad_values = dot(probs.T, upstream, 1, 0).astype(BF16)
    grad_probs = dot(upstream, values, 1, 1)
    centre = jnp.sum(weights * grad_probs, axis=-1, keepdims=True)
    grad_scores = (weights * (grad_probs - centre) * scale).astype(BF16)
    grad_query = dot(grad_scores, keys, 1, 0).astype(BF16)
    grad_keys = dot(grad_scores.T, query, 1, 0).astype(BF16)
    for h in range(HEADS):
        comb[at, h * HS : (h + 1) * HS] = grad_query[h * BLOCK : (h + 1) * BLOCK]
    comb[at, HEADS * HS : (HEADS + 1) * HS] = grad_keys
    comb[at, (HEADS + 1) * HS :] = grad_values


SLABS = 4
SLAB = D // SLABS


def slab_copy(proj, proj_v, sem, k):
    at = pl.ds(k * SLAB, SLAB)
    return pltpu.make_async_copy(proj.at[at], proj_v.at[at], sem.at[k])


def join(proj, proj_v, sem, x, acc, joined):
    for k in range(SLABS):
        slab_copy(proj, proj_v, sem, k).wait()
        at = slice(k * SLAB, (k + 1) * SLAB)
        part = dot(x[:, at], proj_v[at, :], 1, 0)
        if k == SLABS - 1:
            joined[...] = (acc[...] + part).astype(BF16)
        elif k:
            acc[...] += part
        else:
            acc[...] = part


NZ, NY, NX = 8, 4, 4


def wrap(i, n):
    return lax.rem(i + n, n)


def vote_kernel(info, tok, cot, tok_a, cot_a, tok_b, cot_b, proj, comb01, xt01, out,
                cand_t, cand_c, proj_v, x3, up3, acc3, joined3, comb3, xt3, grad, mail,
                part, wz, wx, wy, rzp0, rzp1, rzm0, rzm1, szp0, szp1, szm0,
                szm1, rx, sx, ry, sy, ux, uy, uz, vx, vy, vz, tx, ty, tz, qx, qy, qz, res, fin,
                loc, psem, s0, r0, s1, r1, s2, r2, s3, r3, s4, r4):
    z, xh, y, xl, core = [lax.axis_index(a) for a in DP_REP]
    x = xh * 2 + xl

    def at_x(i):
        return {"dp_1": lax.div(i, 2), "rep_0": lax.rem(i, 2)}

    def at_y(i):
        return {"dp_2": i}

    def at_z(i):
        return {"dp_0": i}

    partner = {"rep_1": 1 - core}

    loads = [(tok.at[2], cand_t.at[0]), (tok_a, cand_t.at[1]), (tok_b, cand_t.at[2])]
    loads += [(cot.at[2], cand_c.at[0]), (cot_a, cand_c.at[1]), (cot_b, cand_c.at[2])]
    loads = [pltpu.make_async_copy(a, b, loc.at[i]) for i, (a, b) in enumerate(loads)]
    for load in loads[:3]:
        load.start()
    for k in range(SLABS):
        slab_copy(proj, proj_v, psem, k).start()
    for load in loads[3:]:
        load.start()

    barrier = pltpu.get_barrier_semaphore()
    peers = [partner]
    peers += [at_x(wrap(x + d, NX)) for d in range(1, NX)]
    peers += [at_y(wrap(y + d, NY)) for d in range(1, NY)]
    peers += [at_z(wrap(z + d, NZ)) for d in range(1, NZ)]
    for peer in peers:
        pl.semaphore_signal(barrier, inc=1, device_id=peer, device_id_type=MESH)

    sent = []

    def send(src, dst, ss, rs, dev):
        copy = pltpu.make_async_remote_copy(
            src_ref=src, dst_ref=dst, send_sem=ss, recv_sem=rs, device_id=dev, device_id_type=MESH
        )
        copy.start()
        sent.append(copy)
        return copy

    def add(*refs):
        total = refs[0][...].astype(F32)
        for ref in refs[1:]:
            total = total + ref[...].astype(F32)
        return total

    def chosen(c):
        way = jnp.broadcast_to(info[1:2, 0:1], c.shape[1:])
        return jnp.where(way == 1, c[1], jnp.where(way == 2, c[2], c[0]))

    for load in loads[:3]:
        load.wait()
    x3[...] = chosen(cand_t)
    for r in range(D // 512):
        xt3[r * 512 : (r + 1) * 512, :] = x3[:, r * 512 : (r + 1) * 512].T
    join(proj, proj_v, psem, x3, acc3, joined3)
    for load in loads[3:]:
        load.wait()
    up3[...] = chosen(cand_c)
    attention(slice(None), info[2:3, 0:1], joined3, up3, comb3)
    pl.semaphore_wait(barrier, len(peers))

    tile, chunk = 128, 512
    other = 1 - core

    def step(begin, end):
        if begin is not None:
            j, to_partner, buf = begin
            cols = pl.ds(pl.multiple_of(((other if to_partner else core) * 3 + j) * HS, HS), HS)

        total = jnp.zeros((8, HS), F32)
        for q in range(D // chunk):
            if begin is not None:
                at = pl.ds(q * chunk, chunk)
                new = dot(xt01[at, :], comb01[:, cols], 1, 0)
                new = new + dot(xt3[at, :], comb3[:, cols], 1, 0)
                grad[buf, at, :] = new
                total = total + jnp.sum((new * new).reshape(chunk // 8, 8, HS), axis=0)
            if end is None:
                continue
            for t in range(chunk // tile):
                a, h = divmod(q * (chunk // tile) + t, 2)
                old = grad[end[2], pl.ds(a * 256 + h * tile, tile), :]
                soft = (old / (jnp.abs(old) + end[3])).reshape(NY, 2, 16, HS)
                if end[1]:
                    mail[end[0], a, h] = soft.astype(BF16)
                    continue
                both = (soft + part[end[0], a, h].astype(F32)).astype(BF16)
                if end[0] == 0:
                    wz[a, h] = both
                elif end[0] == 1:
                    for l in range(2):
                        wx[h, l, a] = both[:, l]
                else:
                    for b in range(NY):
                        wy[b, a, h] = both[b]
        if begin is None:
            return None
        total = jnp.sum(jnp.sum(total, axis=0, keepdims=True), axis=1, keepdims=True)
        return (*begin, 0.25 * jnp.sqrt(total * (1.0 / (D * HS)) + 1e-06))

    first = {}

    def post(j):
        first[j] = send(mail.at[j], part.at[j], s0.at[j], r0.at[j], partner)

    now = step((0, True, 0), None)
    now = step((1, True, 1), now)
    post(0)
    now = step((2, True, 0), now)
    post(1)
    now = step((0, False, 1), now)
    post(2)
    first[0].wait_recv()
    now = step((1, False, 0), now)

    up_z, down_z = at_z(wrap(z + 1, NZ)), at_z(wrap(z - 1, NZ))

    def zpiece(d, h):
        return wz.at[wrap(z + d, NZ), h]

    zp0 = [send(zpiece(4, 0), rzp0.at[0], s1.at[0], r1.at[0], up_z)]
    zm1 = [send(zpiece(-4, 1), rzm1.at[0], s1.at[1], r1.at[1], down_z)]
    zp1 = [send(zpiece(3, 1), rzp1.at[0], s1.at[2], r1.at[2], up_z)]
    zm0 = [send(zpiece(-3, 0), rzm0.at[0], s1.at[3], r1.at[3], down_z)]

    def four_ring(j, c, w, dev, recv, base):
        ahead, behind = dev(wrap(c + 1, 4)), dev(wrap(c - 1, 4))
        far = wrap(c + 2, 4)
        lo, hi = pl.ds(0, 4), pl.ds(4, 4)
        sem = lambda i: (s2.at[base + i], r2.at[base + i])
        return [
            send(w(far).at[lo], recv.at[0], *sem(0), ahead),
            send(w(far).at[hi], recv.at[1], *sem(1), behind),
            send(w(wrap(c + 1, 4)).at[hi], recv.at[3], *sem(2), ahead),
            send(w(wrap(c - 1, 4)).at[lo], recv.at[4], *sem(3), behind),
        ]

    def relay(c, w, dev, recv, hold, base, begun):
        ahead, behind = dev(wrap(c + 1, 4)), dev(wrap(c - 1, 4))
        sem = lambda i: (s2.at[base + i], r2.at[base + i])
        out_copies = []
        for i, (step, half, slot, to) in enumerate(((1, 0, 2, ahead), (-1, 4, 5, behind))):
            begun[i].wait_recv()
            mine = w(wrap(c + step, 4))

            @pl.loop(0, 4)
            def _(a):
                hold[i, a] = add(mine.at[half + a], recv.at[i, a]).astype(BF16)

            out_copies.append(send(hold.at[i], recv.at[slot], *sem(4 + i), to))
        return out_copies

    wx_of = lambda c: wx.at[lax.div(c, 2), lax.rem(c, 2)]
    wy_of = lambda c: wy.at[c]

    first[1].wait_recv()
    now = step((2, False, 1), now)
    bx = four_ring(1, x, wx_of, at_x, rx, 0)
    first[2].wait_recv()
    step(None, now)
    by = four_ring(2, y, wy_of, at_y, ry, 6)

    def z_relay(k):
        def hop(chain, recv, hold, d, h, sem, to):
            chain[k - 1].wait_recv()
            hold[k - 1] = add(zpiece(d, h), recv.at[k - 1]).astype(BF16)
            chain.append(send(hold.at[k - 1], recv.at[k], s1.at[sem], r1.at[sem], to))

        hop(zp0, rzp0, szp0, 4 - k, 0, 4 * k, up_z)
        hop(zm1, rzm1, szm1, k - 4, 1, 4 * k + 1, down_z)
        if k < 3:
            hop(zp1, rzp1, szp1, 3 - k, 1, 4 * k + 2, up_z)
            hop(zm0, rzm0, szm0, k - 3, 0, 4 * k + 3, down_z)

    z_relay(1)
    cx = relay(x, wx_of, at_x, rx, sx, 0, bx)
    cy = relay(y, wy_of, at_y, ry, sy, 6, by)
    z_relay(2)
    z_relay(3)

    def settle(c, w, recv, begun, later, store):
        later[0].wait_recv()
        begun[2].wait_recv()
        begun[3].wait_recv()
        later[1].wait_recv()
        mine = w(c)

        @pl.loop(0, 4)
        def _(a):
            store(a, add(mine.at[a], recv.at[2, a], recv.at[4, a]))
            store(4 + a, add(mine.at[4 + a], recv.at[3, a], recv.at[5, a]))

    def store_x(a, v):
        ux[:, a] = v.astype(BF16)

    def store_y(a, v):
        uy[:, :, a] = v.astype(BF16)

    def spread(u, c, n, dev, recv, ss, rs, base):
        return [
            send(u(wrap(c + d, n)), recv.at[d - 1], ss.at[base + d - 1], rs.at[base + d - 1],
                 dev(wrap(c + d, n)))
            for d in range(1, n)
        ]

    ux_of = lambda c: ux.at[c]
    uy_of = lambda c: uy.at[lax.div(c, 2), lax.rem(c, 2)]
    uz_of = lambda c: uz.at[lax.div(c, 2), lax.rem(c, 2)]
    settle(x, wx_of, rx, bx, cx, store_x)
    dx = spread(ux_of, y, NY, at_y, vx, s3, r3, 0)
    settle(y, wy_of, ry, by, cy, store_y)
    dy = spread(uy_of, x, NX, at_x, vy, s3, r3, 3)
    for chain in (zp0, zm0, zp1, zm1):
        chain[-1].wait_recv()
    for h, (a, b) in enumerate(((rzp0.at[3], rzm0.at[2]), (rzp1.at[2], rzm1.at[3]))):
        v = add(zpiece(0, h), a, b)
        for l in range(2):
            uz[h, l] = v[:, l].astype(BF16)
    dz = spread(uz_of, x, NX, at_x, vz, s3, r3, 6)

    def gather(copies, u, c, recv, hold):
        for copy in copies:
            copy.wait_recv()
        hold[...] = add(u(c), *[recv.at[i] for i in range(len(copies))]).astype(BF16)

    gather(dx, ux_of, y, vx, tx)
    ex = spread(lambda c: tx.at[c], z, NZ, at_z, qx, s4, r4, 0)
    gather(dy, uy_of, x, vy, ty)
    ey = spread(lambda c: ty.at[c], z, NZ, at_z, qy, s4, r4, 7)
    gather(dz, uz_of, x, vz, tz)
    ez = spread(lambda c: tz.at[c], y, NY, at_y, qz, s4, r4, 14)

    def finish(j, copies, mine, recv):
        for copy in copies:
            copy.wait_recv()
        total = add(mine, *[recv.at[i] for i in range(len(copies))]) * (1.0 / 16.0)
        res[j, 0] = total[0:8]
        res[j, 1] = total[8:16]

    finish(0, ez, tz.at[y], qz)
    finish(1, ex, tx.at[z], qx)
    finish(2, ey, ty.at[z], qy)
    ends = [
        send(res.at[j, 1 - core], fin.at[j], s0.at[3 + j], r0.at[3 + j], partner) for j in range(3)
    ]
    for j in range(3):
        out[core * 3 + j] = res[j, core]
    for j in range(3):
        ends[j].wait_recv()
        out[(1 - core) * 3 + j] = fin[j]
    for copy in sent:
        copy.wait_send()


def vote_sum(info, tokens, cotangent, moved, projection, comb, xt):
    vmem = pltpu.VMEM
    t = (16, HS)
    bf = lambda *dims: vmem(dims + t, BF16)
    sems = lambda n: pltpu.SemaphoreType.DMA((n,))
    scratch = [
        vmem((3, BLOCK, D), BF16),
        vmem((3, BLOCK, HEADS * HS), BF16),
        vmem((D, GROUPS * HS), BF16),
        vmem((BLOCK, D), BF16),
        vmem((BLOCK, HEADS * HS), BF16),
        vmem((BLOCK, GROUPS * HS), F32),
        vmem((BLOCK, GROUPS * HS), BF16),
        vmem((BLOCK, GROUPS * HS), BF16),
        vmem((D, BLOCK), BF16),
        vmem((2, D, HS), F32),
        bf(3, 8, 2, 4, 2),
        bf(3, 8, 2, 4, 2),
        bf(8, 2, 4, 2),
        bf(2, 2, 8, 4),
        bf(4, 8, 2, 2),
        bf(4, 4, 2), bf(3, 4, 2), bf(3, 4, 2), bf(4, 4, 2),
        bf(3, 4, 2), bf(2, 4, 2), bf(2, 4, 2), bf(3, 4, 2),
        bf(6, 4, 4), bf(2, 4, 4),
        bf(6, 4, 2, 2), bf(2, 4, 2, 2),
        bf(4, 8), bf(2, 2, 8), bf(2, 2, 4),
        bf(3, 8), bf(3, 8), bf(3, 4),
        bf(8), bf(8), bf(4),
        bf(7), bf(7), bf(3),
        vmem((3, 2, 8, HS), F32),
        vmem((3, 8, HS), F32),
        sems(6), sems(SLABS),
        sems(6), sems(6), sems(16), sems(16), sems(12), sems(12), sems(9), sems(9), sems(17), sems(17),
    ]
    return pl.pallas_call(
        vote_kernel,
        out_shape=jax.ShapeDtypeStruct((GROUPS, 8, HS), F32),
        in_specs=[pl.BlockSpec(memory_space=vmem)]
        + [pl.BlockSpec(memory_space=pl.ANY)] * 7
        + [pl.BlockSpec(memory_space=vmem)] * 2,
        out_specs=pl.BlockSpec(memory_space=pltpu.VMEM),
        scratch_shapes=scratch,
        compiler_params=pltpu.CompilerParams(
            collective_id=1, has_side_effects=True, vmem_limit_bytes=52 << 20
        ),
        name="vote_sum",
    )(info, tokens, cotangent, *moved, projection, comb, xt)


LEVELS = 6
PAIRS = [(a, b) for a in range(LEVELS) for b in range(a + 1, LEVELS)]
ALONE = {0: (0, 2), 1: (1, 2), 2: (0, 2), 3: (2, 3), 4: (2, 4), 5: (2, 5)}
APART = [((0, 1), (2, 3, 4, 5)), ((3, 4), (0, 1, 2, 5)), ((3, 5), (0, 1, 2, 4)), ((4, 5), (0, 1, 2))]
APART += [((n, 4), (3,)) for n in range(3)] + [((n, 5), (4,)) for n in range(3)]
APART = [(a, b, c, v) for (a, b), bits in APART for c in bits for v in range(2)]


def flipped(i, m):
    return i + m - 2 * m * lax.rem(lax.div(i, m), 2)


def across(level):
    if level < 2:
        return {"dp_2": flipped(lax.axis_index("dp_2"), 1 << level)}
    if level == 2:
        return {"dp_1": 1 - lax.axis_index("dp_1")}
    return {"dp_0": flipped(lax.axis_index("dp_0"), 1 << (level - 3))}


def plan_kernel(dest, lengths, tok, cot, proj, info, comb, xt, x01, up01, proj_v, acc, joined,
                mine, mixed, from_plane, from_z, loc, psem, ss, rs):
    z, xh, y, xl, core = [lax.axis_index(a) for a in DP_REP]
    x = xh * 2 + xl

    def at_plane(dx, dy, c):
        i = wrap(x + dx, NX)
        return {"dp_1": lax.div(i, 2), "rep_0": lax.rem(i, 2), "dp_2": wrap(y + dy, NY), "rep_1": c}

    plane = [(dx, dy, c) for dx in range(NX) for dy in range(NY) for c in range(2)][1:]
    plane = [at_plane(dx, dy, 1 - core if c else core) for dx, dy, c in plane]
    column = [{"dp_0": wrap(z + d, NZ)} for d in range(1, NZ)]
    peers = plane + column

    halves = [pl.ds(0, BLOCK), pl.ds(BLOCK, BLOCK)]
    loads = [(tok.at[b], x01.at[halves[b]]) for b in range(2)]
    loads += [(cot.at[b], up01.at[halves[b]]) for b in range(2)]
    loads = [pltpu.make_async_copy(a, b, loc.at[i]) for i, (a, b) in enumerate(loads)]
    for load in loads[:2]:
        load.start()
    for k in range(SLABS):
        slab_copy(proj, proj_v, psem, k).start()
    for load in loads[2:]:
        load.start()

    barrier = pltpu.get_barrier_semaphore()
    for peer in peers:
        pl.semaphore_signal(barrier, inc=1, device_id=peer, device_id_type=MESH)

    here = (xh * NY + y) * 4 + xl * 2 + core
    rank = z * 8 + xh * NY + y
    wide = (1, 128)
    lane = lax.broadcasted_iota(jnp.int32, wide, 1)
    target = jnp.full(wide, dest[0], jnp.int32)
    code = jnp.zeros(wide, jnp.int32)
    for level in range(LEVELS):
        code = jnp.where(target == flipped(rank, 1 << level), level + 1, code)
    code = code * 256 + jnp.full(wide, lengths[3], jnp.int32)
    mine[...] = jnp.where((lane == here) & (target >= 0), code, 0)

    for load in loads[:2]:
        load.wait()

    def spread(src, stage, landing, base):
        copies = []
        for i, peer in enumerate(stage):
            copy = pltpu.make_async_remote_copy(
                src_ref=src, dst_ref=landing.at[i], send_sem=ss.at[base + i],
                recv_sem=rs.at[base + i], device_id=peer, device_id_type=MESH,
            )
            copy.start()
            copies.append(copy)
        return copies

    pl.semaphore_wait(barrier, len(peers))
    first = spread(mine, plane, from_plane, 0)
    join(proj, proj_v, psem, x01, acc, joined)
    for load in loads[2:]:
        load.wait()
    for copy in first:
        copy.wait_recv()
    row = mine[...]
    for i in range(len(plane)):
        row = jnp.maximum(row, from_plane[i])
    mixed[...] = row
    second = spread(mixed, column, from_z, len(plane))
    for b in range(2):
        attention(halves[b], lengths[b], joined, up01, comb)
    for r in range(D // 512):
        xt[r * 512 : (r + 1) * 512, :] = x01[:, r * 512 : (r + 1) * 512].T
    for copy in second:
        copy.wait_recv()

    shape = (8, 128)
    behind = lax.broadcasted_iota(jnp.int32, shape, 0)
    lane = lax.broadcasted_iota(jnp.int32, shape, 1)
    table = jnp.broadcast_to(mixed[...], shape)
    for k in range(1, NZ):
        table = jnp.where(behind == k, jnp.broadcast_to(from_z[k - 1], shape), table)
    level_of = lax.shift_right_logical(table, 8)

    def largest(v):
        v = v.astype(F32)
        return jnp.max(jnp.max(v, axis=1, keepdims=True), axis=0, keepdims=True)

    active = jnp.zeros((1, 1), F32)
    sender = jnp.zeros(shape, jnp.int32)
    for level in range(LEVELS):
        found = level_of == level + 1
        active += largest(jnp.where(found, 1 << level, 0))
        if level < 2:
            there, back = here + (flipped(y, 1 << level) - y) * 4, z * 0
        elif level == 2:
            there, back = here + (1 - 2 * xh) * NY * 4, z * 0
        else:
            there, back = here, wrap(z - flipped(z, 1 << (level - 3)), NZ)
        sender = jnp.where(found & (lane == there) & (behind == back), table, sender)
    inbound = largest(lax.shift_right_logical(sender, 8))
    arriving = largest(jnp.bitwise_and(sender, 255))
    third = jnp.where(inbound > 0.0, arriving, jnp.full((1, 1), lengths[2], jnp.int32).astype(F32))
    branch = jnp.full((1, 1), float(len(PAIRS)), F32)
    way = jnp.ones((1, 1), F32)
    for p, (a, b) in enumerate(PAIRS):
        sets = [(1 << a) + (1 << b)] + [1 << s for s, both in ALONE.items() if both == (a, b)]
        hit = active == float(sets[0])
        for other in sets[1:] + ([0] if p == 0 else []):
            hit = hit | (active == float(other))
        branch = jnp.where(hit, float(p), branch)
        by = jnp.where(inbound == a + 1.0, 1.0, jnp.where(inbound == b + 1.0, 2.0, 0.0))
        way = jnp.where(hit, by, way)
    zrow = wrap(z - behind, NZ)
    ranks = zrow * 8 + lax.div(lane, 4)

    def has(level, c, v):
        bit = jnp.bitwise_and(lax.shift_right_logical(ranks, c), 1)
        return largest(jnp.where((level_of == level + 1) & (bit == v), 1, 0))

    seen = {(a, c, v): has(a, c, v) for a, c, v in sorted({(l, c, v) for a, b, c, _ in APART
                                                           for l in (a, b) for v in range(2)})}
    for p, (a, b, c, v) in enumerate(APART):
        clear = seen[a, c, 1 - v] + seen[b, c, v] == 0.0
        clear = clear & (active == float((1 << a) + (1 << b)))
        branch = jnp.where(clear, float(len(PAIRS) + 1 + p), branch)
        way = jnp.where(clear, jnp.where(inbound > 0.0, 1.0, 0.0), way)
    told = jnp.zeros(shape, F32)
    for i, v in enumerate((branch, way, third, inbound, active)):
        told = jnp.where(behind == i, v, told)
    info[...] = told.astype(jnp.int32)
    for copy in first + second:
        copy.wait_send()


def plan(destination, lengths, tokens, cotangent, projection):
    vmem = pltpu.VMEM
    plane, column = 2 * NX * NY - 1, NZ - 1
    width = GROUPS * HS
    return pl.pallas_call(
        plan_kernel,
        out_shape=(
            jax.ShapeDtypeStruct((8, 128), jnp.int32),
            jax.ShapeDtypeStruct((2 * BLOCK, width), BF16),
            jax.ShapeDtypeStruct((D, 2 * BLOCK), BF16),
        ),
        in_specs=[pl.BlockSpec(memory_space=pltpu.SMEM)] * 2
        + [pl.BlockSpec(memory_space=pltpu.HBM)] * 3,
        out_specs=[pl.BlockSpec(memory_space=vmem)] * 3,
        scratch_shapes=[
            vmem((2 * BLOCK, D), BF16),
            vmem((2 * BLOCK, HEADS * HS), BF16),
            vmem((D, width), BF16),
            vmem((2 * BLOCK, width), F32),
            vmem((2 * BLOCK, width), BF16),
            vmem((1, 128), jnp.int32),
            vmem((1, 128), jnp.int32),
            vmem((plane, 1, 128), jnp.int32),
            vmem((column, 1, 128), jnp.int32),
            pltpu.SemaphoreType.DMA((4,)),
            pltpu.SemaphoreType.DMA((SLABS,)),
            pltpu.SemaphoreType.DMA((plane + column,)),
            pltpu.SemaphoreType.DMA((plane + column,)),
        ],
        compiler_params=pltpu.CompilerParams(
            collective_id=2, has_side_effects=True, vmem_limit_bytes=52 << 20
        ),
        name="plan",
    )(destination, lengths, tokens, cotangent, projection)


def move_apart(p):
    a, b, c, v = APART[p]

    def kernel(tokens, cotangent, tok_a, cot_a, tok_b, cot_b, ss, rs):
        here = {name: lax.axis_index(name) for name in DP}
        rank = (here["dp_0"] * 2 + here["dp_1"]) * NY + here["dp_2"]
        bit = lax.rem(lax.div(rank, 1 << c), 2)
        in_a = bit if v else 1 - bit
        to_a, to_b = {**here, **across(a)}, {**here, **across(b)}
        peer = {name: to_b[name] + in_a * (to_a[name] - to_b[name]) for name in DP}
        barrier = pltpu.get_barrier_semaphore()
        pl.semaphore_signal(barrier, inc=1, device_id=peer, device_id_type=MESH)
        pl.semaphore_wait(barrier, 1)
        copies = []
        for i, (src, dst) in enumerate(((tokens, tok_a), (cotangent, cot_a))):
            copies.append(pltpu.make_async_remote_copy(
                src_ref=src.at[3], dst_ref=dst, send_sem=ss.at[i], recv_sem=rs.at[i],
                device_id=peer, device_id_type=MESH,
            ))
            copies[-1].start()
        for copy in copies:
            copy.wait()

    return mover(kernel, 3 + len(PAIRS) + p)


def move_pair(p):
    peers_of = PAIRS[p]

    def kernel(tokens, cotangent, tok_a, cot_a, tok_b, cot_b, ss, rs):
        peers = [across(level) for level in peers_of]
        barrier = pltpu.get_barrier_semaphore()
        for peer in peers:
            pl.semaphore_signal(barrier, inc=1, device_id=peer, device_id_type=MESH)
        pl.semaphore_wait(barrier, 2)
        copies = []
        for i, (src, dst, peer) in enumerate((
            (tokens, tok_a, peers[0]), (tokens, tok_b, peers[1]),
            (cotangent, cot_a, peers[0]), (cotangent, cot_b, peers[1]),
        )):
            copies.append(pltpu.make_async_remote_copy(
                src_ref=src.at[3], dst_ref=dst, send_sem=ss.at[i], recv_sem=rs.at[i],
                device_id=peer, device_id_type=MESH,
            ))
            copies[-1].start()
        for copy in copies:
            copy.wait()

    return mover(kernel, 3 + p)


def mover(kernel, collective_id):
    def call(tokens, cotangent, info):
        block = jax.ShapeDtypeStruct(tokens.shape[1:], BF16)
        upstream = jax.ShapeDtypeStruct(cotangent.shape[1:], BF16)
        return pl.pallas_call(
            kernel,
            out_shape=(block, upstream, block, upstream),
            in_specs=[pl.BlockSpec(memory_space=pl.ANY)] * 2,
            out_specs=[pl.BlockSpec(memory_space=pl.ANY)] * 4,
            scratch_shapes=[pltpu.SemaphoreType.DMA((4,)), pltpu.SemaphoreType.DMA((4,))],
            compiler_params=pltpu.CompilerParams(
                collective_id=collective_id, has_side_effects=True, vmem_limit_bytes=2 << 20
            ),
            name="move",
        )(tokens, cotangent)

    return call


def swapped(value, axis, apart):
    mask = 2**apart
    pairs = [(source, source ^ mask) for source in range(lax.axis_size(axis))]
    return lax.ppermute(value, axis, pairs)


def move_many(tokens, cotangent, info):
    kept = (tokens[2], cotangent[2])
    for level in range(LEVELS):

        def trade(kept, level=level):
            got = swapped((tokens[3], cotangent[3]), DP, level)
            arrived = info[3, 0] == level + 1
            return jax.tree.map(lambda new, old: jnp.where(arrived, new, old), got, kept)

        needed = jnp.bitwise_and(jnp.right_shift(info[4, 0], level), 1) == 1
        kept = lax.cond(needed, trade, lambda kept: kept, kept)
    return (*kept, *kept)


def shards(tokens, cotangent, projection, block_lengths, destination):
    lengths = block_lengths[0]
    info, comb, xt = plan(destination, lengths, tokens, cotangent, projection)
    branches = [move_pair(p) for p in range(len(PAIRS))] + [move_many]
    branches += [move_apart(p) for p in range(len(APART))]
    moved = lax.switch(info[0, 0], branches, tokens, cotangent, info)
    summed = vote_sum(info, tokens, cotangent, moved, projection, comb, xt)
    return summed.transpose(1, 0, 2).reshape(8, GROUPS * HS)


def solution(mesh):
    split = Mesh(mesh.devices.reshape(8, 2, 4, 2, 2), DP_REP)
    placed = (P(DP_REP, None, None), P(DP_REP, None, None), P(), P(DP_REP, None), P(DP_REP))
    return jax.shard_map(
        shards, mesh=split, in_specs=placed, out_specs=P(DP_REP, None), check_vma=False
    )
```

```python
import math

import jax
import jax.numpy as jnp
from jax import lax
from jax.experimental import pallas as pl
from jax.experimental.pallas import tpu as pltpu
from jax.sharding import Mesh
from jax.sharding import PartitionSpec as P

HS = 256
HEADS = 4
BLOCK = 128
DP_REP = ("dp_0", "dp_1", "dp_2", "rep_0", "rep_1")
REP = ("rep_0", "rep_1")
DP = ("dp_0", "dp_1", "dp_2")
GROUPS = HEADS + 2
D = 2048
MESH = pl.DeviceIdType.MESH
F32 = jnp.float32
BF16 = jnp.bfloat16


def dot(a, b, ca, cb):
    return lax.dot_general(a, b, (((ca,), (cb,)), ((), ())), preferred_element_type=F32)


def attention(at, length, joined, up, comb):
    scale = HS ** (-0.5)

    def heads(ref):
        return jnp.concatenate([ref[at, h * HS : (h + 1) * HS] for h in range(HEADS)], axis=0)

    query = heads(joined)
    keys = joined[at, HEADS * HS : (HEADS + 1) * HS]
    values = joined[at, (HEADS + 1) * HS :]
    shape = (HEADS * BLOCK, BLOCK)
    row = lax.rem(lax.broadcasted_iota(jnp.int32, shape, 0), BLOCK)
    col = lax.broadcasted_iota(jnp.int32, shape, 1)
    allowed = (col <= row) & (col < jnp.broadcast_to(length, shape))
    scores = jnp.where(allowed, dot(query, keys, 1, 1) * scale, -1e30)
    peak = jnp.max(scores, axis=-1, keepdims=True)
    expo = jnp.exp(scores - peak)
    weights = expo / jnp.sum(expo, axis=-1, keepdims=True)
    wide = (HEADS * BLOCK, HS)
    live = lax.rem(lax.broadcasted_iota(jnp.int32, wide, 0), BLOCK) < jnp.broadcast_to(length, wide)
    upstream = jnp.where(live, heads(up).astype(F32), 0.0).astype(BF16)
    probs = weights.astype(BF16)
    grad_values = dot(probs.T, upstream, 1, 0).astype(BF16)
    grad_probs = dot(upstream, values, 1, 1)
    centre = jnp.sum(weights * grad_probs, axis=-1, keepdims=True)
    grad_scores = (weights * (grad_probs - centre) * scale).astype(BF16)
    grad_query = dot(grad_scores, keys, 1, 0).astype(BF16)
    grad_keys = dot(grad_scores.T, query, 1, 0).astype(BF16)
    for h in range(HEADS):
        comb[at, h * HS : (h + 1) * HS] = grad_query[h * BLOCK : (h + 1) * BLOCK]
    comb[at, HEADS * HS : (HEADS + 1) * HS] = grad_keys
    comb[at, (HEADS + 1) * HS :] = grad_values


SLABS = 4
SLAB = D // SLABS


def slab_copy(proj, proj_v, sem, k):
    at = pl.ds(k * SLAB, SLAB)
    return pltpu.make_async_copy(proj.at[at], proj_v.at[at], sem.at[k])


def join(proj, proj_v, sem, x, acc, joined):
    for k in range(SLABS):
        slab_copy(proj, proj_v, sem, k).wait()
        at = slice(k * SLAB, (k + 1) * SLAB)
        part = dot(x[:, at], proj_v[at, :], 1, 0)
        if k == SLABS - 1:
            joined[...] = (acc[...] + part).astype(BF16)
        elif k:
            acc[...] += part
        else:
            acc[...] = part


NZ, NY, NX = 8, 4, 4


def wrap(i, n):
    return lax.rem(i + n, n)


def vote_kernel(info, tok, cot, tok_a, cot_a, tok_b, cot_b, proj, comb01, xt01, out,
                cand_t, cand_c, proj_v, x3, up3, acc3, joined3, comb3, xt3, grad, mail,
                part, wz, wx, wy, rzp0, rzp1, rzm0, rzm1, szp0, szp1, szm0,
                szm1, rx, sx, ry, sy, ux, uy, uz, vx, vy, vz, tx, ty, tz, qx, qy, qz, res, fin,
                loc, psem, s0, r0, s1, r1, s2, r2, s3, r3, s4, r4):
    z, xh, y, xl, core = [lax.axis_index(a) for a in DP_REP]
    x = xh * 2 + xl

    def at_x(i):
        return {"dp_1": lax.div(i, 2), "rep_0": lax.rem(i, 2)}

    def at_y(i):
        return {"dp_2": i}

    def at_z(i):
        return {"dp_0": i}

    partner = {"rep_1": 1 - core}

    loads = [(tok.at[2], cand_t.at[0]), (tok_a, cand_t.at[1]), (tok_b, cand_t.at[2])]
    loads += [(cot.at[2], cand_c.at[0]), (cot_a, cand_c.at[1]), (cot_b, cand_c.at[2])]
    loads = [pltpu.make_async_copy(a, b, loc.at[i]) for i, (a, b) in enumerate(loads)]
    for load in loads[:3]:
        load.start()
    for k in range(SLABS):
        slab_copy(proj, proj_v, psem, k).start()
    for load in loads[3:]:
        load.start()

    barrier = pltpu.get_barrier_semaphore()
    peers = [partner]
    peers += [at_x(wrap(x + d, NX)) for d in range(1, NX)]
    peers += [at_y(wrap(y + d, NY)) for d in range(1, NY)]
    peers += [at_z(wrap(z + d, NZ)) for d in range(1, NZ)]
    for peer in peers:
        pl.semaphore_signal(barrier, inc=1, device_id=peer, device_id_type=MESH)

    sent = []

    def send(src, dst, ss, rs, dev):
        copy = pltpu.make_async_remote_copy(
            src_ref=src, dst_ref=dst, send_sem=ss, recv_sem=rs, device_id=dev, device_id_type=MESH
        )
        copy.start()
        sent.append(copy)
        return copy

    def add(*refs):
        total = refs[0][...].astype(F32)
        for ref in refs[1:]:
            total = total + ref[...].astype(F32)
        return total

    def chosen(c):
        way = jnp.broadcast_to(info[1:2, 0:1], c.shape[1:])
        return jnp.where(way == 1, c[1], jnp.where(way == 2, c[2], c[0]))

    for load in loads[:3]:
        load.wait()
    x3[...] = chosen(cand_t)
    for r in range(D // 512):
        xt3[r * 512 : (r + 1) * 512, :] = x3[:, r * 512 : (r + 1) * 512].T
    join(proj, proj_v, psem, x3, acc3, joined3)
    for load in loads[3:]:
        load.wait()
    up3[...] = chosen(cand_c)
    attention(slice(None), info[2:3, 0:1], joined3, up3, comb3)
    pl.semaphore_wait(barrier, len(peers))

    tile, chunk = 128, 512
    other = 1 - core

    def step(begin, end):
        if begin is not None:
            j, to_partner, buf = begin
            cols = pl.ds(pl.multiple_of(((other if to_partner else core) * 3 + j) * HS, HS), HS)

        total = jnp.zeros((8, HS), F32)
        for q in range(D // chunk):
            if begin is not None:
                at = pl.ds(q * chunk, chunk)
                new = dot(xt01[at, :], comb01[:, cols], 1, 0)
                new = new + dot(xt3[at, :], comb3[:, cols], 1, 0)
                grad[buf, at, :] = new
                total = total + jnp.sum((new * new).reshape(chunk // 8, 8, HS), axis=0)
            if end is None:
                continue
            for t in range(chunk // tile):
                a, h = divmod(q * (chunk // tile) + t, 2)
                old = grad[end[2], pl.ds(a * 256 + h * tile, tile), :]
                soft = (old / (jnp.abs(old) + end[3])).reshape(NY, 2, 16, HS)
                if end[1]:
                    mail[end[0], a, h] = soft.astype(BF16)
                    continue
                both = (soft + part[end[0], a, h].astype(F32)).astype(BF16)
                if end[0] == 0:
                    wz[a, h] = both
                elif end[0] == 1:
                    for l in range(2):
                        wx[h, l, a] = both[:, l]
                else:
                    for b in range(NY):
                        wy[b, a, h] = both[b]
        if begin is None:
            return None
        total = jnp.sum(jnp.sum(total, axis=0, keepdims=True), axis=1, keepdims=True)
        return (*begin, 0.25 * jnp.sqrt(total * (1.0 / (D * HS)) + 1e-06))

    first = {}

    def post(j):
        first[j] = send(mail.at[j], part.at[j], s0.at[j], r0.at[j], partner)

    now = step((0, True, 0), None)
    now = step((1, True, 1), now)
    post(0)
    now = step((2, True, 0), now)
    post(1)
    now = step((0, False, 1), now)
    post(2)
    first[0].wait_recv()
    now = step((1, False, 0), now)

    up_z, down_z = at_z(wrap(z + 1, NZ)), at_z(wrap(z - 1, NZ))

    def zpiece(d, h):
        return wz.at[wrap(z + d, NZ), h]

    zp0 = [send(zpiece(4, 0), rzp0.at[0], s1.at[0], r1.at[0], up_z)]
    zm1 = [send(zpiece(-4, 1), rzm1.at[0], s1.at[1], r1.at[1], down_z)]
    zp1 = [send(zpiece(3, 1), rzp1.at[0], s1.at[2], r1.at[2], up_z)]
    zm0 = [send(zpiece(-3, 0), rzm0.at[0], s1.at[3], r1.at[3], down_z)]

    def four_ring(j, c, w, dev, recv, base):
        ahead, behind = dev(wrap(c + 1, 4)), dev(wrap(c - 1, 4))
        far = wrap(c + 2, 4)
        lo, hi = pl.ds(0, 4), pl.ds(4, 4)
        sem = lambda i: (s2.at[base + i], r2.at[base + i])
        return [
            send(w(far).at[lo], recv.at[0], *sem(0), ahead),
            send(w(far).at[hi], recv.at[1], *sem(1), behind),
            send(w(wrap(c + 1, 4)).at[hi], recv.at[3], *sem(2), ahead),
            send(w(wrap(c - 1, 4)).at[lo], recv.at[4], *sem(3), behind),
        ]

    def relay(c, w, dev, recv, hold, base, begun):
        ahead, behind = dev(wrap(c + 1, 4)), dev(wrap(c - 1, 4))
        sem = lambda i: (s2.at[base + i], r2.at[base + i])
        out_copies = []
        for i, (step, half, slot, to) in enumerate(((1, 0, 2, ahead), (-1, 4, 5, behind))):
            begun[i].wait_recv()
            mine = w(wrap(c + step, 4))

            @pl.loop(0, 4)
            def _(a):
                hold[i, a] = add(mine.at[half + a], recv.at[i, a]).astype(BF16)

            out_copies.append(send(hold.at[i], recv.at[slot], *sem(4 + i), to))
        return out_copies

    wx_of = lambda c: wx.at[lax.div(c, 2), lax.rem(c, 2)]
    wy_of = lambda c: wy.at[c]

    first[1].wait_recv()
    now = step((2, False, 1), now)
    bx = four_ring(1, x, wx_of, at_x, rx, 0)
    first[2].wait_recv()
    step(None, now)
    by = four_ring(2, y, wy_of, at_y, ry, 6)

    def z_relay(k):
        def hop(chain, recv, hold, d, h, sem, to):
            chain[k - 1].wait_recv()
            hold[k - 1] = add(zpiece(d, h), recv.at[k - 1]).astype(BF16)
            chain.append(send(hold.at[k - 1], recv.at[k], s1.at[sem], r1.at[sem], to))

        hop(zp0, rzp0, szp0, 4 - k, 0, 4 * k, up_z)
        hop(zm1, rzm1, szm1, k - 4, 1, 4 * k + 1, down_z)
        if k < 3:
            hop(zp1, rzp1, szp1, 3 - k, 1, 4 * k + 2, up_z)
            hop(zm0, rzm0, szm0, k - 3, 0, 4 * k + 3, down_z)

    z_relay(1)
    cx = relay(x, wx_of, at_x, rx, sx, 0, bx)
    cy = relay(y, wy_of, at_y, ry, sy, 6, by)
    z_relay(2)
    z_relay(3)

    def settle(c, w, recv, begun, later, store):
        later[0].wait_recv()
        begun[2].wait_recv()
        begun[3].wait_recv()
        later[1].wait_recv()
        mine = w(c)

        @pl.loop(0, 4)
        def _(a):
            store(a, add(mine.at[a], recv.at[2, a], recv.at[4, a]))
            store(4 + a, add(mine.at[4 + a], recv.at[3, a], recv.at[5, a]))

    def store_x(a, v):
        ux[:, a] = v.astype(BF16)

    def store_y(a, v):
        uy[:, :, a] = v.astype(BF16)

    def spread(u, c, n, dev, recv, ss, rs, base):
        return [
            send(u(wrap(c + d, n)), recv.at[d - 1], ss.at[base + d - 1], rs.at[base + d - 1],
                 dev(wrap(c + d, n)))
            for d in range(1, n)
        ]

    ux_of = lambda c: ux.at[c]
    uy_of = lambda c: uy.at[lax.div(c, 2), lax.rem(c, 2)]
    uz_of = lambda c: uz.at[lax.div(c, 2), lax.rem(c, 2)]
    settle(x, wx_of, rx, bx, cx, store_x)
    dx = spread(ux_of, y, NY, at_y, vx, s3, r3, 0)
    settle(y, wy_of, ry, by, cy, store_y)
    dy = spread(uy_of, x, NX, at_x, vy, s3, r3, 3)
    for chain in (zp0, zm0, zp1, zm1):
        chain[-1].wait_recv()
    for h, (a, b) in enumerate(((rzp0.at[3], rzm0.at[2]), (rzp1.at[2], rzm1.at[3]))):
        v = add(zpiece(0, h), a, b)
        for l in range(2):
            uz[h, l] = v[:, l].astype(BF16)
    dz = spread(uz_of, x, NX, at_x, vz, s3, r3, 6)

    def gather(copies, u, c, recv, hold):
        for copy in copies:
            copy.wait_recv()
        hold[...] = add(u(c), *[recv.at[i] for i in range(len(copies))]).astype(BF16)

    gather(dx, ux_of, y, vx, tx)
    ex = spread(lambda c: tx.at[c], z, NZ, at_z, qx, s4, r4, 0)
    gather(dy, uy_of, x, vy, ty)
    ey = spread(lambda c: ty.at[c], z, NZ, at_z, qy, s4, r4, 7)
    gather(dz, uz_of, x, vz, tz)
    ez = spread(lambda c: tz.at[c], y, NY, at_y, qz, s4, r4, 14)

    def finish(j, copies, mine, recv):
        for copy in copies:
            copy.wait_recv()
        total = add(mine, *[recv.at[i] for i in range(len(copies))]) * (1.0 / 16.0)
        res[j, 0] = total[0:8]
        res[j, 1] = total[8:16]

    finish(0, ez, tz.at[y], qz)
    finish(1, ex, tx.at[z], qx)
    finish(2, ey, ty.at[z], qy)
    ends = [
        send(res.at[j, 1 - core], fin.at[j], s0.at[3 + j], r0.at[3 + j], partner) for j in range(3)
    ]
    for j in range(3):
        out[core * 3 + j] = res[j, core]
    for j in range(3):
        ends[j].wait_recv()
        out[(1 - core) * 3 + j] = fin[j]
    for copy in sent:
        copy.wait_send()


def vote_sum(info, tokens, cotangent, moved, projection, comb, xt):
    vmem = pltpu.VMEM
    t = (16, HS)
    bf = lambda *dims: vmem(dims + t, BF16)
    sems = lambda n: pltpu.SemaphoreType.DMA((n,))
    scratch = [
        vmem((3, BLOCK, D), BF16),
        vmem((3, BLOCK, HEADS * HS), BF16),
        vmem((D, GROUPS * HS), BF16),
        vmem((BLOCK, D), BF16),
        vmem((BLOCK, HEADS * HS), BF16),
        vmem((BLOCK, GROUPS * HS), F32),
        vmem((BLOCK, GROUPS * HS), BF16),
        vmem((BLOCK, GROUPS * HS), BF16),
        vmem((D, BLOCK), BF16),
        vmem((2, D, HS), F32),
        bf(3, 8, 2, 4, 2),
        bf(3, 8, 2, 4, 2),
        bf(8, 2, 4, 2),
        bf(2, 2, 8, 4),
        bf(4, 8, 2, 2),
        bf(4, 4, 2), bf(3, 4, 2), bf(3, 4, 2), bf(4, 4, 2),
        bf(3, 4, 2), bf(2, 4, 2), bf(2, 4, 2), bf(3, 4, 2),
        bf(6, 4, 4), bf(2, 4, 4),
        bf(6, 4, 2, 2), bf(2, 4, 2, 2),
        bf(4, 8), bf(2, 2, 8), bf(2, 2, 4),
        bf(3, 8), bf(3, 8), bf(3, 4),
        bf(8), bf(8), bf(4),
        bf(7), bf(7), bf(3),
        vmem((3, 2, 8, HS), F32),
        vmem((3, 8, HS), F32),
        sems(6), sems(SLABS),
        sems(6), sems(6), sems(16), sems(16), sems(12), sems(12), sems(9), sems(9), sems(17), sems(17),
    ]
    return pl.pallas_call(
        vote_kernel,
        out_shape=jax.ShapeDtypeStruct((GROUPS, 8, HS), F32),
        in_specs=[pl.BlockSpec(memory_space=vmem)]
        + [pl.BlockSpec(memory_space=pl.ANY)] * 7
        + [pl.BlockSpec(memory_space=vmem)] * 2,
        out_specs=pl.BlockSpec(memory_space=pltpu.VMEM),
        scratch_shapes=scratch,
        compiler_params=pltpu.CompilerParams(
            collective_id=1, has_side_effects=True, vmem_limit_bytes=52 << 20
        ),
        name="vote_sum",
    )(info, tokens, cotangent, *moved, projection, comb, xt)


LEVELS = 6
PAIRS = [(a, b) for a in range(LEVELS) for b in range(a + 1, LEVELS)]
ALONE = {0: (0, 2), 1: (1, 2), 2: (0, 2), 3: (2, 3), 4: (2, 4), 5: (2, 5)}


def flipped(i, m):
    return i + m - 2 * m * lax.rem(lax.div(i, m), 2)


def across(level):
    if level < 2:
        return {"dp_2": flipped(lax.axis_index("dp_2"), 1 << level)}
    if level == 2:
        return {"dp_1": 1 - lax.axis_index("dp_1")}
    return {"dp_0": flipped(lax.axis_index("dp_0"), 1 << (level - 3))}


def plan_kernel(dest, lengths, tok, cot, proj, info, comb, xt, x01, up01, proj_v, acc, joined,
                mine, mixed, from_plane, from_z, loc, psem, ss, rs):
    z, xh, y, xl, core = [lax.axis_index(a) for a in DP_REP]
    x = xh * 2 + xl

    def at_plane(dx, dy, c):
        i = wrap(x + dx, NX)
        return {"dp_1": lax.div(i, 2), "rep_0": lax.rem(i, 2), "dp_2": wrap(y + dy, NY), "rep_1": c}

    plane = [(dx, dy, c) for dx in range(NX) for dy in range(NY) for c in range(2)][1:]
    plane = [at_plane(dx, dy, 1 - core if c else core) for dx, dy, c in plane]
    column = [{"dp_0": wrap(z + d, NZ)} for d in range(1, NZ)]
    peers = plane + column

    halves = [pl.ds(0, BLOCK), pl.ds(BLOCK, BLOCK)]
    loads = [(tok.at[b], x01.at[halves[b]]) for b in range(2)]
    loads += [(cot.at[b], up01.at[halves[b]]) for b in range(2)]
    loads = [pltpu.make_async_copy(a, b, loc.at[i]) for i, (a, b) in enumerate(loads)]
    for load in loads[:2]:
        load.start()
    for k in range(SLABS):
        slab_copy(proj, proj_v, psem, k).start()
    for load in loads[2:]:
        load.start()

    barrier = pltpu.get_barrier_semaphore()
    for peer in peers:
        pl.semaphore_signal(barrier, inc=1, device_id=peer, device_id_type=MESH)

    here = (xh * NY + y) * 4 + xl * 2 + core
    rank = z * 8 + xh * NY + y
    wide = (1, 128)
    lane = lax.broadcasted_iota(jnp.int32, wide, 1)
    target = jnp.full(wide, dest[0], jnp.int32)
    code = jnp.zeros(wide, jnp.int32)
    for level in range(LEVELS):
        code = jnp.where(target == flipped(rank, 1 << level), level + 1, code)
    code = code * 256 + jnp.full(wide, lengths[3], jnp.int32)
    mine[...] = jnp.where((lane == here) & (target >= 0), code, 0)

    for load in loads[:2]:
        load.wait()

    def spread(src, stage, landing, base):
        copies = []
        for i, peer in enumerate(stage):
            copy = pltpu.make_async_remote_copy(
                src_ref=src, dst_ref=landing.at[i], send_sem=ss.at[base + i],
                recv_sem=rs.at[base + i], device_id=peer, device_id_type=MESH,
            )
            copy.start()
            copies.append(copy)
        return copies

    pl.semaphore_wait(barrier, len(peers))
    first = spread(mine, plane, from_plane, 0)
    join(proj, proj_v, psem, x01, acc, joined)
    for load in loads[2:]:
        load.wait()
    for copy in first:
        copy.wait_recv()
    row = mine[...]
    for i in range(len(plane)):
        row = jnp.maximum(row, from_plane[i])
    mixed[...] = row
    second = spread(mixed, column, from_z, len(plane))
    for b in range(2):
        attention(halves[b], lengths[b], joined, up01, comb)
    for r in range(D // 512):
        xt[r * 512 : (r + 1) * 512, :] = x01[:, r * 512 : (r + 1) * 512].T
    for copy in second:
        copy.wait_recv()

    shape = (8, 128)
    behind = lax.broadcasted_iota(jnp.int32, shape, 0)
    lane = lax.broadcasted_iota(jnp.int32, shape, 1)
    table = jnp.broadcast_to(mixed[...], shape)
    for k in range(1, NZ):
        table = jnp.where(behind == k, jnp.broadcast_to(from_z[k - 1], shape), table)
    level_of = lax.shift_right_logical(table, 8)

    def largest(v):
        v = v.astype(F32)
        return jnp.max(jnp.max(v, axis=1, keepdims=True), axis=0, keepdims=True)

    active = jnp.zeros((1, 1), F32)
    sender = jnp.zeros(shape, jnp.int32)
    for level in range(LEVELS):
        found = level_of == level + 1
        active += largest(jnp.where(found, 1 << level, 0))
        if level < 2:
            there, back = here + (flipped(y, 1 << level) - y) * 4, z * 0
        elif level == 2:
            there, back = here + (1 - 2 * xh) * NY * 4, z * 0
        else:
            there, back = here, wrap(z - flipped(z, 1 << (level - 3)), NZ)
        sender = jnp.where(found & (lane == there) & (behind == back), table, sender)
    inbound = largest(lax.shift_right_logical(sender, 8))
    arriving = largest(jnp.bitwise_and(sender, 255))
    third = jnp.where(inbound > 0.0, arriving, jnp.full((1, 1), lengths[2], jnp.int32).astype(F32))
    branch = jnp.full((1, 1), float(len(PAIRS)), F32)
    way = jnp.ones((1, 1), F32)
    for p, (a, b) in enumerate(PAIRS):
        sets = [(1 << a) + (1 << b)] + [1 << s for s, both in ALONE.items() if both == (a, b)]
        hit = active == float(sets[0])
        for other in sets[1:] + ([0] if p == 0 else []):
            hit = hit | (active == float(other))
        branch = jnp.where(hit, float(p), branch)
        by = jnp.where(inbound == a + 1.0, 1.0, jnp.where(inbound == b + 1.0, 2.0, 0.0))
        way = jnp.where(hit, by, way)
    told = jnp.zeros(shape, F32)
    for i, v in enumerate((branch, way, third, inbound, active)):
        told = jnp.where(behind == i, v, told)
    info[...] = told.astype(jnp.int32)
    for copy in first + second:
        copy.wait_send()


def plan(destination, lengths, tokens, cotangent, projection):
    vmem = pltpu.VMEM
    plane, column = 2 * NX * NY - 1, NZ - 1
    width = GROUPS * HS
    return pl.pallas_call(
        plan_kernel,
        out_shape=(
            jax.ShapeDtypeStruct((8, 128), jnp.int32),
            jax.ShapeDtypeStruct((2 * BLOCK, width), BF16),
            jax.ShapeDtypeStruct((D, 2 * BLOCK), BF16),
        ),
        in_specs=[pl.BlockSpec(memory_space=pltpu.SMEM)] * 2
        + [pl.BlockSpec(memory_space=pltpu.HBM)] * 3,
        out_specs=[pl.BlockSpec(memory_space=vmem)] * 3,
        scratch_shapes=[
            vmem((2 * BLOCK, D), BF16),
            vmem((2 * BLOCK, HEADS * HS), BF16),
            vmem((D, width), BF16),
            vmem((2 * BLOCK, width), F32),
            vmem((2 * BLOCK, width), BF16),
            vmem((1, 128), jnp.int32),
            vmem((1, 128), jnp.int32),
            vmem((plane, 1, 128), jnp.int32),
            vmem((column, 1, 128), jnp.int32),
            pltpu.SemaphoreType.DMA((4,)),
            pltpu.SemaphoreType.DMA((SLABS,)),
            pltpu.SemaphoreType.DMA((plane + column,)),
            pltpu.SemaphoreType.DMA((plane + column,)),
        ],
        compiler_params=pltpu.CompilerParams(
            collective_id=2, has_side_effects=True, vmem_limit_bytes=52 << 20
        ),
        name="plan",
    )(destination, lengths, tokens, cotangent, projection)


def move_pair(p):
    peers_of = PAIRS[p]

    def kernel(tokens, cotangent, tok_a, cot_a, tok_b, cot_b, ss, rs):
        peers = [across(level) for level in peers_of]
        barrier = pltpu.get_barrier_semaphore()
        for peer in peers:
            pl.semaphore_signal(barrier, inc=1, device_id=peer, device_id_type=MESH)
        pl.semaphore_wait(barrier, 2)
        copies = []
        for i, (src, dst, peer) in enumerate((
            (tokens, tok_a, peers[0]), (tokens, tok_b, peers[1]),
            (cotangent, cot_a, peers[0]), (cotangent, cot_b, peers[1]),
        )):
            copies.append(pltpu.make_async_remote_copy(
                src_ref=src.at[3], dst_ref=dst, send_sem=ss.at[i], recv_sem=rs.at[i],
                device_id=peer, device_id_type=MESH,
            ))
            copies[-1].start()
        for copy in copies:
            copy.wait()

    def call(tokens, cotangent, info):
        block = jax.ShapeDtypeStruct(tokens.shape[1:], BF16)
        upstream = jax.ShapeDtypeStruct(cotangent.shape[1:], BF16)
        return pl.pallas_call(
            kernel,
            out_shape=(block, upstream, block, upstream),
            in_specs=[pl.BlockSpec(memory_space=pl.ANY)] * 2,
            out_specs=[pl.BlockSpec(memory_space=pl.ANY)] * 4,
            scratch_shapes=[pltpu.SemaphoreType.DMA((4,)), pltpu.SemaphoreType.DMA((4,))],
            compiler_params=pltpu.CompilerParams(
                collective_id=3 + p, has_side_effects=True, vmem_limit_bytes=2 << 20
            ),
            name="move",
        )(tokens, cotangent)

    return call


def swapped(value, axis, apart):
    mask = 2**apart
    pairs = [(source, source ^ mask) for source in range(lax.axis_size(axis))]
    return lax.ppermute(value, axis, pairs)


def move_many(tokens, cotangent, info):
    kept = (tokens[2], cotangent[2])
    for level in range(LEVELS):

        def trade(kept, level=level):
            got = swapped((tokens[3], cotangent[3]), DP, level)
            arrived = info[3, 0] == level + 1
            return jax.tree.map(lambda new, old: jnp.where(arrived, new, old), got, kept)

        needed = jnp.bitwise_and(jnp.right_shift(info[4, 0], level), 1) == 1
        kept = lax.cond(needed, trade, lambda kept: kept, kept)
    return (*kept, *kept)


def shards(tokens, cotangent, projection, block_lengths, destination):
    lengths = block_lengths[0]
    info, comb, xt = plan(destination, lengths, tokens, cotangent, projection)
    branches = [move_pair(p) for p in range(len(PAIRS))] + [move_many]
    moved = lax.switch(info[0, 0], branches, tokens, cotangent, info)
    summed = vote_sum(info, tokens, cotangent, moved, projection, comb, xt)
    return summed.transpose(1, 0, 2).reshape(8, GROUPS * HS)


def solution(mesh):
    split = Mesh(mesh.devices.reshape(8, 2, 4, 2, 2), DP_REP)
    placed = (P(DP_REP, None, None), P(DP_REP, None, None), P(), P(DP_REP, None), P(DP_REP))
    return jax.shard_map(
        shards, mesh=split, in_specs=placed, out_specs=P(DP_REP, None), check_vma=False
    )
```

```python
import math

import jax
import jax.numpy as jnp
from jax import lax
from jax.experimental import pallas as pl
from jax.experimental.pallas import tpu as pltpu
from jax.sharding import Mesh
from jax.sharding import PartitionSpec as P

HS = 256
HEADS = 4
BLOCK = 128
DP_REP = ("dp_0", "dp_1", "dp_2", "rep_0", "rep_1")
REP = ("rep_0", "rep_1")
DP = ("dp_0", "dp_1", "dp_2")
GROUPS = HEADS + 2
D = 2048
MESH = pl.DeviceIdType.MESH
F32 = jnp.float32
BF16 = jnp.bfloat16


def dot(a, b, ca, cb):
    return lax.dot_general(a, b, (((ca,), (cb,)), ((), ())), preferred_element_type=F32)


def attention(at, length, joined, up, comb):
    scale = HS ** (-0.5)

    def heads(ref):
        return jnp.concatenate([ref[at, h * HS : (h + 1) * HS] for h in range(HEADS)], axis=0)

    query = heads(joined)
    keys = joined[at, HEADS * HS : (HEADS + 1) * HS]
    values = joined[at, (HEADS + 1) * HS :]
    shape = (HEADS * BLOCK, BLOCK)
    row = lax.rem(lax.broadcasted_iota(jnp.int32, shape, 0), BLOCK)
    col = lax.broadcasted_iota(jnp.int32, shape, 1)
    allowed = (col <= row) & (col < jnp.broadcast_to(length, shape))
    scores = jnp.where(allowed, dot(query, keys, 1, 1) * scale, -1e30)
    peak = jnp.max(scores, axis=-1, keepdims=True)
    expo = jnp.exp(scores - peak)
    weights = expo / jnp.sum(expo, axis=-1, keepdims=True)
    wide = (HEADS * BLOCK, HS)
    live = lax.rem(lax.broadcasted_iota(jnp.int32, wide, 0), BLOCK) < jnp.broadcast_to(length, wide)
    upstream = jnp.where(live, heads(up).astype(F32), 0.0).astype(BF16)
    probs = weights.astype(BF16)
    grad_values = dot(probs.T, upstream, 1, 0).astype(BF16)
    grad_probs = dot(upstream, values, 1, 1)
    centre = jnp.sum(weights * grad_probs, axis=-1, keepdims=True)
    grad_scores = (weights * (grad_probs - centre) * scale).astype(BF16)
    grad_query = dot(grad_scores, keys, 1, 0).astype(BF16)
    grad_keys = dot(grad_scores.T, query, 1, 0).astype(BF16)
    for h in range(HEADS):
        comb[at, h * HS : (h + 1) * HS] = grad_query[h * BLOCK : (h + 1) * BLOCK]
    comb[at, HEADS * HS : (HEADS + 1) * HS] = grad_keys
    comb[at, (HEADS + 1) * HS :] = grad_values


SLABS = 4
SLAB = D // SLABS


def slab_copy(proj, proj_v, sem, k):
    at = pl.ds(k * SLAB, SLAB)
    return pltpu.make_async_copy(proj.at[at], proj_v.at[at], sem.at[k])


def join(proj, proj_v, sem, x, acc, joined):
    for k in range(SLABS):
        slab_copy(proj, proj_v, sem, k).wait()
        at = slice(k * SLAB, (k + 1) * SLAB)
        part = dot(x[:, at], proj_v[at, :], 1, 0)
        if k == SLABS - 1:
            joined[...] = (acc[...] + part).astype(BF16)
        elif k:
            acc[...] += part
        else:
            acc[...] = part


NZ, NY, NX = 8, 4, 4


def wrap(i, n):
    return lax.rem(i + n, n)


def vote_kernel(info, tok, cot, tok_a, cot_a, tok_b, cot_b, proj, comb01, xt01, out,
                cand_t, cand_c, proj_v, x3, up3, acc3, joined3, comb3, xt3, grad, mail,
                part, wz, wx, wy, rzp0, rzp1, rzm0, rzm1, szp0, szp1, szm0,
                szm1, rx, sx, ry, sy, ux, uy, uz, vx, vy, vz, tx, ty, tz, qx, qy, qz, res, fin,
                loc, psem, s0, r0, s1, r1, s2, r2, s3, r3, s4, r4):
    z, xh, y, xl, core = [lax.axis_index(a) for a in DP_REP]
    x = xh * 2 + xl

    def at_x(i):
        return {"dp_1": lax.div(i, 2), "rep_0": lax.rem(i, 2)}

    def at_y(i):
        return {"dp_2": i}

    def at_z(i):
        return {"dp_0": i}

    partner = {"rep_1": 1 - core}

    loads = [(tok.at[2], cand_t.at[0]), (tok_a, cand_t.at[1]), (tok_b, cand_t.at[2])]
    loads += [(cot.at[2], cand_c.at[0]), (cot_a, cand_c.at[1]), (cot_b, cand_c.at[2])]
    loads = [pltpu.make_async_copy(a, b, loc.at[i]) for i, (a, b) in enumerate(loads)]
    for load in loads[:3]:
        load.start()
    for k in range(SLABS):
        slab_copy(proj, proj_v, psem, k).start()
    for load in loads[3:]:
        load.start()

    barrier = pltpu.get_barrier_semaphore()
    peers = [partner]
    peers += [at_x(wrap(x + d, NX)) for d in range(1, NX)]
    peers += [at_y(wrap(y + d, NY)) for d in range(1, NY)]
    peers += [at_z(wrap(z + d, NZ)) for d in range(1, NZ)]
    for peer in peers:
        pl.semaphore_signal(barrier, inc=1, device_id=peer, device_id_type=MESH)

    sent = []

    def send(src, dst, ss, rs, dev):
        copy = pltpu.make_async_remote_copy(
            src_ref=src, dst_ref=dst, send_sem=ss, recv_sem=rs, device_id=dev, device_id_type=MESH
        )
        copy.start()
        sent.append(copy)
        return copy

    def add(*refs):
        total = refs[0][...].astype(F32)
        for ref in refs[1:]:
            total = total + ref[...].astype(F32)
        return total

    def chosen(c):
        way = jnp.broadcast_to(info[1:2, 0:1], c.shape[1:])
        return jnp.where(way == 1, c[1], jnp.where(way == 2, c[2], c[0]))

    for load in loads[:3]:
        load.wait()
    x3[...] = chosen(cand_t)
    for r in range(D // 512):
        xt3[r * 512 : (r + 1) * 512, :] = x3[:, r * 512 : (r + 1) * 512].T
    join(proj, proj_v, psem, x3, acc3, joined3)
    for load in loads[3:]:
        load.wait()
    up3[...] = chosen(cand_c)
    attention(slice(None), info[2:3, 0:1], joined3, up3, comb3)
    pl.semaphore_wait(barrier, len(peers))

    tile, chunk = 128, 512
    other = 1 - core

    def step(begin, end):
        if begin is not None:
            j, to_partner, buf = begin
            cols = pl.ds(pl.multiple_of(((other if to_partner else core) * 3 + j) * HS, HS), HS)

        total = jnp.zeros((8, HS), F32)
        for q in range(D // chunk):
            if begin is not None:
                at = pl.ds(q * chunk, chunk)
                new = dot(xt01[at, :], comb01[:, cols], 1, 0)
                new = new + dot(xt3[at, :], comb3[:, cols], 1, 0)
                grad[buf, at, :] = new
                total = total + jnp.sum((new * new).reshape(chunk // 8, 8, HS), axis=0)
            if end is None:
                continue
            for t in range(chunk // tile):
                a, h = divmod(q * (chunk // tile) + t, 2)
                old = grad[end[2], pl.ds(a * 256 + h * tile, tile), :]
                soft = (old / (jnp.abs(old) + end[3])).reshape(NY, 2, 16, HS)
                if end[1]:
                    mail[end[0], a, h] = soft.astype(BF16)
                    continue
                both = (soft + part[end[0], a, h].astype(F32)).astype(BF16)
                if end[0] == 0:
                    wz[a, h] = both
                elif end[0] == 1:
                    for l in range(2):
                        wx[h, l, a] = both[:, l]
                else:
                    for b in range(NY):
                        wy[b, a, h] = both[b]
        if begin is None:
            return None
        total = jnp.sum(jnp.sum(total, axis=0, keepdims=True), axis=1, keepdims=True)
        return (*begin, 0.25 * jnp.sqrt(total * (1.0 / (D * HS)) + 1e-06))

    first = {}

    def post(j):
        first[j] = send(mail.at[j], part.at[j], s0.at[j], r0.at[j], partner)

    now = step((0, True, 0), None)
    now = step((1, True, 1), now)
    post(0)
    now = step((2, True, 0), now)
    post(1)
    now = step((0, False, 1), now)
    post(2)
    first[0].wait_recv()
    now = step((1, False, 0), now)

    up_z, down_z = at_z(wrap(z + 1, NZ)), at_z(wrap(z - 1, NZ))

    def zpiece(d, h):
        return wz.at[wrap(z + d, NZ), h]

    zp0 = [send(zpiece(4, 0), rzp0.at[0], s1.at[0], r1.at[0], up_z)]
    zm1 = [send(zpiece(-4, 1), rzm1.at[0], s1.at[1], r1.at[1], down_z)]
    zp1 = [send(zpiece(3, 1), rzp1.at[0], s1.at[2], r1.at[2], up_z)]
    zm0 = [send(zpiece(-3, 0), rzm0.at[0], s1.at[3], r1.at[3], down_z)]

    def four_ring(j, c, w, dev, recv, base):
        ahead, behind = dev(wrap(c + 1, 4)), dev(wrap(c - 1, 4))
        far = wrap(c + 2, 4)
        lo, hi = pl.ds(0, 4), pl.ds(4, 4)
        sem = lambda i: (s2.at[base + i], r2.at[base + i])
        return [
            send(w(far).at[lo], recv.at[0], *sem(0), ahead),
            send(w(far).at[hi], recv.at[1], *sem(1), behind),
            send(w(wrap(c + 1, 4)).at[hi], recv.at[3], *sem(2), ahead),
            send(w(wrap(c - 1, 4)).at[lo], recv.at[4], *sem(3), behind),
        ]

    def relay(c, w, dev, recv, hold, base, begun):
        ahead, behind = dev(wrap(c + 1, 4)), dev(wrap(c - 1, 4))
        sem = lambda i: (s2.at[base + i], r2.at[base + i])
        out_copies = []
        for i, (step, half, slot, to) in enumerate(((1, 0, 2, ahead), (-1, 4, 5, behind))):
            begun[i].wait_recv()
            mine = w(wrap(c + step, 4))

            @pl.loop(0, 4)
            def _(a):
                hold[i, a] = add(mine.at[half + a], recv.at[i, a]).astype(BF16)

            out_copies.append(send(hold.at[i], recv.at[slot], *sem(4 + i), to))
        return out_copies

    wx_of = lambda c: wx.at[lax.div(c, 2), lax.rem(c, 2)]
    wy_of = lambda c: wy.at[c]

    first[1].wait_recv()
    now = step((2, False, 1), now)
    bx = four_ring(1, x, wx_of, at_x, rx, 0)
    first[2].wait_recv()
    step(None, now)
    by = four_ring(2, y, wy_of, at_y, ry, 6)

    def z_relay(k):
        def hop(chain, recv, hold, d, h, sem, to):
            chain[k - 1].wait_recv()
            hold[k - 1] = add(zpiece(d, h), recv.at[k - 1]).astype(BF16)
            chain.append(send(hold.at[k - 1], recv.at[k], s1.at[sem], r1.at[sem], to))

        hop(zp0, rzp0, szp0, 4 - k, 0, 4 * k, up_z)
        hop(zm1, rzm1, szm1, k - 4, 1, 4 * k + 1, down_z)
        if k < 3:
            hop(zp1, rzp1, szp1, 3 - k, 1, 4 * k + 2, up_z)
            hop(zm0, rzm0, szm0, k - 3, 0, 4 * k + 3, down_z)

    z_relay(1)
    cx = relay(x, wx_of, at_x, rx, sx, 0, bx)
    cy = relay(y, wy_of, at_y, ry, sy, 6, by)
    z_relay(2)
    z_relay(3)

    def settle(c, w, recv, begun, later, store):
        later[0].wait_recv()
        begun[2].wait_recv()
        begun[3].wait_recv()
        later[1].wait_recv()
        mine = w(c)

        @pl.loop(0, 4)
        def _(a):
            store(a, add(mine.at[a], recv.at[2, a], recv.at[4, a]))
            store(4 + a, add(mine.at[4 + a], recv.at[3, a], recv.at[5, a]))

    def store_x(a, v):
        ux[:, a] = v.astype(BF16)

    def store_y(a, v):
        uy[:, :, a] = v.astype(BF16)

    def spread(u, c, n, dev, recv, ss, rs, base):
        return [
            send(u(wrap(c + d, n)), recv.at[d - 1], ss.at[base + d - 1], rs.at[base + d - 1],
                 dev(wrap(c + d, n)))
            for d in range(1, n)
        ]

    ux_of = lambda c: ux.at[c]
    uy_of = lambda c: uy.at[lax.div(c, 2), lax.rem(c, 2)]
    uz_of = lambda c: uz.at[lax.div(c, 2), lax.rem(c, 2)]
    settle(x, wx_of, rx, bx, cx, store_x)
    dx = spread(ux_of, y, NY, at_y, vx, s3, r3, 0)
    settle(y, wy_of, ry, by, cy, store_y)
    dy = spread(uy_of, x, NX, at_x, vy, s3, r3, 3)
    for chain in (zp0, zm0, zp1, zm1):
        chain[-1].wait_recv()
    for h, (a, b) in enumerate(((rzp0.at[3], rzm0.at[2]), (rzp1.at[2], rzm1.at[3]))):
        v = add(zpiece(0, h), a, b)
        for l in range(2):
            uz[h, l] = v[:, l].astype(BF16)
    dz = spread(uz_of, x, NX, at_x, vz, s3, r3, 6)

    def gather(copies, u, c, recv, hold):
        for copy in copies:
            copy.wait_recv()
        hold[...] = add(u(c), *[recv.at[i] for i in range(len(copies))]).astype(BF16)

    gather(dx, ux_of, y, vx, tx)
    ex = spread(lambda c: tx.at[c], z, NZ, at_z, qx, s4, r4, 0)
    gather(dy, uy_of, x, vy, ty)
    ey = spread(lambda c: ty.at[c], z, NZ, at_z, qy, s4, r4, 7)
    gather(dz, uz_of, x, vz, tz)
    ez = spread(lambda c: tz.at[c], y, NY, at_y, qz, s4, r4, 14)

    def finish(j, copies, mine, recv):
        for copy in copies:
            copy.wait_recv()
        total = add(mine, *[recv.at[i] for i in range(len(copies))]) * (1.0 / 16.0)
        res[j, 0] = total[0:8]
        res[j, 1] = total[8:16]

    finish(0, ez, tz.at[y], qz)
    finish(1, ex, tx.at[z], qx)
    finish(2, ey, ty.at[z], qy)
    ends = [
        send(res.at[j, 1 - core], fin.at[j], s0.at[3 + j], r0.at[3 + j], partner) for j in range(3)
    ]
    for j in range(3):
        out[core * 3 + j] = res[j, core]
    for j in range(3):
        ends[j].wait_recv()
        out[(1 - core) * 3 + j] = fin[j]
    for copy in sent:
        copy.wait_send()


def vote_sum(info, tokens, cotangent, moved, projection, comb, xt):
    vmem = pltpu.VMEM
    t = (16, HS)
    bf = lambda *dims: vmem(dims + t, BF16)
    sems = lambda n: pltpu.SemaphoreType.DMA((n,))
    scratch = [
        vmem((3, BLOCK, D), BF16),
        vmem((3, BLOCK, HEADS * HS), BF16),
        vmem((D, GROUPS * HS), BF16),
        vmem((BLOCK, D), BF16),
        vmem((BLOCK, HEADS * HS), BF16),
        vmem((BLOCK, GROUPS * HS), F32),
        vmem((BLOCK, GROUPS * HS), BF16),
        vmem((BLOCK, GROUPS * HS), BF16),
        vmem((D, BLOCK), BF16),
        vmem((2, D, HS), F32),
        bf(3, 8, 2, 4, 2),
        bf(3, 8, 2, 4, 2),
        bf(8, 2, 4, 2),
        bf(2, 2, 8, 4),
        bf(4, 8, 2, 2),
        bf(4, 4, 2), bf(3, 4, 2), bf(3, 4, 2), bf(4, 4, 2),
        bf(3, 4, 2), bf(2, 4, 2), bf(2, 4, 2), bf(3, 4, 2),
        bf(6, 4, 4), bf(2, 4, 4),
        bf(6, 4, 2, 2), bf(2, 4, 2, 2),
        bf(4, 8), bf(2, 2, 8), bf(2, 2, 4),
        bf(3, 8), bf(3, 8), bf(3, 4),
        bf(8), bf(8), bf(4),
        bf(7), bf(7), bf(3),
        vmem((3, 2, 8, HS), F32),
        vmem((3, 8, HS), F32),
        sems(6), sems(SLABS),
        sems(6), sems(6), sems(16), sems(16), sems(12), sems(12), sems(9), sems(9), sems(17), sems(17),
    ]
    return pl.pallas_call(
        vote_kernel,
        out_shape=jax.ShapeDtypeStruct((GROUPS, 8, HS), F32),
        in_specs=[pl.BlockSpec(memory_space=vmem)]
        + [pl.BlockSpec(memory_space=pl.ANY)] * 7
        + [pl.BlockSpec(memory_space=vmem)] * 2,
        out_specs=pl.BlockSpec(memory_space=pltpu.VMEM),
        scratch_shapes=scratch,
        compiler_params=pltpu.CompilerParams(
            collective_id=1, has_side_effects=True, vmem_limit_bytes=52 << 20
        ),
        name="vote_sum",
    )(info, tokens, cotangent, *moved, projection, comb, xt)


LEVELS = 6
PAIRS = [(a, b) for a in range(LEVELS) for b in range(a + 1, LEVELS)]
ALONE = {0: (0, 2), 1: (1, 2), 2: (0, 2), 3: (2, 3), 4: (2, 4), 5: (2, 5)}
APART = [((0, 1), (2, 3, 4, 5)), ((3, 5), (0, 1, 2)), ((4, 5), (0, 1, 2))]
APART += [((n, 4), (3,)) for n in range(3)]
APART = [(a, b, c, v) for (a, b), bits in APART for c in bits for v in range(2)]


def flipped(i, m):
    return i + m - 2 * m * lax.rem(lax.div(i, m), 2)


def across(level):
    if level < 2:
        return {"dp_2": flipped(lax.axis_index("dp_2"), 1 << level)}
    if level == 2:
        return {"dp_1": 1 - lax.axis_index("dp_1")}
    return {"dp_0": flipped(lax.axis_index("dp_0"), 1 << (level - 3))}


def plan_kernel(dest, lengths, tok, cot, proj, info, comb, xt, x01, up01, proj_v, acc, joined,
                mine, mixed, from_plane, from_z, loc, psem, ss, rs):
    z, xh, y, xl, core = [lax.axis_index(a) for a in DP_REP]
    x = xh * 2 + xl

    def at_plane(dx, dy, c):
        i = wrap(x + dx, NX)
        return {"dp_1": lax.div(i, 2), "rep_0": lax.rem(i, 2), "dp_2": wrap(y + dy, NY), "rep_1": c}

    plane = [(dx, dy, c) for dx in range(NX) for dy in range(NY) for c in range(2)][1:]
    plane = [at_plane(dx, dy, 1 - core if c else core) for dx, dy, c in plane]
    column = [{"dp_0": wrap(z + d, NZ)} for d in range(1, NZ)]
    peers = plane + column

    halves = [pl.ds(0, BLOCK), pl.ds(BLOCK, BLOCK)]
    loads = [(tok.at[b], x01.at[halves[b]]) for b in range(2)]
    loads += [(cot.at[b], up01.at[halves[b]]) for b in range(2)]
    loads = [pltpu.make_async_copy(a, b, loc.at[i]) for i, (a, b) in enumerate(loads)]
    for load in loads[:2]:
        load.start()
    for k in range(SLABS):
        slab_copy(proj, proj_v, psem, k).start()
    for load in loads[2:]:
        load.start()

    barrier = pltpu.get_barrier_semaphore()
    for peer in peers:
        pl.semaphore_signal(barrier, inc=1, device_id=peer, device_id_type=MESH)

    here = (xh * NY + y) * 4 + xl * 2 + core
    rank = z * 8 + xh * NY + y
    wide = (1, 128)
    lane = lax.broadcasted_iota(jnp.int32, wide, 1)
    target = jnp.full(wide, dest[0], jnp.int32)
    code = jnp.zeros(wide, jnp.int32)
    for level in range(LEVELS):
        code = jnp.where(target == flipped(rank, 1 << level), level + 1, code)
    code = code * 256 + jnp.full(wide, lengths[3], jnp.int32)
    mine[...] = jnp.where((lane == here) & (target >= 0), code, 0)

    for load in loads[:2]:
        load.wait()

    def spread(src, stage, landing, base):
        copies = []
        for i, peer in enumerate(stage):
            copy = pltpu.make_async_remote_copy(
                src_ref=src, dst_ref=landing.at[i], send_sem=ss.at[base + i],
                recv_sem=rs.at[base + i], device_id=peer, device_id_type=MESH,
            )
            copy.start()
            copies.append(copy)
        return copies

    pl.semaphore_wait(barrier, len(peers))
    first = spread(mine, plane, from_plane, 0)
    join(proj, proj_v, psem, x01, acc, joined)
    for load in loads[2:]:
        load.wait()
    for copy in first:
        copy.wait_recv()
    row = mine[...]
    for i in range(len(plane)):
        row = jnp.maximum(row, from_plane[i])
    mixed[...] = row
    second = spread(mixed, column, from_z, len(plane))
    for b in range(2):
        attention(halves[b], lengths[b], joined, up01, comb)
    for r in range(D // 512):
        xt[r * 512 : (r + 1) * 512, :] = x01[:, r * 512 : (r + 1) * 512].T
    for copy in second:
        copy.wait_recv()

    shape = (8, 128)
    behind = lax.broadcasted_iota(jnp.int32, shape, 0)
    lane = lax.broadcasted_iota(jnp.int32, shape, 1)
    table = jnp.broadcast_to(mixed[...], shape)
    for k in range(1, NZ):
        table = jnp.where(behind == k, jnp.broadcast_to(from_z[k - 1], shape), table)
    level_of = lax.shift_right_logical(table, 8)

    def largest(v):
        v = v.astype(F32)
        return jnp.max(jnp.max(v, axis=1, keepdims=True), axis=0, keepdims=True)

    active = jnp.zeros((1, 1), F32)
    sender = jnp.zeros(shape, jnp.int32)
    for level in range(LEVELS):
        found = level_of == level + 1
        active += largest(jnp.where(found, 1 << level, 0))
        if level < 2:
            there, back = here + (flipped(y, 1 << level) - y) * 4, z * 0
        elif level == 2:
            there, back = here + (1 - 2 * xh) * NY * 4, z * 0
        else:
            there, back = here, wrap(z - flipped(z, 1 << (level - 3)), NZ)
        sender = jnp.where(found & (lane == there) & (behind == back), table, sender)
    inbound = largest(lax.shift_right_logical(sender, 8))
    arriving = largest(jnp.bitwise_and(sender, 255))
    third = jnp.where(inbound > 0.0, arriving, jnp.full((1, 1), lengths[2], jnp.int32).astype(F32))
    branch = jnp.full((1, 1), float(len(PAIRS)), F32)
    way = jnp.ones((1, 1), F32)
    for p, (a, b) in enumerate(PAIRS):
        sets = [(1 << a) + (1 << b)] + [1 << s for s, both in ALONE.items() if both == (a, b)]
        hit = active == float(sets[0])
        for other in sets[1:] + ([0] if p == 0 else []):
            hit = hit | (active == float(other))
        branch = jnp.where(hit, float(p), branch)
        by = jnp.where(inbound == a + 1.0, 1.0, jnp.where(inbound == b + 1.0, 2.0, 0.0))
        way = jnp.where(hit, by, way)
    zrow = wrap(z - behind, NZ)
    ranks = zrow * 8 + lax.div(lane, 4)

    def has(level, c, v):
        bit = jnp.bitwise_and(lax.shift_right_logical(ranks, c), 1)
        return largest(jnp.where((level_of == level + 1) & (bit == v), 1, 0))

    seen = {(a, c, v): has(a, c, v) for a, c, v in sorted({(l, c, v) for a, b, c, _ in APART
                                                           for l in (a, b) for v in range(2)})}
    for p, (a, b, c, v) in enumerate(APART):
        clear = seen[a, c, 1 - v] + seen[b, c, v] == 0.0
        clear = clear & (active == float((1 << a) + (1 << b)))
        branch = jnp.where(clear, float(len(PAIRS) + 1 + p), branch)
        way = jnp.where(clear, jnp.where(inbound > 0.0, 1.0, 0.0), way)
    told = jnp.zeros(shape, F32)
    for i, v in enumerate((branch, way, third, inbound, active)):
        told = jnp.where(behind == i, v, told)
    info[...] = told.astype(jnp.int32)
    for copy in first + second:
        copy.wait_send()


def plan(destination, lengths, tokens, cotangent, projection):
    vmem = pltpu.VMEM
    plane, column = 2 * NX * NY - 1, NZ - 1
    width = GROUPS * HS
    return pl.pallas_call(
        plan_kernel,
        out_shape=(
            jax.ShapeDtypeStruct((8, 128), jnp.int32),
            jax.ShapeDtypeStruct((2 * BLOCK, width), BF16),
            jax.ShapeDtypeStruct((D, 2 * BLOCK), BF16),
        ),
        in_specs=[pl.BlockSpec(memory_space=pltpu.SMEM)] * 2
        + [pl.BlockSpec(memory_space=pltpu.HBM)] * 3,
        out_specs=[pl.BlockSpec(memory_space=vmem)] * 3,
        scratch_shapes=[
            vmem((2 * BLOCK, D), BF16),
            vmem((2 * BLOCK, HEADS * HS), BF16),
            vmem((D, width), BF16),
            vmem((2 * BLOCK, width), F32),
            vmem((2 * BLOCK, width), BF16),
            vmem((1, 128), jnp.int32),
            vmem((1, 128), jnp.int32),
            vmem((plane, 1, 128), jnp.int32),
            vmem((column, 1, 128), jnp.int32),
            pltpu.SemaphoreType.DMA((4,)),
            pltpu.SemaphoreType.DMA((SLABS,)),
            pltpu.SemaphoreType.DMA((plane + column,)),
            pltpu.SemaphoreType.DMA((plane + column,)),
        ],
        compiler_params=pltpu.CompilerParams(
            collective_id=2, has_side_effects=True, vmem_limit_bytes=52 << 20
        ),
        name="plan",
    )(destination, lengths, tokens, cotangent, projection)


def move_apart(p):
    a, b, c, v = APART[p]

    def kernel(tokens, cotangent, tok_a, cot_a, tok_b, cot_b, ss, rs):
        here = {name: lax.axis_index(name) for name in DP}
        rank = (here["dp_0"] * 2 + here["dp_1"]) * NY + here["dp_2"]
        bit = lax.rem(lax.div(rank, 1 << c), 2)
        in_a = bit if v else 1 - bit
        to_a, to_b = {**here, **across(a)}, {**here, **across(b)}
        peer = {name: to_b[name] + in_a * (to_a[name] - to_b[name]) for name in DP}
        barrier = pltpu.get_barrier_semaphore()
        pl.semaphore_signal(barrier, inc=1, device_id=peer, device_id_type=MESH)
        pl.semaphore_wait(barrier, 1)
        copies = []
        for i, (src, dst) in enumerate(((tokens, tok_a), (cotangent, cot_a))):
            copies.append(pltpu.make_async_remote_copy(
                src_ref=src.at[3], dst_ref=dst, send_sem=ss.at[i], recv_sem=rs.at[i],
                device_id=peer, device_id_type=MESH,
            ))
            copies[-1].start()
        for copy in copies:
            copy.wait()

    return mover(kernel, 3 + len(PAIRS) + p)


def move_pair(p):
    peers_of = PAIRS[p]

    def kernel(tokens, cotangent, tok_a, cot_a, tok_b, cot_b, ss, rs):
        peers = [across(level) for level in peers_of]
        barrier = pltpu.get_barrier_semaphore()
        for peer in peers:
            pl.semaphore_signal(barrier, inc=1, device_id=peer, device_id_type=MESH)
        pl.semaphore_wait(barrier, 2)
        copies = []
        for i, (src, dst, peer) in enumerate((
            (tokens, tok_a, peers[0]), (tokens, tok_b, peers[1]),
            (cotangent, cot_a, peers[0]), (cotangent, cot_b, peers[1]),
        )):
            copies.append(pltpu.make_async_remote_copy(
                src_ref=src.at[3], dst_ref=dst, send_sem=ss.at[i], recv_sem=rs.at[i],
                device_id=peer, device_id_type=MESH,
            ))
            copies[-1].start()
        for copy in copies:
            copy.wait()

    return mover(kernel, 3 + p)


def mover(kernel, collective_id):
    def call(tokens, cotangent, info):
        block = jax.ShapeDtypeStruct(tokens.shape[1:], BF16)
        upstream = jax.ShapeDtypeStruct(cotangent.shape[1:], BF16)
        return pl.pallas_call(
            kernel,
            out_shape=(block, upstream, block, upstream),
            in_specs=[pl.BlockSpec(memory_space=pl.ANY)] * 2,
            out_specs=[pl.BlockSpec(memory_space=pl.ANY)] * 4,
            scratch_shapes=[pltpu.SemaphoreType.DMA((4,)), pltpu.SemaphoreType.DMA((4,))],
            compiler_params=pltpu.CompilerParams(
                collective_id=collective_id, has_side_effects=True, vmem_limit_bytes=2 << 20
            ),
            name="move",
        )(tokens, cotangent)

    return call


def many_kernel(info, tokens, cotangent, tok_a, cot_a, tok_b, cot_b, all_t, all_c, own, ss, rs):
    peers = [across(level) for level in range(LEVELS)]
    barrier = pltpu.get_barrier_semaphore()
    for peer in peers:
        pl.semaphore_signal(barrier, inc=1, device_id=peer, device_id_type=MESH)
    keep = [
        pltpu.make_async_copy(tokens.at[2], tok_a, own.at[0]),
        pltpu.make_async_copy(cotangent.at[2], cot_a, own.at[1]),
    ]
    for copy in keep:
        copy.start()
    pl.semaphore_wait(barrier, LEVELS)
    copies = []
    for level, peer in enumerate(peers):
        for i, (src, dst) in enumerate(((tokens, all_t), (cotangent, all_c))):
            copies.append(pltpu.make_async_remote_copy(
                src_ref=src.at[3], dst_ref=dst.at[level], send_sem=ss.at[2 * level + i],
                recv_sem=rs.at[2 * level + i], device_id=peer, device_id_type=MESH,
            ))
            copies[-1].start()
    for copy in keep:
        copy.wait()
    for copy in copies:
        copy.wait()
    for level in range(LEVELS):
        for got, out in ((all_t, tok_a), (all_c, cot_a)):
            arrived = jnp.broadcast_to(info[3:4, 0:1], out.shape) == level + 1
            out[...] = jnp.where(arrived, got[level], out[...])


def move_many(tokens, cotangent, info):
    block, upstream = tokens.shape[1:], cotangent.shape[1:]
    like = [jax.ShapeDtypeStruct(s, BF16) for s in (block, upstream)]
    vmem = pltpu.VMEM
    return pl.pallas_call(
        many_kernel,
        out_shape=(*like, *like),
        in_specs=[pl.BlockSpec(memory_space=vmem)] + [pl.BlockSpec(memory_space=pl.ANY)] * 2,
        out_specs=[pl.BlockSpec(memory_space=vmem)] * 2 + [pl.BlockSpec(memory_space=pl.ANY)] * 2,
        scratch_shapes=[
            vmem((LEVELS,) + block, BF16),
            vmem((LEVELS,) + upstream, BF16),
            pltpu.SemaphoreType.DMA((2,)),
            pltpu.SemaphoreType.DMA((2 * LEVELS,)),
            pltpu.SemaphoreType.DMA((2 * LEVELS,)),
        ],
        compiler_params=pltpu.CompilerParams(
            collective_id=3 + len(PAIRS) + len(APART), has_side_effects=True,
            vmem_limit_bytes=10 << 20,
        ),
        name="move_many",
    )(info, tokens, cotangent)


def shards(tokens, cotangent, projection, block_lengths, destination):
    lengths = block_lengths[0]
    info, comb, xt = plan(destination, lengths, tokens, cotangent, projection)
    branches = [move_pair(p) for p in range(len(PAIRS))] + [move_many]
    branches += [move_apart(p) for p in range(len(APART))]
    moved = lax.switch(info[0, 0], branches, tokens, cotangent, info)
    summed = vote_sum(info, tokens, cotangent, moved, projection, comb, xt)
    return summed.transpose(1, 0, 2).reshape(8, GROUPS * HS)


def solution(mesh):
    split = Mesh(mesh.devices.reshape(8, 2, 4, 2, 2), DP_REP)
    placed = (P(DP_REP, None, None), P(DP_REP, None, None), P(), P(DP_REP, None), P(DP_REP))
    return jax.shard_map(
        shards, mesh=split, in_specs=placed, out_specs=P(DP_REP, None), check_vma=False
    )
```
